128 devices in a mesh: gx: 4 (over z_lo, core), gy: 16 (over x, y), gz: 2 (over z_hi).
Axes of the slice: x: 4, y: 4, z: 4 (z_hi: 2, z_lo: 2; z = z_hi * 2 + z_lo), core: 2. Of those that a mesh axis runs over, the one named last changes fastest.
Arguments:
- eigvecs: bfloat16 [64, 128, 96, 512], P('gx', 'gy', 'gz'), may hold values from -7 to 7, as said below
- material: float32 [2, 64, 128, 96], P(None, 'gx', 'gy', 'gz'), may hold values from 0.5 to 2
Outputs:
- stiffness: float32 [512, 512], P(('gx', 'gy', 'gz'))
- mass_matrix: float32 [512, 512], P(('gx', 'gy', 'gz'))
The draws below stay inside these ranges and needn't reach their ends.
Inputs may be any that keep to these rules, and one draw needn't show every extreme that they name: `eigvecs`: entries are a rough part plus a part that varies slowly over the grid.
All inputs are finite; a program needn't handle non-finite values.
Results may differ from the reference program's by a relative error of at most 0.0003.
Values may be sent and summed in bfloat16 or wider, within the bound.
A program may use at most 128 MiB of HBM per device.

```python
import math
import jax
import jax.numpy as jnp
from jax import lax

K = 512
NX = 64
NY = 128
NZ = 96


def draw_eigvecs(key, part):
    keys = jax.random.split(key, 7)
    rough = jnp.clip(jax.random.normal(keys[0], (NX, NY, NZ, K), jnp.float32), -4.0, 4.0)
    amplitude = 2.0
    freq_x = jax.random.randint(keys[1], (K,), 1, 4).astype(jnp.float32)
    freq_y = jax.random.randint(keys[2], (K,), 1, 4).astype(jnp.float32)
    freq_z = jax.random.randint(keys[3], (K,), 1, 4).astype(jnp.float32)
    phase_x = jax.random.uniform(keys[4], (K,), jnp.float32)
    phase_y = jax.random.uniform(keys[5], (K,), jnp.float32)
    phase_z = jax.random.uniform(keys[6], (K,), jnp.float32)
    coord_x = jnp.arange(NX, dtype=jnp.float32)[:, None] / NX
    coord_y = jnp.arange(NY, dtype=jnp.float32)[:, None] / NY
    coord_z = jnp.arange(NZ, dtype=jnp.float32)[:, None] / NZ
    wave_x = jnp.cos(2.0 * jnp.pi * (coord_x * freq_x + phase_x))
    wave_y = jnp.cos(2.0 * jnp.pi * (coord_y * freq_y + phase_y))
    wave_z = jnp.cos(2.0 * jnp.pi * (coord_z * freq_z + phase_z))
    smooth = wave_x[:, None, None, :] * wave_y[None, :, None, :] * wave_z[None, None, :, :]
    return (rough + amplitude * smooth).astype(jnp.bfloat16)


def shard_levels(own_key, shape, cuts, low, top_value):
    factor_of = 1.0
    for dim, shards_of in cuts:
        heights = jax.random.uniform(jax.random.fold_in(jax.random.fold_in(own_key, 6), dim), (shards_of,), jnp.float32, low / len(cuts), top_value / len(cuts))
        factor_of = factor_of * jnp.repeat(jnp.exp(heights), shape[dim] // shards_of).reshape((-1,) + (1,) * (len(shape) - 1 - dim))
    return factor_of


def setup_inputs(seed: int = 0) -> dict:
    streams_of = jax.random.split(jax.random.key(seed), 3)
    eigvecs = draw_eigvecs(jax.random.fold_in(streams_of[2], 71), 0)
    material = jnp.clip(jnp.exp(math.log(2.0) - 1.3862944 * jax.random.uniform(streams_of[1], (2, NX, NY, NZ), jnp.float32) ** shard_levels(streams_of[1], (2, NX, NY, NZ), ((1, 4), (2, 16), (3, 2)), -0.2, 0.2)), 0.5, 2.0)
    return {"eigvecs": eigvecs, "material": material}


stencil_offsets = [(dx, dy, dz) for dx in (-1, 0, 1) for dy in (-1, 0, 1) for dz in (-1, 0, 1) if (dx, dy, dz) != (0, 0, 0)]


def coupling(offset):
    nonzero = sum(abs(entry) for entry in offset)
    return 0.25 * 0.5 ** (nonzero - 1)


def mass_weight(offset):
    weight = 1.0
    for entry in offset:
        weight = weight * (4.0 / 6.0 if entry == 0 else 1.0 / 6.0)
    return weight


def apply_operators(padded, padded_material):
    size_x = padded.shape[0] - 2
    size_y = padded.shape[1] - 2
    size_z = padded.shape[2] - 2
    centre = padded[1:-1, 1:-1, 1:-1].astype(jnp.float32)
    kappa_centre = padded_material[0, 1:-1, 1:-1, 1:-1]
    rho_centre = padded_material[1, 1:-1, 1:-1, 1:-1]
    stiff_sum = jnp.zeros(centre.shape, jnp.float32)
    mass_sum = mass_weight((0, 0, 0)) * rho_centre[..., None] * centre
    for offset in stencil_offsets:
        lower = (1 + offset[0], 1 + offset[1], 1 + offset[2])
        shifted = padded[lower[0]:lower[0] + size_x, lower[1]:lower[1] + size_y, lower[2]:lower[2] + size_z].astype(jnp.float32)
        kappa_side = padded_material[0, lower[0]:lower[0] + size_x, lower[1]:lower[1] + size_y, lower[2]:lower[2] + size_z]
        rho_side = padded_material[1, lower[0]:lower[0] + size_x, lower[1]:lower[1] + size_y, lower[2]:lower[2] + size_z]
        stiff_sum = stiff_sum + (coupling(offset) * 0.5 * (kappa_centre + kappa_side))[..., None] * (centre - shifted)
        mass_sum = mass_sum + (mass_weight(offset) * 0.5 * (rho_centre + rho_side))[..., None] * shifted
    return stiff_sum.astype(jnp.bfloat16), mass_sum.astype(jnp.bfloat16)


def reference(eigvecs, material):
    cells = NX * NY * NZ
    block_cols = 32
    padded_material = jnp.pad(material, ((0, 0), (1, 1), (1, 1), (1, 1)))
    flat_vectors = eigvecs.reshape(cells, K)

    def column_block(block_index):
        first_col = block_index * block_cols
        col_block = lax.dynamic_slice_in_dim(eigvecs, first_col, block_cols, 3)
        padded = jnp.pad(col_block, ((1, 1), (1, 1), (1, 1), (0, 0)))
        stiff_vecs, mass_vecs = apply_operators(padded, padded_material)
        dims = (((0,), (0,)), ((), ()))
        stiff_cols = lax.dot_general(flat_vectors, stiff_vecs.reshape(cells, block_cols), dims, preferred_element_type=jnp.float32)
        mass_cols = lax.dot_general(flat_vectors, mass_vecs.reshape(cells, block_cols), dims, preferred_element_type=jnp.float32)
        return stiff_cols, mass_cols

    stiff_blocks, mass_blocks = lax.map(column_block, jnp.arange(K // block_cols, dtype=jnp.int32))
    stiffness = jnp.transpose(stiff_blocks, (1, 0, 2)).reshape(K, K) / cells
    mass_matrix = jnp.transpose(mass_blocks, (1, 0, 2)).reshape(K, K) / cells
    return stiffness, mass_matrix
```

```python
import functools

import jax
import jax.numpy as jnp
import numpy as np
from jax import lax
from jax.experimental import pallas as pl
from jax.experimental.pallas import tpu as pltpu
from jax.sharding import PartitionSpec as P

MESH = pl.DeviceIdType.MESH
F32 = jnp.float32
BF16 = jnp.bfloat16
HIGH = lax.Precision.HIGHEST

SX, SY, SZ, K = 16, 8, 48, 512
PX, PY = SX + 2, SY + 2
HALF = PY // 2
CELLS = 64 * 128 * 96
DIM0 = (((0,), (0,)), ((), ()))


def constants():
    rows = HALF * SZ
    tz = np.zeros((rows, rows), np.float32)
    for r in range(rows):
        for c in (r - 1, r, r + 1):
            if 0 <= c < rows and c // SZ == r // SZ:
                tz[r, c] = 2.0 if c == r else 1.0
    sel = np.zeros((SX * SY, 256), np.float32)
    txy = np.zeros((SX * SY, 256), np.float32)
    for x in range(SX):
        for y in range(SY):
            row = x * SY + y
            sel[row, (x + 1) * PY + y + 1] = 1.0
            for dx in (-1, 0, 1):
                for dy in (-1, 0, 1):
                    txy[row, (x + 1 + dx) * PY + y + 1 + dy] = (2 - abs(dx)) * (2 - abs(dy))
    places = {}
    for x in range(SX):
        for y in range(SY):
            places[(x, y)] = x * SY + y
    for x in range(SX):
        places[(x, SY)] = 128 + x
        places[(x, -1)] = 144 + x
    for y in range(SY):
        places[(SX, y)] = 160 + y
        places[(-1, y)] = 176 + y
    places[(SX, SY)] = 192
    places[(SX, -1)] = 208 + 7
    places[(-1, SY)] = 224
    places[(-1, -1)] = 240 + 7
    t2 = np.zeros((128, 256), np.float32)
    t4 = np.zeros((128, 256), np.float32)
    for x in range(SX):
        for y in range(SY):
            for dx in (-1, 0, 1):
                for dy in (-1, 0, 1):
                    place = places[(x + dx, y + dy)]
                    t2[x * SY + y, place] = (2 - abs(dx)) * (2 - abs(dy))
                    t4[x * SY + y, place] = (4 - 3 * abs(dx)) * (4 - 3 * abs(dy))
    pick = np.zeros((64, 128), np.float32)
    for x in range(SX):
        pick[x, x * SY] = 1.0
        pick[16 + x, x * SY + 7] = 1.0
    for y in range(SY):
        pick[32 + y, y] = 1.0
        pick[48 + y, 15 * SY + y] = 1.0
    return tz, sel, txy, t2, t4, np.ascontiguousarray(t2.T), pick


def local_kernel(
    v_hbm, mat, tz_ref, sel_ref, txy_ref, t2_ref, t4_ref, t2t_ref, pick_ref, out,
    vp, az, bz, ya, yb, xbuf, vt, coef, acc, zf, zs, zh, zface,
    own_sem, up_send, dn_send, up_recv, dn_recv, side_send, side_recv, z_send, z_recv,
):
    gx, gy, gz = lax.axis_index("gx"), lax.axis_index("gy"), lax.axis_index("gz")
    other = 1 - gz

    def at(dx, dy, z):
        return {"gx": lax.rem(gx + dx + 4, 4), "gy": lax.rem(gy + dy + 16, 16), "gz": z}

    around = [(dx, dy) for dx in (-1, 0, 1) for dy in (-1, 0, 1)]
    barrier = pltpu.get_barrier_semaphore()
    for dx, dy in around:
        if (dx, dy) != (0, 0):
            pl.semaphore_signal(barrier, inc=1, device_id=at(dx, dy, gz), device_id_type=MESH)
        pl.semaphore_signal(barrier, inc=1, device_id=at(dx, dy, other), device_id_type=MESH)

    def own_copy(x):
        return pltpu.make_async_copy(v_hbm.at[x], vp.at[x + 1, pl.ds(1, SY)], own_sem.at[x])

    @pl.loop(0, SX)
    def _(x):
        own_copy(x).start()

    def has(dx, dy):
        ok = jnp.bool_(True)
        if dx == 1:
            ok = jnp.logical_and(ok, gx < 3)
        if dx == -1:
            ok = jnp.logical_and(ok, gx > 0)
        if dy == 1:
            ok = jnp.logical_and(ok, gy < 15)
        if dy == -1:
            ok = jnp.logical_and(ok, gy > 0)
        return ok

    def remote(src, dst, send, recv, where):
        return pltpu.make_async_remote_copy(
            src_ref=src, dst_ref=dst, send_sem=send, recv_sem=recv, device_id=where, device_id_type=MESH
        )

    def up(x):
        return remote(v_hbm.at[x, SY - 1], vp.at[x + 1, 0], up_send.at[x], up_recv.at[x], at(0, 1, gz))

    def down(x):
        return remote(v_hbm.at[x, 0], vp.at[x + 1, PY - 1], dn_send.at[x], dn_recv.at[x], at(0, -1, gz))

    def side(index):
        dx, dy = sides[index]
        src_x = SX - 1 if dx == 1 else 0
        dst_x = 0 if dx == 1 else PX - 1
        if dy == 0:
            src, dst = v_hbm.at[src_x], vp.at[dst_x, pl.ds(1, SY)]
        elif dy == 1:
            src, dst = v_hbm.at[src_x, SY - 1], vp.at[dst_x, 0]
        else:
            src, dst = v_hbm.at[src_x, 0], vp.at[dst_x, PY - 1]
        return remote(src, dst, side_send.at[index], side_recv.at[index], at(dx, dy, gz))

    sides = [(1, 0), (1, 1), (1, -1), (-1, 0), (-1, 1), (-1, -1)]

    @pl.when(jnp.logical_not(has(0, -1)))
    def _():
        vp[:, 0] = jnp.zeros((PX, SZ, K), BF16)

    @pl.when(jnp.logical_not(has(0, 1)))
    def _():
        vp[:, PY - 1] = jnp.zeros((PX, SZ, K), BF16)

    @pl.when(jnp.logical_not(has(-1, 0)))
    def _():
        vp[0] = jnp.zeros((PY, SZ, K), BF16)

    @pl.when(jnp.logical_not(has(1, 0)))
    def _():
        vp[PX - 1] = jnp.zeros((PY, SZ, K), BF16)

    zrows = [(0, 0, 0, 128)]
    zrows += [(0, 1, 128, 16), (0, -1, 144, 16), (1, 0, 160, 16), (-1, 0, 176, 16)]
    zrows += [(1, 1, 192, 16), (1, -1, 208, 16), (-1, 1, 224, 16), (-1, -1, 240, 16)]
    for dx, dy, first, count in zrows[1:]:

        @pl.when(jnp.logical_not(has(dx, dy)))
        def _():
            zh[pl.ds(first, count)] = jnp.zeros((count, K), BF16)

    pl.semaphore_wait(barrier, 17)

    @pl.when(has(1, 0))
    def _():
        side(0).start()

    @pl.when(has(-1, 0))
    def _():
        side(3).start()

    for index in (1, 2, 4, 5):

        @pl.when(has(*sides[index]))
        def _():
            side(index).start()

    @pl.loop(0, SX)
    def _(x):
        @pl.when(has(0, 1))
        def _():
            up(x).start()

        @pl.when(has(0, -1))
        def _():
            down(x).start()

    kappa = mat[0].reshape(SX * SY, SZ)
    rho = mat[1].reshape(SX * SY, SZ)
    own_kappa = lax.dot_general(kappa, sel_ref[...], DIM0, precision=HIGH, preferred_element_type=F32)
    own_rho = lax.dot_general(rho, sel_ref[...], DIM0, precision=HIGH, preferred_element_type=F32)
    near = lax.dot_general(kappa, txy_ref[...], DIM0, precision=HIGH, preferred_element_type=F32)
    edge_row = jnp.zeros((1, 256), F32)
    near = (
        jnp.concatenate([edge_row, near[:-1]], axis=0)
        + 2.0 * near
        + jnp.concatenate([near[1:], edge_row], axis=0)
    )
    alpha = 2.0 * own_kappa + near * (1.0 / 32.0)
    beta = own_kappa * (1.0 / 16.0)
    for xp in range(PX):
        span = slice(xp * PY, xp * PY + PY)
        coef[xp, 0, :, 0:PY] = alpha[:, span]
        coef[xp, 1, :, 0:PY] = beta[:, span]
        coef[xp, 2, :, 0:PY] = own_rho[:, span]

    @pl.loop(0, SX)
    def _(x):
        own_copy(x).wait()
        low = vp[x + 1, 1 : 1 + SY, 0:16, :].astype(F32)
        high = vp[x + 1, 1 : 1 + SY, SZ - 16 : SZ, :].astype(F32)
        spot = lax.broadcasted_iota(jnp.int32, (1, 16, 1), 1)
        low = jnp.sum(jnp.where(spot == 0, low, 0.0), axis=1)
        high = jnp.sum(jnp.where(spot == 15, high, 0.0), axis=1)
        zf[pl.ds(pl.multiple_of(x * SY, SY), SY)] = jnp.where(gz == 0, high, low)

    zface[...] = zf[...].astype(BF16)
    zs[...] = jnp.dot(pick_ref[...], zface[...], preferred_element_type=F32).astype(BF16)

    def zcopy(index, dx, dy):
        first, count = zrows[index][2:]
        if (dx, dy) == (0, 0):
            src = zface
        elif dx == 0:
            src = zs.at[pl.ds(16 if dy == 1 else 0, 16)]
        else:
            src = zs.at[pl.ds(48 if dx == 1 else 32, 16)]
        return remote(
            src, zh.at[pl.ds(first, count)], z_send.at[index], z_recv.at[index], at(dx, dy, other)
        )

    for index, (dx, dy, _, _) in enumerate(zrows):

        @pl.when(has(-dx, -dy))
        def _():
            zcopy(index, -dx, -dy).start()

    acc[...] = jnp.zeros_like(acc)

    def wait_plane(xp):
        @pl.when(jnp.logical_and(xp >= 1, xp <= SX))
        def _():
            @pl.when(has(0, -1))
            def _():
                up(xp - 1).wait_recv()

            @pl.when(has(0, 1))
            def _():
                down(xp - 1).wait_recv()

        @pl.when(xp == 0)
        def _():
            for index in (0, 1, 2):
                dx, dy = sides[index]

                @pl.when(has(-dx, -dy))
                def _():
                    side(index).wait_recv()

        @pl.when(xp == PX - 1)
        def _():
            for index in (3, 4, 5):
                dx, dy = sides[index]

                @pl.when(has(-dx, -dy))
                def _():
                    side(index).wait_recv()

    def plane_stage(xp, slot):
        wait_plane(xp)
        for b in range(2):
            for c in range(2):
                lanes = slice(256 * c, 256 * c + 256)
                own = vp[xp, HALF * b : HALF * b + HALF, :, lanes]
                a = jnp.dot(
                    tz_ref[...], own.reshape(HALF * SZ, 256), preferred_element_type=F32
                ).astype(BF16).reshape(HALF, SZ, 256)
                az[HALF * b : HALF * b + HALF, :, lanes] = a
                bz[HALF * b : HALF * b + HALF, :, lanes] = a + (own + own)
        for y in range(SY):
            mid = az[y + 1]
            ya[slot, y] = (az[y] + az[y + 2]) + (mid + mid)
            mid = bz[y + 1]
            yb[slot, y] = (bz[y] + bz[y + 2]) + BF16(4.0) * mid

    def cell_stage(x):
        s0, s1, s2 = lax.rem(x, 3), lax.rem(x + 1, 3), lax.rem(x + 2, 3)
        for y in range(SY):
            al = coef[x + 1, 0, :, y + 1 : y + 2]
            be = coef[x + 1, 1, :, y + 1 : y + 2]
            ro = coef[x + 1, 2, :, y + 1 : y + 2]
            mid = ya[s1, y]
            u = (ya[s0, y] + ya[s2, y]) + (mid + mid)
            mid = yb[s1, y]
            m = (yb[s0, y] + yb[s2, y]) + BF16(4.0) * mid
            own = vp[x + 1, y + 1].astype(F32)
            xbuf[pl.ds(y * SZ, SZ), 0:K] = (al * own - be * u.astype(F32)).astype(BF16)
            xbuf[pl.ds(y * SZ, SZ), K : 2 * K] = (ro * m.astype(F32)).astype(BF16)
        vt[...] = vp[x + 1, 1 : 1 + SY].reshape(SY * SZ, K).T
        for c in range(4):
            lanes = slice(256 * c, 256 * c + 256)
            acc[:, lanes] += jnp.dot(vt[...], xbuf[:, lanes], preferred_element_type=F32)

    plane_stage(jnp.int32(0), jnp.int32(0))
    plane_stage(jnp.int32(1), jnp.int32(1))

    @pl.loop(0, SX)
    def _(x):
        plane_stage(x + 2, lax.rem(x + 2, 3))
        cell_stage(x)

    def halo_rows(xp, yp):
        return coef[xp, 0, :, yp : yp + 1] * vp[xp, yp].astype(F32)

    for xp in (0, PX - 1):
        for y in range(SY):
            xbuf[y * SZ : y * SZ + SZ, 0:K] = halo_rows(xp, y + 1).astype(BF16)
        vt[...] = vp[xp, 1 : 1 + SY].reshape(SY * SZ, K).T
        for c in range(2):
            lanes = slice(256 * c, 256 * c + 256)
            acc[:, lanes] += jnp.dot(vt[...], xbuf[:, lanes], preferred_element_type=F32)
    for yp in (0, PY - 1):
        @pl.loop(0, 3)
        def _(part):
            for i in range(6):
                xbuf[i * SZ : i * SZ + SZ, 0:K] = halo_rows(part * 6 + i, yp).astype(BF16)
            turned = vp[pl.ds(part * 6, 6), yp].reshape(6 * SZ, K).T
            for c in range(2):
                lanes = slice(256 * c, 256 * c + 256)
                acc[:, lanes] += jnp.dot(turned, xbuf[0 : 6 * SZ, lanes], preferred_element_type=F32)

    for index, (dx, dy, _, _) in enumerate(zrows):

        @pl.when(has(dx, dy))
        def _():
            zcopy(index, -dx, -dy).wait_recv()

    lane = lax.broadcasted_iota(jnp.int32, (SX * SY, SZ), 1)
    at_edge = lane == jnp.where(gz == 0, SZ - 1, 0)
    kappa_edge = jnp.sum(jnp.where(at_edge, kappa, 0.0), axis=1, keepdims=True)
    rho_edge = jnp.sum(jnp.where(at_edge, rho, 0.0), axis=1, keepdims=True)
    far = zh[...]
    du = jnp.dot(t2_ref[...], far, preferred_element_type=F32)
    dm = jnp.dot(t4_ref[...], far, preferred_element_type=F32)
    xbuf[0:128, 0:K] = (kappa_edge * (-1.0 / 16.0) * du).astype(BF16)
    xbuf[0:128, K : 2 * K] = (rho_edge * dm).astype(BF16)
    turned = zface[...].T
    for c in range(4):
        lanes = slice(256 * c, 256 * c + 256)
        acc[:, lanes] += jnp.dot(turned, xbuf[0:128, lanes], preferred_element_type=F32)
    reach = jnp.dot(
        t2t_ref[...], jnp.broadcast_to(kappa_edge, (128, 128)), precision=HIGH, preferred_element_type=F32
    ) * (1.0 / 32.0)
    for c in range(4):
        lanes = slice(128 * c, 128 * c + 128)
        xbuf[0:256, lanes] = (reach * far[:, lanes].astype(F32)).astype(BF16)
    turned = far.T
    for c in range(2):
        lanes = slice(256 * c, 256 * c + 256)
        acc[:, lanes] += jnp.dot(turned, xbuf[0:256, lanes], preferred_element_type=F32)

    for half, scale in ((0, 0.5 / CELLS), (1, 0.5 / (216.0 * CELLS))):
        for i in range(4):
            for j in range(i, 4):
                rows = slice(128 * i, 128 * i + 128)
                cols = slice(128 * j, 128 * j + 128)
                there = slice(K * half + 128 * j, K * half + 128 * j + 128)
                back = slice(K * half + 128 * i, K * half + 128 * i + 128)
                both = (acc[rows, there] + acc[cols, back].T) * scale
                out[rows, there] = both
                if i != j:
                    out[cols, back] = both.T

    @pl.loop(0, SX)
    def _(x):
        @pl.when(has(0, 1))
        def _():
            up(x).wait_send()

        @pl.when(has(0, -1))
        def _():
            down(x).wait_send()

    for index in range(6):

        @pl.when(has(*sides[index]))
        def _():
            side(index).wait_send()

    for index, (dx, dy, _, _) in enumerate(zrows):

        @pl.when(has(-dx, -dy))
        def _():
            zcopy(index, -dx, -dy).wait_send()


def local_products(eigvecs, material):
    tz, sel, txy, t2, t4, t2t, pick = constants()
    small = (
        jnp.asarray(tz, BF16), jnp.asarray(sel), jnp.asarray(txy), jnp.asarray(t2, BF16),
        jnp.asarray(t4, BF16), jnp.asarray(t2t), jnp.asarray(pick, BF16),
    )
    vmem = pl.BlockSpec(memory_space=pltpu.VMEM)
    dma = pltpu.SemaphoreType.DMA
    return pl.pallas_call(
        local_kernel,
        out_shape=jax.ShapeDtypeStruct((K, 2 * K), F32),
        in_specs=[pl.BlockSpec(memory_space=pl.ANY)] + [vmem] * 8,
        out_specs=vmem,
        scratch_shapes=[
            pltpu.VMEM((PX, PY, SZ, K), BF16),
            pltpu.VMEM((PY, SZ, K), BF16),
            pltpu.VMEM((PY, SZ, K), BF16),
            pltpu.VMEM((3, SY, SZ, K), BF16),
            pltpu.VMEM((3, SY, SZ, K), BF16),
            pltpu.VMEM((SY * SZ, 2 * K), BF16),
            pltpu.VMEM((K, SY * SZ), BF16),
            pltpu.VMEM((PX, 3, SZ, 128), F32),
            pltpu.VMEM((K, 2 * K), F32),
            pltpu.VMEM((SX * SY, K), F32),
            pltpu.VMEM((64, K), BF16),
            pltpu.VMEM((256, K), BF16),
            pltpu.VMEM((SX * SY, K), BF16),
            dma((SX,)), dma((SX,)), dma((SX,)), dma((SX,)), dma((SX,)),
            dma((6,)), dma((6,)), dma((9,)), dma((9,)),
        ],
        compiler_params=pltpu.CompilerParams(
            collective_id=0, has_side_effects=True, vmem_limit_bytes=60 * 1024 * 1024
        ),
    )(eigvecs, material, *small)


def split_up(x, dim, devices):
    dims = x.shape
    parts = x.reshape(*dims[:dim], devices, dims[dim] // devices, *dims[dim + 1 :])
    return jnp.moveaxis(parts, dim, 0)


def sum_at_owner(x, axis, dim):
    devices = lax.axis_size(axis)
    parts = lax.all_to_all(split_up(x, dim, devices), axis, 0, 0, tiled=True)
    return jnp.sum(parts, axis=0)


def per_device(eigvecs, material):
    both = local_products(eigvecs, material)
    summed = sum_at_owner(sum_at_owner(sum_at_owner(both, "gx", 0), "gy", 0), "gz", 0)
    return summed[:, :K], summed[:, K:]


def solution(mesh):
    return jax.shard_map(
        per_device,
        mesh=mesh,
        in_specs=(P("gx", "gy", "gz", None), P(None, "gx", "gy", "gz")),
        out_specs=(P(("gx", "gy", "gz"), None), P(("gx", "gy", "gz"), None)),
        check_vma=False,
    )
```

```python
import functools

import jax
import jax.numpy as jnp
import numpy as np
from jax import lax
from jax.experimental import pallas as pl
from jax.experimental.pallas import tpu as pltpu
from jax.sharding import PartitionSpec as P

MESH = pl.DeviceIdType.MESH
F32 = jnp.float32
BF16 = jnp.bfloat16
HIGH = lax.Precision.HIGHEST

SX, SY, SZ, K = 16, 8, 48, 512
PX, PY = SX + 2, SY + 2
HALF = PY // 2
CELLS = 64 * 128 * 96
DIM0 = (((0,), (0,)), ((), ()))
COLORS = ((0, 384), (384, 384), (768, 256))
ORDERS = ("xyz", "yzx", "zxy")


def constants():
    rows = HALF * SZ
    tz = np.zeros((rows, rows), np.float32)
    for r in range(rows):
        for c in (r - 1, r, r + 1):
            if 0 <= c < rows and c // SZ == r // SZ:
                tz[r, c] = 2.0 if c == r else 1.0
    sel = np.zeros((SX * SY, 256), np.float32)
    txy = np.zeros((SX * SY, 256), np.float32)
    for x in range(SX):
        for y in range(SY):
            row = x * SY + y
            sel[row, (x + 1) * PY + y + 1] = 1.0
            for dx in (-1, 0, 1):
                for dy in (-1, 0, 1):
                    txy[row, (x + 1 + dx) * PY + y + 1 + dy] = (2 - abs(dx)) * (2 - abs(dy))
    places = {}
    for x in range(SX):
        for y in range(SY):
            places[(x, y)] = x * SY + y
    for x in range(SX):
        places[(x, SY)] = 128 + x
        places[(x, -1)] = 144 + x
    for y in range(SY):
        places[(SX, y)] = 160 + y
        places[(-1, y)] = 176 + y
    places[(SX, SY)] = 192
    places[(SX, -1)] = 208 + 7
    places[(-1, SY)] = 224
    places[(-1, -1)] = 240 + 7
    t2 = np.zeros((128, 256), np.float32)
    t4 = np.zeros((128, 256), np.float32)
    for x in range(SX):
        for y in range(SY):
            for dx in (-1, 0, 1):
                for dy in (-1, 0, 1):
                    place = places[(x + dx, y + dy)]
                    t2[x * SY + y, place] = (2 - abs(dx)) * (2 - abs(dy))
                    t4[x * SY + y, place] = (4 - 3 * abs(dx)) * (4 - 3 * abs(dy))
    pick = np.zeros((64, 128), np.float32)
    for x in range(SX):
        pick[x, x * SY] = 1.0
        pick[16 + x, x * SY + 7] = 1.0
    for y in range(SY):
        pick[32 + y, y] = 1.0
        pick[48 + y, 15 * SY + y] = 1.0
    return tz, sel, txy, t2, t4, np.ascontiguousarray(t2.T), pick


def local_kernel(
    v_hbm, mat, tz_ref, sel_ref, txy_ref, t2_ref, t4_ref, t2t_ref, pick_ref, stiff_out, mass_out,
    vp, az, bz, ya, yb, xbuf, vt, coef, acc, zf, zs, zh, zface,
    own_sem, up_send, dn_send, up_recv, dn_recv, side_send, side_recv, z_send, z_recv,
    sym, core_in, *ring,
):
    core_send, core_recv, ring_send, ring_recv = ring[-4:]
    ring = ring[:-4]
    gx, gy, gz = lax.axis_index("gx"), lax.axis_index("gy"), lax.axis_index("gz")
    other = 1 - gz

    def at(dx, dy, z):
        return {"gx": lax.rem(gx + dx + 4, 4), "gy": lax.rem(gy + dy + 16, 16), "gz": z}

    around = [(dx, dy) for dx in (-1, 0, 1) for dy in (-1, 0, 1)]
    barrier = pltpu.get_barrier_semaphore()
    for dx, dy in around:
        if (dx, dy) != (0, 0):
            pl.semaphore_signal(barrier, inc=1, device_id=at(dx, dy, gz), device_id_type=MESH)
        pl.semaphore_signal(barrier, inc=1, device_id=at(dx, dy, other), device_id_type=MESH)

    core, z_lo = lax.rem(gx, 2), lax.div(gx, 2)
    ring_x, ring_y = lax.div(gy, 4), lax.rem(gy, 4)
    ring_z = 2 * gz + z_lo
    partner = {"gx": gx + 1 - 2 * core, "gy": gy, "gz": gz}

    def ring_place(dim, k):
        mine = {"x": ring_x, "y": ring_y, "z": ring_z}[dim]
        return lax.rem(mine + k, 4)

    def ring_peer(dim, k):
        spot = ring_place(dim, k)
        if dim == "x":
            return {"gx": gx, "gy": 4 * spot + ring_y, "gz": gz}
        if dim == "y":
            return {"gx": gx, "gy": 4 * ring_x + spot, "gz": gz}
        return {"gx": 2 * lax.rem(spot, 2) + core, "gy": gy, "gz": lax.div(spot, 2)}

    pl.semaphore_signal(barrier, inc=1, device_id=partner, device_id_type=MESH)
    for dim in "xyz":
        for k in (1, 2, 3):
            pl.semaphore_signal(barrier, inc=1, device_id=ring_peer(dim, k), device_id_type=MESH)

    def own_copy(x):
        return pltpu.make_async_copy(v_hbm.at[x], vp.at[x + 1, pl.ds(1, SY)], own_sem.at[x])

    @pl.loop(0, SX)
    def _(x):
        own_copy(x).start()

    def has(dx, dy):
        ok = jnp.bool_(True)
        if dx == 1:
            ok = jnp.logical_and(ok, gx < 3)
        if dx == -1:
            ok = jnp.logical_and(ok, gx > 0)
        if dy == 1:
            ok = jnp.logical_and(ok, gy < 15)
        if dy == -1:
            ok = jnp.logical_and(ok, gy > 0)
        return ok

    def remote(src, dst, send, recv, where):
        return pltpu.make_async_remote_copy(
            src_ref=src, dst_ref=dst, send_sem=send, recv_sem=recv, device_id=where, device_id_type=MESH
        )

    def up(x):
        return remote(v_hbm.at[x, SY - 1], vp.at[x + 1, 0], up_send.at[x], up_recv.at[x], at(0, 1, gz))

    def down(x):
        return remote(v_hbm.at[x, 0], vp.at[x + 1, PY - 1], dn_send.at[x], dn_recv.at[x], at(0, -1, gz))

    def side(index):
        dx, dy = sides[index]
        src_x = SX - 1 if dx == 1 else 0
        dst_x = 0 if dx == 1 else PX - 1
        if dy == 0:
            src, dst = v_hbm.at[src_x], vp.at[dst_x, pl.ds(1, SY)]
        elif dy == 1:
            src, dst = v_hbm.at[src_x, SY - 1], vp.at[dst_x, 0]
        else:
            src, dst = v_hbm.at[src_x, 0], vp.at[dst_x, PY - 1]
        return remote(src, dst, side_send.at[index], side_recv.at[index], at(dx, dy, gz))

    sides = [(1, 0), (1, 1), (1, -1), (-1, 0), (-1, 1), (-1, -1)]

    @pl.when(jnp.logical_not(has(0, -1)))
    def _():
        vp[:, 0] = jnp.zeros((PX, SZ, K), BF16)

    @pl.when(jnp.logical_not(has(0, 1)))
    def _():
        vp[:, PY - 1] = jnp.zeros((PX, SZ, K), BF16)

    @pl.when(jnp.logical_not(has(-1, 0)))
    def _():
        vp[0] = jnp.zeros((PY, SZ, K), BF16)

    @pl.when(jnp.logical_not(has(1, 0)))
    def _():
        vp[PX - 1] = jnp.zeros((PY, SZ, K), BF16)

    zrows = [(0, 0, 0, 128)]
    zrows += [(0, 1, 128, 16), (0, -1, 144, 16), (1, 0, 160, 16), (-1, 0, 176, 16)]
    zrows += [(1, 1, 192, 16), (1, -1, 208, 16), (-1, 1, 224, 16), (-1, -1, 240, 16)]
    for dx, dy, first, count in zrows[1:]:

        @pl.when(jnp.logical_not(has(dx, dy)))
        def _():
            zh[pl.ds(first, count)] = jnp.zeros((count, K), BF16)

    pl.semaphore_wait(barrier, 27)

    @pl.when(has(1, 0))
    def _():
        side(0).start()

    @pl.when(has(-1, 0))
    def _():
        side(3).start()

    for index in (1, 2, 4, 5):

        @pl.when(has(*sides[index]))
        def _():
            side(index).start()

    @pl.loop(0, SX)
    def _(x):
        @pl.when(has(0, 1))
        def _():
            up(x).start()

        @pl.when(has(0, -1))
        def _():
            down(x).start()

    kappa = mat[0].reshape(SX * SY, SZ)
    rho = mat[1].reshape(SX * SY, SZ)
    own_kappa = lax.dot_general(kappa, sel_ref[...], DIM0, precision=HIGH, preferred_element_type=F32)
    own_rho = lax.dot_general(rho, sel_ref[...], DIM0, precision=HIGH, preferred_element_type=F32)
    near = lax.dot_general(kappa, txy_ref[...], DIM0, precision=HIGH, preferred_element_type=F32)
    edge_row = jnp.zeros((1, 256), F32)
    near = (
        jnp.concatenate([edge_row, near[:-1]], axis=0)
        + 2.0 * near
        + jnp.concatenate([near[1:], edge_row], axis=0)
    )
    alpha = 2.0 * own_kappa + near * (1.0 / 32.0)
    beta = own_kappa * (1.0 / 16.0)
    for xp in range(PX):
        span = slice(xp * PY, xp * PY + PY)
        coef[xp, 0, :, 0:PY] = alpha[:, span]
        coef[xp, 1, :, 0:PY] = beta[:, span]
        coef[xp, 2, :, 0:PY] = own_rho[:, span]

    @pl.loop(0, SX)
    def _(x):
        own_copy(x).wait()
        low = vp[x + 1, 1 : 1 + SY, 0:16, :].astype(F32)
        high = vp[x + 1, 1 : 1 + SY, SZ - 16 : SZ, :].astype(F32)
        spot = lax.broadcasted_iota(jnp.int32, (1, 16, 1), 1)
        low = jnp.sum(jnp.where(spot == 0, low, 0.0), axis=1)
        high = jnp.sum(jnp.where(spot == 15, high, 0.0), axis=1)
        zf[pl.ds(pl.multiple_of(x * SY, SY), SY)] = jnp.where(gz == 0, high, low)

    zface[...] = zf[...].astype(BF16)
    zs[...] = jnp.dot(pick_ref[...], zface[...], preferred_element_type=F32).astype(BF16)

    def zcopy(index, dx, dy):
        first, count = zrows[index][2:]
        if (dx, dy) == (0, 0):
            src = zface
        elif dx == 0:
            src = zs.at[pl.ds(16 if dy == 1 else 0, 16)]
        else:
            src = zs.at[pl.ds(48 if dx == 1 else 32, 16)]
        return remote(
            src, zh.at[pl.ds(first, count)], z_send.at[index], z_recv.at[index], at(dx, dy, other)
        )

    for index, (dx, dy, _, _) in enumerate(zrows):

        @pl.when(has(-dx, -dy))
        def _():
            zcopy(index, -dx, -dy).start()

    acc[...] = jnp.zeros_like(acc)

    def wait_plane(xp):
        @pl.when(jnp.logical_and(xp >= 1, xp <= SX))
        def _():
            @pl.when(has(0, -1))
            def _():
                up(xp - 1).wait_recv()

            @pl.when(has(0, 1))
            def _():
                down(xp - 1).wait_recv()

        @pl.when(xp == 0)
        def _():
            for index in (0, 1, 2):
                dx, dy = sides[index]

                @pl.when(has(-dx, -dy))
                def _():
                    side(index).wait_recv()

        @pl.when(xp == PX - 1)
        def _():
            for index in (3, 4, 5):
                dx, dy = sides[index]

                @pl.when(has(-dx, -dy))
                def _():
                    side(index).wait_recv()

    def plane_stage(xp, slot):
        wait_plane(xp)
        for b in range(2):
            for c in range(2):
                lanes = slice(256 * c, 256 * c + 256)
                own = vp[xp, HALF * b : HALF * b + HALF, :, lanes]
                a = jnp.dot(
                    tz_ref[...], own.reshape(HALF * SZ, 256), preferred_element_type=F32
                ).astype(BF16).reshape(HALF, SZ, 256)
                az[HALF * b : HALF * b + HALF, :, lanes] = a
                bz[HALF * b : HALF * b + HALF, :, lanes] = a + (own + own)
        for y in range(SY):
            mid = az[y + 1]
            ya[slot, y] = (az[y] + az[y + 2]) + (mid + mid)
            mid = bz[y + 1]
            yb[slot, y] = (bz[y] + bz[y + 2]) + BF16(4.0) * mid

    def cell_stage(x):
        s0, s1, s2 = lax.rem(x, 3), lax.rem(x + 1, 3), lax.rem(x + 2, 3)
        for y in range(SY):
            al = coef[x + 1, 0, :, y + 1 : y + 2]
            be = coef[x + 1, 1, :, y + 1 : y + 2]
            ro = coef[x + 1, 2, :, y + 1 : y + 2]
            mid = ya[s1, y]
            u = (ya[s0, y] + ya[s2, y]) + (mid + mid)
            mid = yb[s1, y]
            m = (yb[s0, y] + yb[s2, y]) + BF16(4.0) * mid
            own = vp[x + 1, y + 1].astype(F32)
            xbuf[pl.ds(y * SZ, SZ), 0:K] = (al * own - be * u.astype(F32)).astype(BF16)
            xbuf[pl.ds(y * SZ, SZ), K : 2 * K] = (ro * m.astype(F32)).astype(BF16)
        vt[...] = vp[x + 1, 1 : 1 + SY].reshape(SY * SZ, K).T
        for c in range(4):
            lanes = slice(256 * c, 256 * c + 256)
            acc[:, lanes] += jnp.dot(vt[...], xbuf[:, lanes], preferred_element_type=F32)

    plane_stage(jnp.int32(0), jnp.int32(0))
    plane_stage(jnp.int32(1), jnp.int32(1))

    @pl.loop(0, SX)
    def _(x):
        plane_stage(x + 2, lax.rem(x + 2, 3))
        cell_stage(x)

    def halo_rows(xp, yp):
        return coef[xp, 0, :, yp : yp + 1] * vp[xp, yp].astype(F32)

    for xp in (0, PX - 1):
        for y in range(SY):
            xbuf[y * SZ : y * SZ + SZ, 0:K] = halo_rows(xp, y + 1).astype(BF16)
        vt[...] = vp[xp, 1 : 1 + SY].reshape(SY * SZ, K).T
        for c in range(2):
            lanes = slice(256 * c, 256 * c + 256)
            acc[:, lanes] += jnp.dot(vt[...], xbuf[:, lanes], preferred_element_type=F32)
    for yp in (0, PY - 1):
        @pl.loop(0, 3)
        def _(part):
            for i in range(6):
                xbuf[i * SZ : i * SZ + SZ, 0:K] = halo_rows(part * 6 + i, yp).astype(BF16)
            turned = vp[pl.ds(part * 6, 6), yp].reshape(6 * SZ, K).T
            for c in range(2):
                lanes = slice(256 * c, 256 * c + 256)
                acc[:, lanes] += jnp.dot(turned, xbuf[0 : 6 * SZ, lanes], preferred_element_type=F32)

    for index, (dx, dy, _, _) in enumerate(zrows):

        @pl.when(has(dx, dy))
        def _():
            zcopy(index, -dx, -dy).wait_recv()

    lane = lax.broadcasted_iota(jnp.int32, (SX * SY, SZ), 1)
    at_edge = lane == jnp.where(gz == 0, SZ - 1, 0)
    kappa_edge = jnp.sum(jnp.where(at_edge, kappa, 0.0), axis=1, keepdims=True)
    rho_edge = jnp.sum(jnp.where(at_edge, rho, 0.0), axis=1, keepdims=True)
    far = zh[...]
    du = jnp.dot(t2_ref[...], far, preferred_element_type=F32)
    dm = jnp.dot(t4_ref[...], far, preferred_element_type=F32)
    xbuf[0:128, 0:K] = (kappa_edge * (-1.0 / 16.0) * du).astype(BF16)
    xbuf[0:128, K : 2 * K] = (rho_edge * dm).astype(BF16)
    turned = zface[...].T
    for c in range(4):
        lanes = slice(256 * c, 256 * c + 256)
        acc[:, lanes] += jnp.dot(turned, xbuf[0:128, lanes], preferred_element_type=F32)
    reach = jnp.dot(
        t2t_ref[...], jnp.broadcast_to(kappa_edge, (128, 128)), precision=HIGH, preferred_element_type=F32
    ) * (1.0 / 32.0)
    for c in range(4):
        lanes = slice(128 * c, 128 * c + 128)
        xbuf[0:256, lanes] = (reach * far[:, lanes].astype(F32)).astype(BF16)
    turned = far.T
    for c in range(2):
        lanes = slice(256 * c, 256 * c + 256)
        acc[:, lanes] += jnp.dot(turned, xbuf[0:256, lanes], preferred_element_type=F32)

    def core_copy(c):
        first, width = COLORS[c]
        cols = pl.ds(first, width)
        return remote(
            sym.at[1 - core, :, :, :, :, :, cols], core_in.at[:, :, :, :, :, cols],
            core_send.at[c], core_recv.at[c], partner,
        )

    def put(gx_row, col, block):
        for part in range(32):
            sym[
                gx_row % 2, gx_row // 2, part // 8, part // 2 % 4, part % 2, :, col : col + 128
            ] = block[4 * part : 4 * part + 4]

    for half, scale in ((0, 0.5 / CELLS), (1, 0.5 / (216.0 * CELLS))):
        for i in range(4):
            for j in range(i, 4):
                rows = slice(128 * i, 128 * i + 128)
                cols = slice(128 * j, 128 * j + 128)
                there = slice(K * half + 128 * j, K * half + 128 * j + 128)
                back = slice(K * half + 128 * i, K * half + 128 * i + 128)
                both = (acc[rows, there] + acc[cols, back].T) * scale
                put(i, K * half + 128 * j, both)
                if i != j:
                    put(j, K * half + 128 * i, both.T)
        if half == 0:
            core_copy(0).start()
        else:
            core_copy(1).start()
            core_copy(2).start()

    held = [[ring[6 * c + 2 * s] for s in range(3)] for c in range(3)]
    landed = [[ring[6 * c + 2 * s + 1] for s in range(3)] for c in range(3)]

    def piece(c, s, spot):
        ref, dim, left = held[c][s], ORDERS[c][s], ORDERS[c][s:]
        index = []
        for name in ("z_lo", "x", "y", "z_hi"):
            if name[0] not in left:
                continue
            if name[0] != dim:
                index.append(slice(None))
            elif name == "z_lo":
                index.append(lax.rem(spot, 2))
            elif name == "z_hi":
                index.append(lax.div(spot, 2))
            else:
                index.append(spot)
        return ref.at[tuple(index)]

    def ring_copy(c, s, k):
        dim = ORDERS[c][s]
        number = 9 * c + 3 * s + k - 1
        return remote(
            piece(c, s, ring_place(dim, k)), landed[c][s].at[k - 1],
            ring_send.at[number], ring_recv.at[number], ring_peer(dim, k),
        )

    for c in range(3):
        first, width = COLORS[c]
        cols = slice(first, first + width)
        core_copy(c).wait_recv()
        for zl in range(2):
            for x in range(4):
                held[c][0][zl, x] = sym[core, zl, x, :, :, :, cols] + core_in[zl, x, :, :, :, cols]
        for k in (2, 1, 3):
            ring_copy(c, 0, k).start()
    for s in range(3):
        for c in range(3):
            first, width = COLORS[c]
            for k in (1, 3, 2):
                ring_copy(c, s, k).wait_recv()
            total = piece(c, s, ring_place(ORDERS[c][s], 0))[...]
            for k in (1, 3, 2):
                total = total + landed[c][s][k - 1]
            if s < 2:
                held[c][s + 1][...] = total
                for k in (2, 1, 3):
                    ring_copy(c, s + 1, k).start()
            else:
                for tile in range(width // 128):
                    col = first + 128 * tile
                    part = total[:, 128 * tile : 128 * tile + 128]
                    if col < K:
                        stiff_out[:, col : col + 128] = part
                    else:
                        mass_out[:, col - K : col - K + 128] = part
    for c in range(3):
        core_copy(c).wait_send()
        for s in range(3):
            for k in (1, 2, 3):
                ring_copy(c, s, k).wait_send()

    @pl.loop(0, SX)
    def _(x):
        @pl.when(has(0, 1))
        def _():
            up(x).wait_send()

        @pl.when(has(0, -1))
        def _():
            down(x).wait_send()

    for index in range(6):

        @pl.when(has(*sides[index]))
        def _():
            side(index).wait_send()

    for index, (dx, dy, _, _) in enumerate(zrows):

        @pl.when(has(-dx, -dy))
        def _():
            zcopy(index, -dx, -dy).wait_send()


def ring_buffers():
    buffers = []
    for (_, width), order in zip(COLORS, ORDERS):
        for s in range(3):
            left = [n for d, n in (("z", 2), ("x", 4), ("y", 4), ("z", 2)) if d in order[s:]]
            after = [n for d, n in (("z", 2), ("x", 4), ("y", 4), ("z", 2)) if d in order[s + 1 :]]
            buffers.append(pltpu.VMEM((*left, 4, width), F32))
            buffers.append(pltpu.VMEM((3, *after, 4, width), F32))
    return buffers


def local_products(eigvecs, material):
    tz, sel, txy, t2, t4, t2t, pick = constants()
    small = (
        jnp.asarray(tz, BF16), jnp.asarray(sel), jnp.asarray(txy), jnp.asarray(t2, BF16),
        jnp.asarray(t4, BF16), jnp.asarray(t2t), jnp.asarray(pick, BF16),
    )
    vmem = pl.BlockSpec(memory_space=pltpu.VMEM)
    dma = pltpu.SemaphoreType.DMA
    return pl.pallas_call(
        local_kernel,
        out_shape=[jax.ShapeDtypeStruct((4, K), F32)] * 2,
        in_specs=[pl.BlockSpec(memory_space=pl.ANY)] + [vmem] * 8,
        out_specs=[vmem, vmem],
        scratch_shapes=[
            pltpu.VMEM((PX, PY, SZ, K), BF16),
            pltpu.VMEM((PY, SZ, K), BF16),
            pltpu.VMEM((PY, SZ, K), BF16),
            pltpu.VMEM((3, SY, SZ, K), BF16),
            pltpu.VMEM((3, SY, SZ, K), BF16),
            pltpu.VMEM((SY * SZ, 2 * K), BF16),
            pltpu.VMEM((K, SY * SZ), BF16),
            pltpu.VMEM((PX, 3, SZ, 128), F32),
            pltpu.VMEM((K, 2 * K), F32),
            pltpu.VMEM((SX * SY, K), F32),
            pltpu.VMEM((64, K), BF16),
            pltpu.VMEM((256, K), BF16),
            pltpu.VMEM((SX * SY, K), BF16),
            dma((SX,)), dma((SX,)), dma((SX,)), dma((SX,)), dma((SX,)),
            dma((6,)), dma((6,)), dma((9,)), dma((9,)),
            pltpu.VMEM((2, 2, 4, 4, 2, 4, 2 * K), F32),
            pltpu.VMEM((2, 4, 4, 2, 4, 2 * K), F32),
            *ring_buffers(),
            dma((3,)), dma((3,)), dma((27,)), dma((27,)),
        ],
        compiler_params=pltpu.CompilerParams(
            collective_id=0, has_side_effects=True, vmem_limit_bytes=60 * 1024 * 1024
        ),
    )(eigvecs, material, *small)


def per_device(eigvecs, material):
    return tuple(local_products(eigvecs, material))


def solution(mesh):
    return jax.shard_map(
        per_device,
        mesh=mesh,
        in_specs=(P("gx", "gy", "gz", None), P(None, "gx", "gy", "gz")),
        out_specs=(P(("gx", "gy", "gz"), None), P(("gx", "gy", "gz"), None)),
        check_vma=False,
    )
```

```python
import functools

import jax
import jax.numpy as jnp
import numpy as np
from jax import lax
from jax.experimental import pallas as pl
from jax.experimental.pallas import tpu as pltpu
from jax.sharding import PartitionSpec as P

MESH = pl.DeviceIdType.MESH
F32 = jnp.float32
BF16 = jnp.bfloat16
HIGH = lax.Precision.HIGHEST

SX, SY, SZ, K = 16, 8, 48, 512
PX, PY = SX + 2, SY + 2
HALF = PY // 2
PAIR_ROWS = 2 * SY * SZ + 4 * SZ
CELLS = 64 * 128 * 96
DIM0 = (((0,), (0,)), ((), ()))
COLORS = ((0, 384), (384, 384), (768, 256))
ORDERS = ("xyz", "yzx", "zxy")


def constants():
    rows = HALF * SZ
    tz = np.zeros((rows, rows), np.float32)
    for r in range(rows):
        for c in (r - 1, r, r + 1):
            if 0 <= c < rows and c // SZ == r // SZ:
                tz[r, c] = 2.0 if c == r else 1.0
    sel = np.zeros((SX * SY, 256), np.float32)
    txy = np.zeros((SX * SY, 256), np.float32)
    for x in range(SX):
        for y in range(SY):
            row = x * SY + y
            sel[row, (x + 1) * PY + y + 1] = 1.0
            for dx in (-1, 0, 1):
                for dy in (-1, 0, 1):
                    txy[row, (x + 1 + dx) * PY + y + 1 + dy] = (2 - abs(dx)) * (2 - abs(dy))
    places = {}
    for x in range(SX):
        for y in range(SY):
            places[(x, y)] = x * SY + y
    for x in range(SX):
        places[(x, SY)] = 128 + x
        places[(x, -1)] = 144 + x
    for y in range(SY):
        places[(SX, y)] = 160 + y
        places[(-1, y)] = 176 + y
    places[(SX, SY)] = 192
    places[(SX, -1)] = 208 + 7
    places[(-1, SY)] = 224
    places[(-1, -1)] = 240 + 7
    t2 = np.zeros((128, 256), np.float32)
    t4 = np.zeros((128, 256), np.float32)
    for x in range(SX):
        for y in range(SY):
            for dx in (-1, 0, 1):
                for dy in (-1, 0, 1):
                    place = places[(x + dx, y + dy)]
                    t2[x * SY + y, place] = (2 - abs(dx)) * (2 - abs(dy))
                    t4[x * SY + y, place] = (4 - 3 * abs(dx)) * (4 - 3 * abs(dy))
    pick = np.zeros((64, 128), np.float32)
    for x in range(SX):
        pick[x, x * SY] = 1.0
        pick[16 + x, x * SY + 7] = 1.0
    for y in range(SY):
        pick[32 + y, y] = 1.0
        pick[48 + y, 15 * SY + y] = 1.0
    return tz, sel, txy, t2, t4, np.ascontiguousarray(t2.T), pick


def local_kernel(
    v_hbm, mat, tz_ref, sel_ref, txy_ref, t2_ref, t4_ref, t2t_ref, pick_ref, stiff_out, mass_out,
    vp, az, bz, ya, yb, xbufs, vts, xbuf, vt, coef, acc, zf, zs, zh, zface,
    own_sem, up_send, dn_send, up_recv, dn_recv, side_send, side_recv, z_send, z_recv,
    sym, core_in, *ring,
):
    core_send, core_recv, ring_send, ring_recv = ring[-4:]
    ring = ring[:-4]
    gx, gy, gz = lax.axis_index("gx"), lax.axis_index("gy"), lax.axis_index("gz")
    other = 1 - gz

    def at(dx, dy, z):
        return {"gx": lax.rem(gx + dx + 4, 4), "gy": lax.rem(gy + dy + 16, 16), "gz": z}

    around = [(dx, dy) for dx in (-1, 0, 1) for dy in (-1, 0, 1)]
    barrier = pltpu.get_barrier_semaphore()
    for dx, dy in around:
        if (dx, dy) != (0, 0):
            pl.semaphore_signal(barrier, inc=1, device_id=at(dx, dy, gz), device_id_type=MESH)
        pl.semaphore_signal(barrier, inc=1, device_id=at(dx, dy, other), device_id_type=MESH)

    core, z_lo = lax.rem(gx, 2), lax.div(gx, 2)
    ring_x, ring_y = lax.div(gy, 4), lax.rem(gy, 4)
    ring_z = 2 * gz + z_lo
    partner = {"gx": gx + 1 - 2 * core, "gy": gy, "gz": gz}

    def ring_place(dim, k):
        mine = {"x": ring_x, "y": ring_y, "z": ring_z}[dim]
        return lax.rem(mine + k, 4)

    def ring_peer(dim, k):
        spot = ring_place(dim, k)
        if dim == "x":
            return {"gx": gx, "gy": 4 * spot + ring_y, "gz": gz}
        if dim == "y":
            return {"gx": gx, "gy": 4 * ring_x + spot, "gz": gz}
        return {"gx": 2 * lax.rem(spot, 2) + core, "gy": gy, "gz": lax.div(spot, 2)}

    pl.semaphore_signal(barrier, inc=1, device_id=partner, device_id_type=MESH)
    for dim in "xyz":
        for k in (1, 2, 3):
            pl.semaphore_signal(barrier, inc=1, device_id=ring_peer(dim, k), device_id_type=MESH)

    def own_copy(x):
        return pltpu.make_async_copy(v_hbm.at[x], vp.at[x + 1, pl.ds(1, SY)], own_sem.at[x])

    @pl.loop(0, SX)
    def _(x):
        own_copy(x).start()

    def has(dx, dy):
        ok = jnp.bool_(True)
        if dx == 1:
            ok = jnp.logical_and(ok, gx < 3)
        if dx == -1:
            ok = jnp.logical_and(ok, gx > 0)
        if dy == 1:
            ok = jnp.logical_and(ok, gy < 15)
        if dy == -1:
            ok = jnp.logical_and(ok, gy > 0)
        return ok

    def remote(src, dst, send, recv, where):
        return pltpu.make_async_remote_copy(
            src_ref=src, dst_ref=dst, send_sem=send, recv_sem=recv, device_id=where, device_id_type=MESH
        )

    def up(x):
        return remote(v_hbm.at[x, SY - 1], vp.at[x + 1, 0], up_send.at[x], up_recv.at[x], at(0, 1, gz))

    def down(x):
        return remote(v_hbm.at[x, 0], vp.at[x + 1, PY - 1], dn_send.at[x], dn_recv.at[x], at(0, -1, gz))

    def side(index):
        dx, dy = sides[index]
        src_x = SX - 1 if dx == 1 else 0
        dst_x = 0 if dx == 1 else PX - 1
        if dy == 0:
            src, dst = v_hbm.at[src_x], vp.at[dst_x, pl.ds(1, SY)]
        elif dy == 1:
            src, dst = v_hbm.at[src_x, SY - 1], vp.at[dst_x, 0]
        else:
            src, dst = v_hbm.at[src_x, 0], vp.at[dst_x, PY - 1]
        return remote(src, dst, side_send.at[index], side_recv.at[index], at(dx, dy, gz))

    sides = [(1, 0), (1, 1), (1, -1), (-1, 0), (-1, 1), (-1, -1)]

    @pl.when(jnp.logical_not(has(0, -1)))
    def _():
        vp[:, 0] = jnp.zeros((PX, SZ, K), BF16)

    @pl.when(jnp.logical_not(has(0, 1)))
    def _():
        vp[:, PY - 1] = jnp.zeros((PX, SZ, K), BF16)

    @pl.when(jnp.logical_not(has(-1, 0)))
    def _():
        vp[0] = jnp.zeros((PY, SZ, K), BF16)

    @pl.when(jnp.logical_not(has(1, 0)))
    def _():
        vp[PX - 1] = jnp.zeros((PY, SZ, K), BF16)

    zrows = [(0, 0, 0, 128)]
    zrows += [(0, 1, 128, 16), (0, -1, 144, 16), (1, 0, 160, 16), (-1, 0, 176, 16)]
    zrows += [(1, 1, 192, 16), (1, -1, 208, 16), (-1, 1, 224, 16), (-1, -1, 240, 16)]
    for dx, dy, first, count in zrows[1:]:

        @pl.when(jnp.logical_not(has(dx, dy)))
        def _():
            zh[pl.ds(first, count)] = jnp.zeros((count, K), BF16)

    pl.semaphore_wait(barrier, 27)

    @pl.when(has(1, 0))
    def _():
        side(0).start()

    @pl.when(has(-1, 0))
    def _():
        side(3).start()

    for index in (1, 2, 4, 5):

        @pl.when(has(*sides[index]))
        def _():
            side(index).start()

    @pl.loop(0, SX)
    def _(x):
        @pl.when(has(0, 1))
        def _():
            up(x).start()

        @pl.when(has(0, -1))
        def _():
            down(x).start()

    kappa = mat[0].reshape(SX * SY, SZ)
    rho = mat[1].reshape(SX * SY, SZ)
    own_kappa = lax.dot_general(kappa, sel_ref[...], DIM0, precision=HIGH, preferred_element_type=F32)
    own_rho = lax.dot_general(rho, sel_ref[...], DIM0, precision=HIGH, preferred_element_type=F32)
    near = lax.dot_general(kappa, txy_ref[...], DIM0, precision=HIGH, preferred_element_type=F32)
    edge_row = jnp.zeros((1, 256), F32)
    near = (
        jnp.concatenate([edge_row, near[:-1]], axis=0)
        + 2.0 * near
        + jnp.concatenate([near[1:], edge_row], axis=0)
    )
    alpha = 2.0 * own_kappa + near * (1.0 / 32.0)
    beta = own_kappa * (1.0 / 16.0)
    for xp in range(PX):
        span = slice(xp * PY, xp * PY + PY)
        coef[xp, 0, :, 0:PY] = alpha[:, span]
        coef[xp, 1, :, 0:PY] = beta[:, span]
        coef[xp, 2, :, 0:PY] = own_rho[:, span]

    @pl.loop(0, SX)
    def _(x):
        own_copy(x).wait()
        low = vp[x + 1, 1 : 1 + SY, 0:16, :].astype(F32)
        high = vp[x + 1, 1 : 1 + SY, SZ - 16 : SZ, :].astype(F32)
        spot = lax.broadcasted_iota(jnp.int32, (1, 16, 1), 1)
        low = jnp.sum(jnp.where(spot == 0, low, 0.0), axis=1)
        high = jnp.sum(jnp.where(spot == 15, high, 0.0), axis=1)
        zf[pl.ds(pl.multiple_of(x * SY, SY), SY)] = jnp.where(gz == 0, high, low)

    zface[...] = zf[...].astype(BF16)
    zs[...] = jnp.dot(pick_ref[...], zface[...], preferred_element_type=F32).astype(BF16)

    def zcopy(index, dx, dy):
        first, count = zrows[index][2:]
        if (dx, dy) == (0, 0):
            src = zface
        elif dx == 0:
            src = zs.at[pl.ds(16 if dy == 1 else 0, 16)]
        else:
            src = zs.at[pl.ds(48 if dx == 1 else 32, 16)]
        return remote(
            src, zh.at[pl.ds(first, count)], z_send.at[index], z_recv.at[index], at(dx, dy, other)
        )

    for index, (dx, dy, _, _) in enumerate(zrows):

        @pl.when(has(-dx, -dy))
        def _():
            zcopy(index, -dx, -dy).start()

    acc[...] = jnp.zeros_like(acc)

    def wait_plane(xp):
        @pl.when(jnp.logical_and(xp >= 1, xp <= SX))
        def _():
            @pl.when(has(0, -1))
            def _():
                up(xp - 1).wait_recv()

            @pl.when(has(0, 1))
            def _():
                down(xp - 1).wait_recv()

        @pl.when(xp == 0)
        def _():
            for index in (0, 1, 2):
                dx, dy = sides[index]

                @pl.when(has(-dx, -dy))
                def _():
                    side(index).wait_recv()

        @pl.when(xp == PX - 1)
        def _():
            for index in (3, 4, 5):
                dx, dy = sides[index]

                @pl.when(has(-dx, -dy))
                def _():
                    side(index).wait_recv()

    def plane_stage(xp, slot):
        for b in range(2):
            for c in range(2):
                lanes = slice(256 * c, 256 * c + 256)
                own = vp[xp, HALF * b : HALF * b + HALF, :, lanes]
                a = jnp.dot(
                    tz_ref[...], own.reshape(HALF * SZ, 256), preferred_element_type=F32
                ).astype(BF16).reshape(HALF, SZ, 256)
                az[slot % 2][HALF * b : HALF * b + HALF, :, lanes] = a
                bz[slot % 2][HALF * b : HALF * b + HALF, :, lanes] = a + (own + own)
        for c in range(2):
            lanes = slice(256 * c, 256 * c + 256)
            a, b = az[slot % 2], bz[slot % 2]
            pair = a[0, :, lanes] + a[1, :, lanes]
            for y in range(SY):
                nxt = a[y + 1, :, lanes] + a[y + 2, :, lanes]
                ya[slot][y, :, lanes] = pair + nxt
                pair = nxt
                yb[slot][y, :, lanes] = (b[y, :, lanes] + b[y + 2, :, lanes]) + BF16(4.0) * b[y + 1, :, lanes]

    def cell_pair(x, slot, side_by):
        x_out, v_out = xbufs[side_by], vts[side_by]
        slots = [(slot + i) % 4 for i in range(4)]
        for y in range(SY):
            cols = [
                [coef[x + 1 + i, n, :, y + 1 : y + 2] for n in range(3)] for i in range(2)
            ]
            for c in range(2):
                lanes = slice(256 * c, 256 * c + 256)
                stage = [ya[n][y, :, lanes] for n in slots]
                sums = [stage[i] + stage[i + 1] for i in range(3)]
                other_stage = [yb[n][y, :, lanes] for n in slots]
                for i in range(2):
                    al, be, ro = cols[i]
                    row = pl.ds(SY * SZ * i + y * SZ, SZ)
                    u = (sums[i] + sums[i + 1]).astype(F32)
                    own = vp[x + 1 + i, y + 1, :, lanes].astype(F32)
                    x_out[row, 256 * c : 256 * c + 256] = (al * own - be * u).astype(BF16)
                    m = (other_stage[i] + other_stage[i + 2]) + BF16(4.0) * other_stage[i + 1]
                    x_out[row, K + 256 * c : K + 256 * c + 256] = (ro * m.astype(F32)).astype(BF16)
        for i in range(2):
            for n, yp in enumerate((0, PY - 1)):
                row = pl.ds(2 * SY * SZ + (2 * i + n) * SZ, SZ)
                x_out[row, 0:K] = halo_rows(x + 1 + i, yp).astype(BF16)
        for i in range(2):
            v_out[:, SY * SZ * i : SY * SZ * i + SY * SZ] = (
                vp[x + 1 + i, 1 : 1 + SY].reshape(SY * SZ, K).T
            )
        sides_of = jnp.concatenate([vp[x + 1 + i, yp] for i in range(2) for yp in (0, PY - 1)], axis=0)
        v_out[:, 2 * SY * SZ : 2 * SY * SZ + 4 * SZ] = sides_of.T

    def gram_pair(side_by):
        x_in, v_in = xbufs[side_by], vts[side_by]
        for c in range(4):
            lanes = slice(256 * c, 256 * c + 256)
            depth = PAIR_ROWS if c < 2 else 2 * SY * SZ
            acc[:, lanes] += jnp.dot(
                v_in[:, 0:depth], x_in[0:depth, lanes], preferred_element_type=F32
            )

    def halo_rows(xp, yp):
        return coef[xp, 0, :, yp : yp + 1] * vp[xp, yp].astype(F32)

    def side_products():
        for xp in (0, PX - 1):
            for y in range(PY):
                xbuf[y * SZ : y * SZ + SZ, 0:K] = halo_rows(xp, y).astype(BF16)
            vt[...] = vp[xp].reshape(PY * SZ, K).T
            for c in range(2):
                lanes = slice(256 * c, 256 * c + 256)
                acc[:, lanes] += jnp.dot(vt[...], xbuf[:, lanes], preferred_element_type=F32)
        for index, (dx, dy, _, _) in enumerate(zrows):

            @pl.when(has(dx, dy))
            def _():
                zcopy(index, -dx, -dy).wait_recv()

        lane = lax.broadcasted_iota(jnp.int32, (SX * SY, SZ), 1)
        at_edge = lane == jnp.where(gz == 0, SZ - 1, 0)
        kappa_edge = jnp.sum(
            jnp.where(at_edge, mat[0].reshape(SX * SY, SZ), 0.0), axis=1, keepdims=True
        )
        rho_edge = jnp.sum(
            jnp.where(at_edge, mat[1].reshape(SX * SY, SZ), 0.0), axis=1, keepdims=True
        )
        far = zh[...]
        du = jnp.dot(t2_ref[...], far, preferred_element_type=F32)
        dm = jnp.dot(t4_ref[...], far, preferred_element_type=F32)
        xbuf[0:128, 0:K] = (kappa_edge * (-1.0 / 16.0) * du).astype(BF16)
        xbuf[0:128, K : 2 * K] = (rho_edge * dm).astype(BF16)
        reach = jnp.dot(
            t2t_ref[...], jnp.broadcast_to(kappa_edge, (128, 128)), precision=HIGH, preferred_element_type=F32
        ) * (1.0 / 32.0)
        for c in range(4):
            lanes = slice(128 * c, 128 * c + 128)
            xbuf[128:384, lanes] = (reach * far[:, lanes].astype(F32)).astype(BF16)
        vt[:, 0:128] = zface[...].T
        vt[:, 128:384] = far.T
        for c in range(4):
            lanes = slice(256 * c, 256 * c + 256)
            depth = 384 if c < 2 else 128
            acc[:, lanes] += jnp.dot(vt[:, 0:depth], xbuf[0:depth, lanes], preferred_element_type=F32)

    for ref in (xbufs[1], vts[1]):
        ref[...] = jnp.zeros_like(ref)
    for n in range(4):
        wait_plane(jnp.int32(n))
        plane_stage(n, n)

    @pl.loop(0, 3)
    def _(t):
        x = 4 * t
        for half in range(2):
            for n in range(2):
                wait_plane(x + 2 * half + 4 + n)
            gram_pair(1 - half)
            cell_pair(x + 2 * half, 2 * half, half)
            for n in range(2):
                plane_stage(x + 2 * half + 4 + n, 2 * half + n)

        @pl.when(t == 1)
        def _():
            wait_plane(jnp.int32(PX - 1))
            side_products()

    wait_plane(jnp.int32(16))
    gram_pair(1)
    cell_pair(12, 0, 0)
    for n in range(2):
        plane_stage(16 + n, n)
    gram_pair(0)
    cell_pair(14, 2, 1)
    gram_pair(1)

    def core_copy(c):
        first, width = COLORS[c]
        cols = pl.ds(first, width)
        return remote(
            sym.at[1 - core, :, :, :, :, :, cols], core_in.at[:, :, :, :, :, cols],
            core_send.at[c], core_recv.at[c], partner,
        )

    def put(gx_row, col, block):
        for part in range(32):
            sym[
                gx_row % 2, gx_row // 2, part // 8, part // 2 % 4, part % 2, :, col : col + 128
            ] = block[4 * part : 4 * part + 4]

    for half, scale in ((0, 0.5 / CELLS), (1, 0.5 / (216.0 * CELLS))):
        for i in range(4):
            for j in range(i, 4):
                rows = slice(128 * i, 128 * i + 128)
                cols = slice(128 * j, 128 * j + 128)
                there = slice(K * half + 128 * j, K * half + 128 * j + 128)
                back = slice(K * half + 128 * i, K * half + 128 * i + 128)
                both = (acc[rows, there] + acc[cols, back].T) * scale
                put(i, K * half + 128 * j, both)
                if i != j:
                    put(j, K * half + 128 * i, both.T)
        if half == 0:
            core_copy(0).start()
        else:
            core_copy(1).start()
            core_copy(2).start()

    held = [[ring[6 * c + 2 * s] for s in range(3)] for c in range(3)]
    landed = [[ring[6 * c + 2 * s + 1] for s in range(3)] for c in range(3)]

    def piece(c, s, spot):
        ref, dim, left = held[c][s], ORDERS[c][s], ORDERS[c][s:]
        index = []
        for name in ("z_lo", "x", "y", "z_hi"):
            if name[0] not in left:
                continue
            if name[0] != dim:
                index.append(slice(None))
            elif name == "z_lo":
                index.append(lax.rem(spot, 2))
            elif name == "z_hi":
                index.append(lax.div(spot, 2))
            else:
                index.append(spot)
        return ref.at[tuple(index)]

    def ring_copy(c, s, k):
        dim = ORDERS[c][s]
        number = 9 * c + 3 * s + k - 1
        return remote(
            piece(c, s, ring_place(dim, k)), landed[c][s].at[k - 1],
            ring_send.at[number], ring_recv.at[number], ring_peer(dim, k),
        )

    for c in range(3):
        first, width = COLORS[c]
        cols = slice(first, first + width)
        core_copy(c).wait_recv()
        for zl in range(2):
            for x in range(4):
                held[c][0][zl, x] = sym[core, zl, x, :, :, :, cols] + core_in[zl, x, :, :, :, cols]
        for k in (2, 1, 3):
            ring_copy(c, 0, k).start()
    for s in range(3):
        for c in range(3):
            first, width = COLORS[c]
            for k in (1, 3, 2):
                ring_copy(c, s, k).wait_recv()
            total = piece(c, s, ring_place(ORDERS[c][s], 0))[...]
            for k in (1, 3, 2):
                total = total + landed[c][s][k - 1]
            if s < 2:
                held[c][s + 1][...] = total
                for k in (2, 1, 3):
                    ring_copy(c, s + 1, k).start()
            else:
                for tile in range(width // 128):
                    col = first + 128 * tile
                    part = total[:, 128 * tile : 128 * tile + 128]
                    if col < K:
                        stiff_out[:, col : col + 128] = part
                    else:
                        mass_out[:, col - K : col - K + 128] = part
    for c in range(3):
        core_copy(c).wait_send()
        for s in range(3):
            for k in (1, 2, 3):
                ring_copy(c, s, k).wait_send()

    @pl.loop(0, SX)
    def _(x):
        @pl.when(has(0, 1))
        def _():
            up(x).wait_send()

        @pl.when(has(0, -1))
        def _():
            down(x).wait_send()

    for index in range(6):

        @pl.when(has(*sides[index]))
        def _():
            side(index).wait_send()

    for index, (dx, dy, _, _) in enumerate(zrows):

        @pl.when(has(-dx, -dy))
        def _():
            zcopy(index, -dx, -dy).wait_send()


def ring_buffers():
    buffers = []
    for (_, width), order in zip(COLORS, ORDERS):
        for s in range(3):
            left = [n for d, n in (("z", 2), ("x", 4), ("y", 4), ("z", 2)) if d in order[s:]]
            after = [n for d, n in (("z", 2), ("x", 4), ("y", 4), ("z", 2)) if d in order[s + 1 :]]
            buffers.append(pltpu.VMEM((*left, 4, width), F32))
            buffers.append(pltpu.VMEM((3, *after, 4, width), F32))
    return buffers


def local_products(eigvecs, material):
    tz, sel, txy, t2, t4, t2t, pick = constants()
    small = (
        jnp.asarray(tz, BF16), jnp.asarray(sel), jnp.asarray(txy), jnp.asarray(t2, BF16),
        jnp.asarray(t4, BF16), jnp.asarray(t2t), jnp.asarray(pick, BF16),
    )
    vmem = pl.BlockSpec(memory_space=pltpu.VMEM)
    dma = pltpu.SemaphoreType.DMA
    return pl.pallas_call(
        local_kernel,
        out_shape=[jax.ShapeDtypeStruct((4, K), F32)] * 2,
        in_specs=[pl.BlockSpec(memory_space=pl.ANY)] + [vmem] * 8,
        out_specs=[vmem, vmem],
        scratch_shapes=[
            pltpu.VMEM((PX, PY, SZ, K), BF16),
            [pltpu.VMEM((PY, SZ, K), BF16)] * 2,
            [pltpu.VMEM((PY, SZ, K), BF16)] * 2,
            [pltpu.VMEM((SY, SZ, K), BF16)] * 4,
            [pltpu.VMEM((SY, SZ, K), BF16)] * 4,
            [pltpu.VMEM((PAIR_ROWS, 2 * K), BF16)] * 2,
            [pltpu.VMEM((K, PAIR_ROWS), BF16)] * 2,
            pltpu.VMEM((PY * SZ, 2 * K), BF16),
            pltpu.VMEM((K, PY * SZ), BF16),
            pltpu.VMEM((PX, 3, SZ, 128), F32),
            pltpu.VMEM((K, 2 * K), F32),
            pltpu.VMEM((SX * SY, K), F32),
            pltpu.VMEM((64, K), BF16),
            pltpu.VMEM((256, K), BF16),
            pltpu.VMEM((SX * SY, K), BF16),
            dma((SX,)), dma((SX,)), dma((SX,)), dma((SX,)), dma((SX,)),
            dma((6,)), dma((6,)), dma((9,)), dma((9,)),
            pltpu.VMEM((2, 2, 4, 4, 2, 4, 2 * K), F32),
            pltpu.VMEM((2, 4, 4, 2, 4, 2 * K), F32),
            *ring_buffers(),
            dma((3,)), dma((3,)), dma((27,)), dma((27,)),
        ],
        compiler_params=pltpu.CompilerParams(
            collective_id=0, has_side_effects=True, vmem_limit_bytes=60 * 1024 * 1024
        ),
    )(eigvecs, material, *small)


def per_device(eigvecs, material):
    return tuple(local_products(eigvecs, material))


def solution(mesh):
    return jax.shard_map(
        per_device,
        mesh=mesh,
        in_specs=(P("gx", "gy", "gz", None), P(None, "gx", "gy", "gz")),
        out_specs=(P(("gx", "gy", "gz"), None), P(("gx", "gy", "gz"), None)),
        check_vma=False,
    )
```

```python
import functools

import jax
import jax.numpy as jnp
import numpy as np
from jax import lax
from jax.experimental import pallas as pl
from jax.experimental.pallas import tpu as pltpu
from jax.sharding import PartitionSpec as P

MESH = pl.DeviceIdType.MESH
F32 = jnp.float32
BF16 = jnp.bfloat16
HIGH = lax.Precision.HIGHEST

SX, SY, SZ, K = 16, 8, 48, 512
PX, PY = SX + 2, SY + 2
HALF = PY // 2
PAIR_ROWS = 2 * SY * SZ + 4 * SZ
CELLS = 64 * 128 * 96
DIM0 = (((0,), (0,)), ((), ()))
COLORS = ((0, 384), (384, 384), (768, 256))
ORDERS = ("xyz", "yzx", "zxy")


def constants():
    rows = HALF * SZ
    tz = np.zeros((rows, rows), np.float32)
    for r in range(rows):
        for c in (r - 1, r, r + 1):
            if 0 <= c < rows and c // SZ == r // SZ:
                tz[r, c] = 2.0 if c == r else 1.0
    sel = np.zeros((SX * SY, 256), np.float32)
    txy = np.zeros((SX * SY, 256), np.float32)
    for x in range(SX):
        for y in range(SY):
            row = x * SY + y
            sel[row, (x + 1) * PY + y + 1] = 1.0
            for dx in (-1, 0, 1):
                for dy in (-1, 0, 1):
                    txy[row, (x + 1 + dx) * PY + y + 1 + dy] = (2 - abs(dx)) * (2 - abs(dy))
    places = {}
    for x in range(SX):
        for y in range(SY):
            places[(x, y)] = x * SY + y
    for x in range(SX):
        places[(x, SY)] = 128 + x
        places[(x, -1)] = 144 + x
    for y in range(SY):
        places[(SX, y)] = 160 + y
        places[(-1, y)] = 176 + y
    places[(SX, SY)] = 192
    places[(SX, -1)] = 208 + 7
    places[(-1, SY)] = 224
    places[(-1, -1)] = 240 + 7
    t2 = np.zeros((128, 256), np.float32)
    t4 = np.zeros((128, 256), np.float32)
    for x in range(SX):
        for y in range(SY):
            for dx in (-1, 0, 1):
                for dy in (-1, 0, 1):
                    place = places[(x + dx, y + dy)]
                    t2[x * SY + y, place] = (2 - abs(dx)) * (2 - abs(dy))
                    t4[x * SY + y, place] = (4 - 3 * abs(dx)) * (4 - 3 * abs(dy))
    pick = np.zeros((64, 128), np.float32)
    for x in range(SX):
        pick[x, x * SY] = 1.0
        pick[16 + x, x * SY + 7] = 1.0
    for y in range(SY):
        pick[32 + y, y] = 1.0
        pick[48 + y, 15 * SY + y] = 1.0
    return tz, sel, txy, t2, t4, np.ascontiguousarray(t2.T), pick


def local_kernel(
    v_hbm, mat, tz_ref, sel_ref, txy_ref, t2_ref, t4_ref, t2t_ref, pick_ref, out,
    vp, az, bz, ya, yb, xbufs, vts, xbuf, vt, coef, acc, zf, zs, zh, zface,
    own_sem, up_send, dn_send, up_recv, dn_recv, side_send, side_recv, z_send, z_recv,
    sym, core_in, *ring,
):
    core_send, core_recv, ring_send, ring_recv = ring[-4:]
    ring = ring[:-4]
    gx, gy, gz = lax.axis_index("gx"), lax.axis_index("gy"), lax.axis_index("gz")
    other = 1 - gz

    def at(dx, dy, z):
        return {"gx": lax.rem(gx + dx + 4, 4), "gy": lax.rem(gy + dy + 16, 16), "gz": z}

    around = [(dx, dy) for dx in (-1, 0, 1) for dy in (-1, 0, 1)]
    barrier = pltpu.get_barrier_semaphore()
    for dx, dy in around:
        if (dx, dy) != (0, 0):
            pl.semaphore_signal(barrier, inc=1, device_id=at(dx, dy, gz), device_id_type=MESH)
        pl.semaphore_signal(barrier, inc=1, device_id=at(dx, dy, other), device_id_type=MESH)

    core, z_lo = lax.rem(gx, 2), lax.div(gx, 2)
    ring_x, ring_y = lax.div(gy, 4), lax.rem(gy, 4)
    ring_z = 2 * gz + z_lo
    partner = {"gx": gx + 1 - 2 * core, "gy": gy, "gz": gz}

    def ring_place(dim, k):
        mine = {"x": ring_x, "y": ring_y, "z": ring_z}[dim]
        return lax.rem(mine + k, 4)

    def ring_peer(dim, k):
        spot = ring_place(dim, k)
        if dim == "x":
            return {"gx": gx, "gy": 4 * spot + ring_y, "gz": gz}
        if dim == "y":
            return {"gx": gx, "gy": 4 * ring_x + spot, "gz": gz}
        return {"gx": 2 * lax.rem(spot, 2) + core, "gy": gy, "gz": lax.div(spot, 2)}

    pl.semaphore_signal(barrier, inc=1, device_id=partner, device_id_type=MESH)
    for dim in "xyz":
        for k in (1, 2, 3):
            pl.semaphore_signal(barrier, inc=1, device_id=ring_peer(dim, k), device_id_type=MESH)

    def own_copy(x):
        return pltpu.make_async_copy(v_hbm.at[x], vp.at[x + 1, pl.ds(1, SY)], own_sem.at[x])

    @pl.loop(0, SX)
    def _(x):
        own_copy(x).start()

    def has(dx, dy):
        ok = jnp.bool_(True)
        if dx == 1:
            ok = jnp.logical_and(ok, gx < 3)
        if dx == -1:
            ok = jnp.logical_and(ok, gx > 0)
        if dy == 1:
            ok = jnp.logical_and(ok, gy < 15)
        if dy == -1:
            ok = jnp.logical_and(ok, gy > 0)
        return ok

    def remote(src, dst, send, recv, where):
        return pltpu.make_async_remote_copy(
            src_ref=src, dst_ref=dst, send_sem=send, recv_sem=recv, device_id=where, device_id_type=MESH
        )

    def up(x):
        return remote(v_hbm.at[x, SY - 1], vp.at[x + 1, 0], up_send.at[x], up_recv.at[x], at(0, 1, gz))

    def down(x):
        return remote(v_hbm.at[x, 0], vp.at[x + 1, PY - 1], dn_send.at[x], dn_recv.at[x], at(0, -1, gz))

    def side(index):
        dx, dy = sides[index]
        src_x = SX - 1 if dx == 1 else 0
        dst_x = 0 if dx == 1 else PX - 1
        if dy == 0:
            src, dst = v_hbm.at[src_x], vp.at[dst_x, pl.ds(1, SY)]
        else:
            row = 0 if dy == 1 else PY - 1
            src, dst = vp.at[src_x + 1, row], vp.at[dst_x, row]
        return remote(src, dst, side_send.at[index], side_recv.at[index], at(dx, 0, gz))

    def side_sent(index):
        dx, dy = sides[index]
        return has(dx, -dy)

    sides = [(1, 0), (1, 1), (1, -1), (-1, 0), (-1, 1), (-1, -1)]

    @pl.when(jnp.logical_not(has(0, -1)))
    def _():
        vp[:, 0] = jnp.zeros((PX, SZ, K), BF16)

    @pl.when(jnp.logical_not(has(0, 1)))
    def _():
        vp[:, PY - 1] = jnp.zeros((PX, SZ, K), BF16)

    @pl.when(jnp.logical_not(has(-1, 0)))
    def _():
        vp[0] = jnp.zeros((PY, SZ, K), BF16)

    @pl.when(jnp.logical_not(has(1, 0)))
    def _():
        vp[PX - 1] = jnp.zeros((PY, SZ, K), BF16)

    zrows = [(0, 0, 0, 128)]
    zrows += [(0, 1, 128, 16), (0, -1, 144, 16), (1, 0, 160, 16), (-1, 0, 176, 16)]
    zrows += [(1, 1, 192, 16), (1, -1, 208, 16), (-1, 1, 224, 16), (-1, -1, 240, 16)]
    for dx, dy, first, count in zrows[1:]:

        @pl.when(jnp.logical_not(has(dx, dy)))
        def _():
            zh[pl.ds(first, count)] = jnp.zeros((count, K), BF16)

    pl.semaphore_wait(barrier, 27)

    @pl.when(has(1, 0))
    def _():
        side(0).start()

    @pl.when(has(-1, 0))
    def _():
        side(3).start()

    def send_plane(x):
        @pl.when(has(0, 1))
        def _():
            up(x).start()

        @pl.when(has(0, -1))
        def _():
            down(x).start()

    send_plane(SX - 1)
    send_plane(0)
    pl.loop(1, SX - 1)(send_plane)

    kappa = mat[0].reshape(SX * SY, SZ)
    rho = mat[1].reshape(SX * SY, SZ)
    own_kappa = lax.dot_general(kappa, sel_ref[...], DIM0, precision=HIGH, preferred_element_type=F32)
    own_rho = lax.dot_general(rho, sel_ref[...], DIM0, precision=HIGH, preferred_element_type=F32)
    near = lax.dot_general(kappa, txy_ref[...], DIM0, precision=HIGH, preferred_element_type=F32)
    edge_row = jnp.zeros((1, 256), F32)
    near = (
        jnp.concatenate([edge_row, near[:-1]], axis=0)
        + 2.0 * near
        + jnp.concatenate([near[1:], edge_row], axis=0)
    )
    alpha = 2.0 * own_kappa + near * (1.0 / 32.0)
    beta = own_kappa * (1.0 / 16.0)
    for xp in range(PX):
        span = slice(xp * PY, xp * PY + PY)
        coef[xp, 0, :, 0:PY] = alpha[:, span]
        coef[xp, 1, :, 0:PY] = beta[:, span]
        coef[xp, 2, :, 0:PY] = own_rho[:, span]

    @pl.loop(0, SX)
    def _(x):
        own_copy(x).wait()
        low = vp[x + 1, 1 : 1 + SY, 0:16, :].astype(F32)
        high = vp[x + 1, 1 : 1 + SY, SZ - 16 : SZ, :].astype(F32)
        spot = lax.broadcasted_iota(jnp.int32, (1, 16, 1), 1)
        low = jnp.sum(jnp.where(spot == 0, low, 0.0), axis=1)
        high = jnp.sum(jnp.where(spot == 15, high, 0.0), axis=1)
        zf[pl.ds(pl.multiple_of(x * SY, SY), SY)] = jnp.where(gz == 0, high, low)

    zface[...] = zf[...].astype(BF16)
    zs[...] = jnp.dot(pick_ref[...], zface[...], preferred_element_type=F32).astype(BF16)

    def zcopy(index, dx, dy):
        first, count = zrows[index][2:]
        if (dx, dy) == (0, 0):
            src = zface
        elif dx == 0:
            src = zs.at[pl.ds(16 if dy == 1 else 0, 16)]
        else:
            src = zs.at[pl.ds(48 if dx == 1 else 32, 16)]
        return remote(
            src, zh.at[pl.ds(first, count)], z_send.at[index], z_recv.at[index], at(dx, dy, other)
        )

    for index, (dx, dy, _, _) in enumerate(zrows):

        @pl.when(has(-dx, -dy))
        def _():
            zcopy(index, -dx, -dy).start()

    def wait_rows(x):
        @pl.when(has(0, -1))
        def _():
            up(x).wait_recv()

        @pl.when(has(0, 1))
        def _():
            down(x).wait_recv()

    wait_rows(SX - 1)
    wait_rows(0)
    for index in (1, 2, 4, 5):

        @pl.when(side_sent(index))
        def _():
            side(index).start()

    acc[...] = jnp.zeros_like(acc)

    def wait_sides(group):
        for index in group:
            dx, dy = sides[index]

            @pl.when(has(-dx, -dy))
            def _():
                side(index).wait_recv()

    def plane_stage(xp, slot):
        for b in range(2):
            for c in range(2):
                lanes = slice(256 * c, 256 * c + 256)
                own = vp[xp, HALF * b : HALF * b + HALF, :, lanes]
                a = jnp.dot(
                    tz_ref[...], own.reshape(HALF * SZ, 256), preferred_element_type=F32
                ).astype(BF16).reshape(HALF, SZ, 256)
                az[slot % 2][HALF * b : HALF * b + HALF, :, lanes] = a
                bz[slot % 2][HALF * b : HALF * b + HALF, :, lanes] = a + (own + own)
        for c in range(2):
            lanes = slice(256 * c, 256 * c + 256)
            a, b = az[slot % 2], bz[slot % 2]
            pair = a[0, :, lanes] + a[1, :, lanes]
            for y in range(SY):
                nxt = a[y + 1, :, lanes] + a[y + 2, :, lanes]
                ya[slot][y, :, lanes] = pair + nxt
                pair = nxt
                yb[slot][y, :, lanes] = (b[y, :, lanes] + b[y + 2, :, lanes]) + BF16(4.0) * b[y + 1, :, lanes]

    def cell_pair(x, slots, side_by):
        x_out, v_out = xbufs[side_by], vts[side_by]
        for y in range(SY):
            cols = [
                [coef[x + 1 + i, n, :, y + 1 : y + 2] for n in range(3)] for i in range(2)
            ]
            for c in range(2):
                lanes = slice(256 * c, 256 * c + 256)
                stage = [ya[n][y, :, lanes] for n in slots]
                sums = [stage[i] + stage[i + 1] for i in range(3)]
                other_stage = [yb[n][y, :, lanes] for n in slots]
                for i in range(2):
                    al, be, ro = cols[i]
                    row = pl.ds(SY * SZ * i + y * SZ, SZ)
                    u = (sums[i] + sums[i + 1]).astype(F32)
                    own = vp[x + 1 + i, y + 1, :, lanes].astype(F32)
                    x_out[row, 256 * c : 256 * c + 256] = (al * own - be * u).astype(BF16)
                    m = (other_stage[i] + other_stage[i + 2]) + BF16(4.0) * other_stage[i + 1]
                    x_out[row, K + 256 * c : K + 256 * c + 256] = (ro * m.astype(F32)).astype(BF16)
        for i in range(2):
            for n, yp in enumerate((0, PY - 1)):
                row = pl.ds(2 * SY * SZ + (2 * i + n) * SZ, SZ)
                x_out[row, 0:K] = halo_rows(x + 1 + i, yp).astype(BF16)
        for i in range(2):
            v_out[:, SY * SZ * i : SY * SZ * i + SY * SZ] = (
                vp[x + 1 + i, 1 : 1 + SY].reshape(SY * SZ, K).T
            )
        sides_of = jnp.concatenate([vp[x + 1 + i, yp] for i in range(2) for yp in (0, PY - 1)], axis=0)
        v_out[:, 2 * SY * SZ : 2 * SY * SZ + 4 * SZ] = sides_of.T

    def gram_pair(side_by):
        x_in, v_in = xbufs[side_by], vts[side_by]
        for c in range(4):
            lanes = slice(256 * c, 256 * c + 256)
            depth = PAIR_ROWS if c < 2 else 2 * SY * SZ
            acc[:, lanes] += jnp.dot(
                v_in[:, 0:depth], x_in[0:depth, lanes], preferred_element_type=F32
            )

    def halo_rows(xp, yp):
        return coef[xp, 0, :, yp : yp + 1] * vp[xp, yp].astype(F32)

    def side_products():
        for xp in (0, PX - 1):
            for y in range(PY):
                xbuf[y * SZ : y * SZ + SZ, 0:K] = halo_rows(xp, y).astype(BF16)
            vt[...] = vp[xp].reshape(PY * SZ, K).T
            for c in range(2):
                lanes = slice(256 * c, 256 * c + 256)
                acc[:, lanes] += jnp.dot(vt[...], xbuf[:, lanes], preferred_element_type=F32)
        for index, (dx, dy, _, _) in enumerate(zrows):

            @pl.when(has(dx, dy))
            def _():
                zcopy(index, -dx, -dy).wait_recv()

        lane = lax.broadcasted_iota(jnp.int32, (SX * SY, SZ), 1)
        at_edge = lane == jnp.where(gz == 0, SZ - 1, 0)
        kappa_edge = jnp.sum(
            jnp.where(at_edge, mat[0].reshape(SX * SY, SZ), 0.0), axis=1, keepdims=True
        )
        rho_edge = jnp.sum(
            jnp.where(at_edge, mat[1].reshape(SX * SY, SZ), 0.0), axis=1, keepdims=True
        )
        far = zh[...]
        du = jnp.dot(t2_ref[...], far, preferred_element_type=F32)
        dm = jnp.dot(t4_ref[...], far, preferred_element_type=F32)
        xbuf[0:128, 0:K] = (kappa_edge * (-1.0 / 16.0) * du).astype(BF16)
        xbuf[0:128, K : 2 * K] = (rho_edge * dm).astype(BF16)
        reach = jnp.dot(
            t2t_ref[...], jnp.broadcast_to(kappa_edge, (128, 128)), precision=HIGH, preferred_element_type=F32
        ) * (1.0 / 32.0)
        for c in range(4):
            lanes = slice(128 * c, 128 * c + 128)
            xbuf[128:384, lanes] = (reach * far[:, lanes].astype(F32)).astype(BF16)
        vt[:, 0:128] = zface[...].T
        vt[:, 128:384] = far.T
        for c in range(4):
            lanes = slice(256 * c, 256 * c + 256)
            depth = 384 if c < 2 else 128
            acc[:, lanes] += jnp.dot(vt[:, 0:depth], xbuf[0:depth, lanes], preferred_element_type=F32)

    for ref in (xbufs[1], vts[1]):
        ref[...] = jnp.zeros_like(ref)
    plane_stage(1, 1)
    for n in (2, 3):
        wait_rows(n - 1)
        plane_stage(n, n)
    wait_sides((0, 1, 2))
    plane_stage(0, 0)

    @pl.loop(0, 3)
    def _(t):
        x = 4 * t
        for half in range(2):
            gram_pair(1 - half)
            cell_pair(x + 2 * half, (0, 1, 2, 3) if half == 0 else (2, 3, 0, 1), half)
            for n in range(2):
                wait_rows(x + 2 * half + 3 + n)
            for n in range(2):
                plane_stage(x + 2 * half + 4 + n, 2 * half + n)

        @pl.when(t == 1)
        def _():
            wait_sides((3, 4, 5))
            side_products()
            plane_stage(SX, 4)
            plane_stage(SX + 1, 5)

    gram_pair(1)
    cell_pair(12, (0, 1, 2, 3), 0)
    gram_pair(0)
    cell_pair(14, (2, 3, 4, 5), 1)
    gram_pair(1)

    def core_copy(c):
        first, width = COLORS[c]
        cols = pl.ds(first, width)
        return remote(
            sym.at[1 - core, :, :, :, :, :, cols], core_in.at[:, :, :, :, :, cols],
            core_send.at[c], core_recv.at[c], partner,
        )

    def put(gx_row, col, block):
        for part in range(32):
            sym[
                gx_row % 2, gx_row // 2, part // 8, part // 2 % 4, part % 2, :, col : col + 128
            ] = block[4 * part : 4 * part + 4]

    for half, scale in ((0, 0.5 / CELLS), (1, 0.5 / (216.0 * CELLS))):
        for i in range(4):
            for j in range(i, 4):
                rows = slice(128 * i, 128 * i + 128)
                cols = slice(128 * j, 128 * j + 128)
                there = slice(K * half + 128 * j, K * half + 128 * j + 128)
                back = slice(K * half + 128 * i, K * half + 128 * i + 128)
                both = (acc[rows, there] + acc[cols, back].T) * scale
                put(i, K * half + 128 * j, both)
                if i != j:
                    put(j, K * half + 128 * i, both.T)
        if half == 0:
            core_copy(0).start()
        else:
            core_copy(1).start()
            core_copy(2).start()

    held = [[ring[6 * c + 2 * s] for s in range(3)] for c in range(3)]
    landed = [[ring[6 * c + 2 * s + 1] for s in range(3)] for c in range(3)]

    def piece(c, s, spot):
        ref, dim, left = held[c][s], ORDERS[c][s], ORDERS[c][s:]
        index = []
        for name in ("z_lo", "x", "y", "z_hi"):
            if name[0] not in left:
                continue
            if name[0] != dim:
                index.append(slice(None))
            elif name == "z_lo":
                index.append(lax.rem(spot, 2))
            elif name == "z_hi":
                index.append(lax.div(spot, 2))
            else:
                index.append(spot)
        return ref.at[tuple(index)]

    def ring_copy(c, s, k):
        dim = ORDERS[c][s]
        number = 9 * c + 3 * s + k - 1
        return remote(
            piece(c, s, ring_place(dim, k)), landed[c][s].at[k - 1],
            ring_send.at[number], ring_recv.at[number], ring_peer(dim, k),
        )

    for c in range(3):
        first, width = COLORS[c]
        cols = slice(first, first + width)
        core_copy(c).wait_recv()
        for zl in range(2):
            for x in range(4):
                held[c][0][zl, x] = sym[core, zl, x, :, :, :, cols] + core_in[zl, x, :, :, :, cols]
        for k in (2, 1, 3):
            ring_copy(c, 0, k).start()
    for s in range(3):
        for c in range(3):
            first, width = COLORS[c]
            for k in (1, 3, 2):
                ring_copy(c, s, k).wait_recv()
            total = piece(c, s, ring_place(ORDERS[c][s], 0))[...]
            for k in (1, 3, 2):
                total = total + landed[c][s][k - 1]
            if s < 2:
                held[c][s + 1][...] = total
                for k in (2, 1, 3):
                    ring_copy(c, s + 1, k).start()
            else:
                for tile in range(width // 128):
                    col = first + 128 * tile
                    part = total[:, 128 * tile : 128 * tile + 128]
                    out[:, col : col + 128] = part
    for c in range(3):
        core_copy(c).wait_send()
        for s in range(3):
            for k in (1, 2, 3):
                ring_copy(c, s, k).wait_send()

    @pl.loop(0, SX)
    def _(x):
        @pl.when(has(0, 1))
        def _():
            up(x).wait_send()

        @pl.when(has(0, -1))
        def _():
            down(x).wait_send()

    for index in range(6):

        @pl.when(side_sent(index))
        def _():
            side(index).wait_send()

    for index, (dx, dy, _, _) in enumerate(zrows):

        @pl.when(has(-dx, -dy))
        def _():
            zcopy(index, -dx, -dy).wait_send()


def ring_buffers():
    buffers = []
    for (_, width), order in zip(COLORS, ORDERS):
        for s in range(3):
            left = [n for d, n in (("z", 2), ("x", 4), ("y", 4), ("z", 2)) if d in order[s:]]
            after = [n for d, n in (("z", 2), ("x", 4), ("y", 4), ("z", 2)) if d in order[s + 1 :]]
            buffers.append(pltpu.VMEM((*left, 4, width), F32))
            buffers.append(pltpu.VMEM((3, *after, 4, width), F32))
    return buffers


def local_products(eigvecs, material):
    tz, sel, txy, t2, t4, t2t, pick = constants()
    small = (
        jnp.asarray(tz, BF16), jnp.asarray(sel), jnp.asarray(txy), jnp.asarray(t2, BF16),
        jnp.asarray(t4, BF16), jnp.asarray(t2t), jnp.asarray(pick, BF16),
    )
    vmem = pl.BlockSpec(memory_space=pltpu.VMEM)
    dma = pltpu.SemaphoreType.DMA
    return pl.pallas_call(
        local_kernel,
        out_shape=jax.ShapeDtypeStruct((4, 2 * K), F32),
        in_specs=[pl.BlockSpec(memory_space=pl.ANY)] + [vmem] * 8,
        out_specs=vmem,
        scratch_shapes=[
            pltpu.VMEM((PX, PY, SZ, K), BF16),
            [pltpu.VMEM((PY, SZ, K), BF16)] * 2,
            [pltpu.VMEM((PY, SZ, K), BF16)] * 2,
            [pltpu.VMEM((SY, SZ, K), BF16)] * 6,
            [pltpu.VMEM((SY, SZ, K), BF16)] * 6,
            [pltpu.VMEM((PAIR_ROWS, 2 * K), BF16)] * 2,
            [pltpu.VMEM((K, PAIR_ROWS), BF16)] * 2,
            pltpu.VMEM((PY * SZ, 2 * K), BF16),
            pltpu.VMEM((K, PY * SZ), BF16),
            pltpu.VMEM((PX, 3, SZ, 128), F32),
            pltpu.VMEM((K, 2 * K), F32),
            pltpu.VMEM((SX * SY, K), F32),
            pltpu.VMEM((64, K), BF16),
            pltpu.VMEM((256, K), BF16),
            pltpu.VMEM((SX * SY, K), BF16),
            dma((SX,)), dma((SX,)), dma((SX,)), dma((SX,)), dma((SX,)),
            dma((6,)), dma((6,)), dma((9,)), dma((9,)),
            pltpu.VMEM((2, 2, 4, 4, 2, 4, 2 * K), F32),
            pltpu.VMEM((2, 4, 4, 2, 4, 2 * K), F32),
            *ring_buffers(),
            dma((3,)), dma((3,)), dma((27,)), dma((27,)),
        ],
        compiler_params=pltpu.CompilerParams(
            collective_id=0, has_side_effects=True, vmem_limit_bytes=60 * 1024 * 1024
        ),
    )(eigvecs, material, *small)


def per_device(eigvecs, material):
    both = local_products(eigvecs, material)
    return both[:, :K], both[:, K:]


def solution(mesh):
    return jax.shard_map(
        per_device,
        mesh=mesh,
        in_specs=(P("gx", "gy", "gz", None), P(None, "gx", "gy", "gz")),
        out_specs=(P(("gx", "gy", "gz"), None), P(("gx", "gy", "gz"), None)),
        check_vma=False,
    )
```

```python
import functools

import jax
import jax.numpy as jnp
import numpy as np
from jax import lax
from jax.experimental import pallas as pl
from jax.experimental.pallas import tpu as pltpu
from jax.sharding import PartitionSpec as P

MESH = pl.DeviceIdType.MESH
F32 = jnp.float32
BF16 = jnp.bfloat16
HIGH = lax.Precision.HIGHEST

SX, SY, SZ, K = 16, 8, 48, 512
PX, PY = SX + 2, SY + 2
HALF = PY // 2
PAIR_ROWS = 2 * SY * SZ + 4 * SZ
CELLS = 64 * 128 * 96
DIM0 = (((0,), (0,)), ((), ()))
COLORS = ((0, 384), (384, 384), (768, 256))
ORDERS = ("xyz", "yzx", "zxy")


def constants():
    rows = HALF * SZ
    tz = np.zeros((rows, rows), np.float32)
    for r in range(rows):
        for c in (r - 1, r, r + 1):
            if 0 <= c < rows and c // SZ == r // SZ:
                tz[r, c] = 2.0 if c == r else 1.0
    sel = np.zeros((SX * SY, 256), np.float32)
    txy = np.zeros((SX * SY, 256), np.float32)
    for x in range(SX):
        for y in range(SY):
            row = x * SY + y
            sel[row, (x + 1) * PY + y + 1] = 1.0
            for dx in (-1, 0, 1):
                for dy in (-1, 0, 1):
                    txy[row, (x + 1 + dx) * PY + y + 1 + dy] = (2 - abs(dx)) * (2 - abs(dy))
    places = {}
    for x in range(SX):
        for y in range(SY):
            places[(x, y)] = x * SY + y
    for x in range(SX):
        places[(x, SY)] = 128 + x
        places[(x, -1)] = 144 + x
    for y in range(SY):
        places[(SX, y)] = 160 + y
        places[(-1, y)] = 176 + y
    places[(SX, SY)] = 192
    places[(SX, -1)] = 208 + 7
    places[(-1, SY)] = 224
    places[(-1, -1)] = 240 + 7
    t2 = np.zeros((128, 256), np.float32)
    t4 = np.zeros((128, 256), np.float32)
    for x in range(SX):
        for y in range(SY):
            for dx in (-1, 0, 1):
                for dy in (-1, 0, 1):
                    place = places[(x + dx, y + dy)]
                    t2[x * SY + y, place] = (2 - abs(dx)) * (2 - abs(dy))
                    t4[x * SY + y, place] = (4 - 3 * abs(dx)) * (4 - 3 * abs(dy))
    pick = np.zeros((64, 128), np.float32)
    for x in range(SX):
        pick[x, x * SY] = 1.0
        pick[16 + x, x * SY + 7] = 1.0
    for y in range(SY):
        pick[32 + y, y] = 1.0
        pick[48 + y, 15 * SY + y] = 1.0
    return tz, sel, txy, t2, t4, np.ascontiguousarray(t2.T), pick


def local_kernel(
    v_hbm, mat, tz_ref, sel_ref, txy_ref, t2_ref, t4_ref, t2t_ref, pick_ref, out,
    vp, az, bz, ya, yb, xbufs, vts, xbuf, vt, coef, acc, zf, zs, zh, zface,
    own_sem, up_send, dn_send, up_recv, dn_recv, side_send, side_recv, z_send, z_recv,
    sym, core_in, *ring,
):
    core_send, core_recv, ring_send, ring_recv = ring[-4:]
    ring = ring[:-4]
    gx, gy, gz = lax.axis_index("gx"), lax.axis_index("gy"), lax.axis_index("gz")
    other = 1 - gz

    def at(dx, dy, z):
        return {"gx": lax.rem(gx + dx + 4, 4), "gy": lax.rem(gy + dy + 16, 16), "gz": z}

    around = [(dx, dy) for dx in (-1, 0, 1) for dy in (-1, 0, 1)]
    barrier = pltpu.get_barrier_semaphore()
    for dx, dy in around:
        if (dx, dy) != (0, 0):
            pl.semaphore_signal(barrier, inc=1, device_id=at(dx, dy, gz), device_id_type=MESH)
        pl.semaphore_signal(barrier, inc=1, device_id=at(dx, dy, other), device_id_type=MESH)

    core, z_lo = lax.rem(gx, 2), lax.div(gx, 2)
    ring_x, ring_y = lax.div(gy, 4), lax.rem(gy, 4)
    ring_z = 2 * gz + z_lo
    partner = {"gx": gx + 1 - 2 * core, "gy": gy, "gz": gz}

    def ring_place(dim, k):
        mine = {"x": ring_x, "y": ring_y, "z": ring_z}[dim]
        return lax.rem(mine + k, 4)

    def ring_peer(dim, k):
        spot = ring_place(dim, k)
        if dim == "x":
            return {"gx": gx, "gy": 4 * spot + ring_y, "gz": gz}
        if dim == "y":
            return {"gx": gx, "gy": 4 * ring_x + spot, "gz": gz}
        return {"gx": 2 * lax.rem(spot, 2) + core, "gy": gy, "gz": lax.div(spot, 2)}

    pl.semaphore_signal(barrier, inc=1, device_id=partner, device_id_type=MESH)
    for dim in "xyz":
        for k in (1, 2, 3):
            pl.semaphore_signal(barrier, inc=1, device_id=ring_peer(dim, k), device_id_type=MESH)

    def own_copy(x):
        return pltpu.make_async_copy(v_hbm.at[x], vp.at[x + 1, pl.ds(1, SY)], own_sem.at[x])

    @pl.loop(0, SX)
    def _(x):
        own_copy(x).start()

    def has(dx, dy):
        ok = jnp.bool_(True)
        if dx == 1:
            ok = jnp.logical_and(ok, gx < 3)
        if dx == -1:
            ok = jnp.logical_and(ok, gx > 0)
        if dy == 1:
            ok = jnp.logical_and(ok, gy < 15)
        if dy == -1:
            ok = jnp.logical_and(ok, gy > 0)
        return ok

    def remote(src, dst, send, recv, where):
        return pltpu.make_async_remote_copy(
            src_ref=src, dst_ref=dst, send_sem=send, recv_sem=recv, device_id=where, device_id_type=MESH
        )

    def up(x):
        return remote(v_hbm.at[x, SY - 1], vp.at[x + 1, 0], up_send.at[x], up_recv.at[x], at(0, 1, gz))

    def down(x):
        return remote(v_hbm.at[x, 0], vp.at[x + 1, PY - 1], dn_send.at[x], dn_recv.at[x], at(0, -1, gz))

    def side(index):
        dx, dy = sides[index]
        src_x = SX - 1 if dx == 1 else 0
        dst_x = 0 if dx == 1 else PX - 1
        if dy == 0:
            src, dst = v_hbm.at[src_x], vp.at[dst_x, pl.ds(1, SY)]
        else:
            row = 0 if dy == 1 else PY - 1
            src, dst = vp.at[src_x + 1, row], vp.at[dst_x, row]
        return remote(src, dst, side_send.at[index], side_recv.at[index], at(dx, 0, gz))

    def side_sent(index):
        dx, dy = sides[index]
        return has(dx, -dy)

    sides = [(1, 0), (1, 1), (1, -1), (-1, 0), (-1, 1), (-1, -1)]

    @pl.when(jnp.logical_not(has(0, -1)))
    def _():
        vp[:, 0] = jnp.zeros((PX, SZ, K), BF16)

    @pl.when(jnp.logical_not(has(0, 1)))
    def _():
        vp[:, PY - 1] = jnp.zeros((PX, SZ, K), BF16)

    @pl.when(jnp.logical_not(has(-1, 0)))
    def _():
        vp[0] = jnp.zeros((PY, SZ, K), BF16)

    @pl.when(jnp.logical_not(has(1, 0)))
    def _():
        vp[PX - 1] = jnp.zeros((PY, SZ, K), BF16)

    zrows = [(0, 0, 0, 128)]
    zrows += [(0, 1, 128, 16), (0, -1, 144, 16), (1, 0, 160, 16), (-1, 0, 176, 16)]
    zrows += [(1, 1, 192, 16), (1, -1, 208, 16), (-1, 1, 224, 16), (-1, -1, 240, 16)]
    for dx, dy, first, count in zrows[1:]:

        @pl.when(jnp.logical_not(has(dx, dy)))
        def _():
            zh[pl.ds(first, count)] = jnp.zeros((count, K), BF16)

    pl.semaphore_wait(barrier, 27)

    @pl.when(has(1, 0))
    def _():
        side(0).start()

    @pl.when(has(-1, 0))
    def _():
        side(3).start()

    def send_plane(x):
        @pl.when(has(0, 1))
        def _():
            up(x).start()

        @pl.when(has(0, -1))
        def _():
            down(x).start()

    send_plane(SX - 1)
    send_plane(0)
    pl.loop(1, 7)(send_plane)

    kappa = mat[0].reshape(SX * SY, SZ)
    rho = mat[1].reshape(SX * SY, SZ)
    own_kappa = lax.dot_general(kappa, sel_ref[...], DIM0, precision=HIGH, preferred_element_type=F32)
    own_rho = lax.dot_general(rho, sel_ref[...], DIM0, precision=HIGH, preferred_element_type=F32)
    near = lax.dot_general(kappa, txy_ref[...], DIM0, precision=HIGH, preferred_element_type=F32)
    edge_row = jnp.zeros((1, 256), F32)
    near = (
        jnp.concatenate([edge_row, near[:-1]], axis=0)
        + 2.0 * near
        + jnp.concatenate([near[1:], edge_row], axis=0)
    )
    alpha = 2.0 * own_kappa + near * (1.0 / 32.0)
    beta = own_kappa * (1.0 / 16.0)
    for xp in range(PX):
        span = slice(xp * PY, xp * PY + PY)
        coef[xp, 0, :, 0:PY] = alpha[:, span]
        coef[xp, 1, :, 0:PY] = beta[:, span]
        coef[xp, 2, :, 0:PY] = own_rho[:, span]

    @pl.loop(0, SX)
    def _(x):
        own_copy(x).wait()
        low = vp[x + 1, 1 : 1 + SY, 0:16, :].astype(F32)
        high = vp[x + 1, 1 : 1 + SY, SZ - 16 : SZ, :].astype(F32)
        spot = lax.broadcasted_iota(jnp.int32, (1, 16, 1), 1)
        low = jnp.sum(jnp.where(spot == 0, low, 0.0), axis=1)
        high = jnp.sum(jnp.where(spot == 15, high, 0.0), axis=1)
        zf[pl.ds(pl.multiple_of(x * SY, SY), SY)] = jnp.where(gz == 0, high, low)

    zface[...] = zf[...].astype(BF16)
    zs[...] = jnp.dot(pick_ref[...], zface[...], preferred_element_type=F32).astype(BF16)

    def zcopy(index, dx, dy):
        first, count = zrows[index][2:]
        if (dx, dy) == (0, 0):
            src = zface
        elif dx == 0:
            src = zs.at[pl.ds(16 if dy == 1 else 0, 16)]
        else:
            src = zs.at[pl.ds(48 if dx == 1 else 32, 16)]
        return remote(
            src, zh.at[pl.ds(first, count)], z_send.at[index], z_recv.at[index], at(dx, dy, other)
        )

    for index, (dx, dy, _, _) in enumerate(zrows):

        @pl.when(has(-dx, -dy))
        def _():
            zcopy(index, -dx, -dy).start()

    pl.loop(7, SX - 1)(send_plane)

    def wait_rows(x):
        @pl.when(has(0, -1))
        def _():
            up(x).wait_recv()

        @pl.when(has(0, 1))
        def _():
            down(x).wait_recv()

    wait_rows(SX - 1)
    wait_rows(0)
    for index in (1, 2, 4, 5):

        @pl.when(side_sent(index))
        def _():
            side(index).start()

    acc[...] = jnp.zeros_like(acc)

    def wait_sides(group):
        for index in group:
            dx, dy = sides[index]

            @pl.when(has(-dx, -dy))
            def _():
                side(index).wait_recv()

    def plane_stage(xp, slot):
        for b in range(2):
            for c in range(2):
                lanes = slice(256 * c, 256 * c + 256)
                own = vp[xp, HALF * b : HALF * b + HALF, :, lanes]
                a = jnp.dot(
                    tz_ref[...], own.reshape(HALF * SZ, 256), preferred_element_type=F32
                ).astype(BF16).reshape(HALF, SZ, 256)
                az[slot % 2][HALF * b : HALF * b + HALF, :, lanes] = a
                bz[slot % 2][HALF * b : HALF * b + HALF, :, lanes] = a + (own + own)
        for c in range(2):
            lanes = slice(256 * c, 256 * c + 256)
            a, b = az[slot % 2], bz[slot % 2]
            pair = a[0, :, lanes] + a[1, :, lanes]
            for y in range(SY):
                nxt = a[y + 1, :, lanes] + a[y + 2, :, lanes]
                ya[slot][y, :, lanes] = pair + nxt
                pair = nxt
                yb[slot][y, :, lanes] = (b[y, :, lanes] + b[y + 2, :, lanes]) + BF16(4.0) * b[y + 1, :, lanes]

    def cell_pair(x, slots, side_by):
        x_out, v_out = xbufs[side_by], vts[side_by]
        for y in range(SY):
            cols = [
                [coef[x + 1 + i, n, :, y + 1 : y + 2] for n in range(3)] for i in range(2)
            ]
            for c in range(2):
                lanes = slice(256 * c, 256 * c + 256)
                stage = [ya[n][y, :, lanes] for n in slots]
                sums = [stage[i] + stage[i + 1] for i in range(3)]
                other_stage = [yb[n][y, :, lanes] for n in slots]
                for i in range(2):
                    al, be, ro = cols[i]
                    row = pl.ds(SY * SZ * i + y * SZ, SZ)
                    u = (sums[i] + sums[i + 1]).astype(F32)
                    own = vp[x + 1 + i, y + 1, :, lanes].astype(F32)
                    x_out[row, 256 * c : 256 * c + 256] = (al * own - be * u).astype(BF16)
                    m = (other_stage[i] + other_stage[i + 2]) + BF16(4.0) * other_stage[i + 1]
                    x_out[row, K + 256 * c : K + 256 * c + 256] = (ro * m.astype(F32)).astype(BF16)
        for i in range(2):
            for n, yp in enumerate((0, PY - 1)):
                row = pl.ds(2 * SY * SZ + (2 * i + n) * SZ, SZ)
                x_out[row, 0:K] = halo_rows(x + 1 + i, yp).astype(BF16)
        for i in range(2):
            v_out[:, SY * SZ * i : SY * SZ * i + SY * SZ] = (
                vp[x + 1 + i, 1 : 1 + SY].reshape(SY * SZ, K).T
            )
        sides_of = jnp.concatenate([vp[x + 1 + i, yp] for i in range(2) for yp in (0, PY - 1)], axis=0)
        v_out[:, 2 * SY * SZ : 2 * SY * SZ + 4 * SZ] = sides_of.T

    def gram_pair(side_by, halves=(0, 1)):
        x_in, v_in = xbufs[side_by], vts[side_by]
        for c in halves:
            lanes = slice(K * c, K * c + K)
            depth = 2 * SY * SZ if c else PAIR_ROWS
            acc[:, lanes] += jnp.dot(
                v_in[:, 0:depth], x_in[0:depth, lanes], preferred_element_type=F32
            )

    def halo_rows(xp, yp):
        return coef[xp, 0, :, yp : yp + 1] * vp[xp, yp].astype(F32)

    def side_products():
        for xp in (0, PX - 1):
            for y in range(PY):
                xbuf[y * SZ : y * SZ + SZ, 0:K] = halo_rows(xp, y).astype(BF16)
            vt[...] = vp[xp].reshape(PY * SZ, K).T
            for c in range(2):
                lanes = slice(256 * c, 256 * c + 256)
                acc[:, lanes] += jnp.dot(vt[...], xbuf[:, lanes], preferred_element_type=F32)
        for index, (dx, dy, _, _) in enumerate(zrows):

            @pl.when(has(dx, dy))
            def _():
                zcopy(index, -dx, -dy).wait_recv()

        lane = lax.broadcasted_iota(jnp.int32, (SX * SY, SZ), 1)
        at_edge = lane == jnp.where(gz == 0, SZ - 1, 0)
        kappa_edge = jnp.sum(
            jnp.where(at_edge, mat[0].reshape(SX * SY, SZ), 0.0), axis=1, keepdims=True
        )
        rho_edge = jnp.sum(
            jnp.where(at_edge, mat[1].reshape(SX * SY, SZ), 0.0), axis=1, keepdims=True
        )
        far = zh[...]
        du = jnp.dot(t2_ref[...], far, preferred_element_type=F32)
        dm = jnp.dot(t4_ref[...], far, preferred_element_type=F32)
        xbuf[0:128, 0:K] = (kappa_edge * (-1.0 / 16.0) * du).astype(BF16)
        xbuf[0:128, K : 2 * K] = (rho_edge * dm).astype(BF16)
        reach = jnp.dot(
            t2t_ref[...], jnp.broadcast_to(kappa_edge, (128, 128)), precision=HIGH, preferred_element_type=F32
        ) * (1.0 / 32.0)
        for c in range(4):
            lanes = slice(128 * c, 128 * c + 128)
            xbuf[128:384, lanes] = (reach * far[:, lanes].astype(F32)).astype(BF16)
        vt[:, 0:128] = zface[...].T
        vt[:, 128:384] = far.T
        for c in range(4):
            lanes = slice(256 * c, 256 * c + 256)
            depth = 384 if c < 2 else 128
            acc[:, lanes] += jnp.dot(vt[:, 0:depth], xbuf[0:depth, lanes], preferred_element_type=F32)

    for ref in (xbufs[1], vts[1]):
        ref[...] = jnp.zeros_like(ref)
    plane_stage(1, 1)
    for n in (2, 3):
        wait_rows(n - 1)
        plane_stage(n, n)
    wait_sides((0, 1, 2))
    plane_stage(0, 0)

    @pl.loop(0, 3)
    def _(t):
        x = 4 * t
        for half in range(2):
            gram_pair(1 - half)
            cell_pair(x + 2 * half, (0, 1, 2, 3) if half == 0 else (2, 3, 0, 1), half)
            for n in range(2):
                wait_rows(x + 2 * half + 3 + n)
            for n in range(2):
                plane_stage(x + 2 * half + 4 + n, 2 * half + n)

        @pl.when(t == 1)
        def _():
            wait_sides((3, 4, 5))
            side_products()
            plane_stage(SX, 4)
            plane_stage(SX + 1, 5)

    gram_pair(1)
    cell_pair(12, (0, 1, 2, 3), 0)
    gram_pair(0)
    cell_pair(14, (2, 3, 4, 5), 1)

    def core_copy(c):
        first, width = COLORS[c]
        cols = pl.ds(first, width)
        return remote(
            sym.at[1 - core, :, :, :, :, :, cols], core_in.at[:, :, :, :, :, cols],
            core_send.at[c], core_recv.at[c], partner,
        )

    def put(gx_row, col, block):
        for part in range(32):
            sym[
                gx_row % 2, gx_row // 2, part // 8, part // 2 % 4, part % 2, :, col : col + 128
            ] = block[4 * part : 4 * part + 4]

    for half, scale in ((0, 0.5 / CELLS), (1, 0.5 / (216.0 * CELLS))):
        gram_pair(1, (half,))
        for i in range(4):
            for j in range(i, 4):
                rows = slice(128 * i, 128 * i + 128)
                cols = slice(128 * j, 128 * j + 128)
                there = slice(K * half + 128 * j, K * half + 128 * j + 128)
                back = slice(K * half + 128 * i, K * half + 128 * i + 128)
                both = (acc[rows, there] + acc[cols, back].T) * scale
                put(i, K * half + 128 * j, both)
                if i != j:
                    put(j, K * half + 128 * i, both.T)
        if half == 0:
            core_copy(0).start()
        else:
            core_copy(1).start()
            core_copy(2).start()

    held = [[ring[6 * c + 2 * s] for s in range(3)] for c in range(3)]
    landed = [[ring[6 * c + 2 * s + 1] for s in range(3)] for c in range(3)]

    def piece(c, s, spot):
        ref, dim, left = held[c][s], ORDERS[c][s], ORDERS[c][s:]
        index = []
        for name in ("z_lo", "x", "y", "z_hi"):
            if name[0] not in left:
                continue
            if name[0] != dim:
                index.append(slice(None))
            elif name == "z_lo":
                index.append(lax.rem(spot, 2))
            elif name == "z_hi":
                index.append(lax.div(spot, 2))
            else:
                index.append(spot)
        return ref.at[tuple(index)]

    def ring_copy(c, s, k):
        dim = ORDERS[c][s]
        number = 9 * c + 3 * s + k - 1
        return remote(
            piece(c, s, ring_place(dim, k)), landed[c][s].at[k - 1],
            ring_send.at[number], ring_recv.at[number], ring_peer(dim, k),
        )

    for c in range(3):
        first, width = COLORS[c]
        cols = slice(first, first + width)
        core_copy(c).wait_recv()
        for zl in range(2):
            for x in range(4):
                held[c][0][zl, x] = sym[core, zl, x, :, :, :, cols] + core_in[zl, x, :, :, :, cols]
        for k in (2, 1, 3):
            ring_copy(c, 0, k).start()
    for s in range(3):
        for c in range(3):
            first, width = COLORS[c]
            for k in (1, 3, 2):
                ring_copy(c, s, k).wait_recv()
            total = piece(c, s, ring_place(ORDERS[c][s], 0))[...]
            for k in (1, 3, 2):
                total = total + landed[c][s][k - 1]
            if s < 2:
                held[c][s + 1][...] = total
                for k in (2, 1, 3):
                    ring_copy(c, s + 1, k).start()
            else:
                for tile in range(width // 128):
                    col = first + 128 * tile
                    part = total[:, 128 * tile : 128 * tile + 128]
                    out[:, col : col + 128] = part
    for c in range(3):
        core_copy(c).wait_send()
        for s in range(3):
            for k in (1, 2, 3):
                ring_copy(c, s, k).wait_send()

    @pl.loop(0, SX)
    def _(x):
        @pl.when(has(0, 1))
        def _():
            up(x).wait_send()

        @pl.when(has(0, -1))
        def _():
            down(x).wait_send()

    for index in range(6):

        @pl.when(side_sent(index))
        def _():
            side(index).wait_send()

    for index, (dx, dy, _, _) in enumerate(zrows):

        @pl.when(has(-dx, -dy))
        def _():
            zcopy(index, -dx, -dy).wait_send()


def ring_buffers():
    buffers = []
    for (_, width), order in zip(COLORS, ORDERS):
        for s in range(3):
            left = [n for d, n in (("z", 2), ("x", 4), ("y", 4), ("z", 2)) if d in order[s:]]
            after = [n for d, n in (("z", 2), ("x", 4), ("y", 4), ("z", 2)) if d in order[s + 1 :]]
            buffers.append(pltpu.VMEM((*left, 4, width), F32))
            buffers.append(pltpu.VMEM((3, *after, 4, width), F32))
    return buffers


def local_products(eigvecs, material):
    tz, sel, txy, t2, t4, t2t, pick = constants()
    small = (
        jnp.asarray(tz, BF16), jnp.asarray(sel), jnp.asarray(txy), jnp.asarray(t2, BF16),
        jnp.asarray(t4, BF16), jnp.asarray(t2t), jnp.asarray(pick, BF16),
    )
    vmem = pl.BlockSpec(memory_space=pltpu.VMEM)
    dma = pltpu.SemaphoreType.DMA
    return pl.pallas_call(
        local_kernel,
        out_shape=jax.ShapeDtypeStruct((4, 2 * K), F32),
        in_specs=[pl.BlockSpec(memory_space=pl.ANY)] + [vmem] * 8,
        out_specs=vmem,
        scratch_shapes=[
            pltpu.VMEM((PX, PY, SZ, K), BF16),
            [pltpu.VMEM((PY, SZ, K), BF16)] * 2,
            [pltpu.VMEM((PY, SZ, K), BF16)] * 2,
            [pltpu.VMEM((SY, SZ, K), BF16)] * 6,
            [pltpu.VMEM((SY, SZ, K), BF16)] * 6,
            [pltpu.VMEM((PAIR_ROWS, 2 * K), BF16)] * 2,
            [pltpu.VMEM((K, PAIR_ROWS), BF16)] * 2,
            pltpu.VMEM((PY * SZ, 2 * K), BF16),
            pltpu.VMEM((K, PY * SZ), BF16),
            pltpu.VMEM((PX, 3, SZ, 128), F32),
            pltpu.VMEM((K, 2 * K), F32),
            pltpu.VMEM((SX * SY, K), F32),
            pltpu.VMEM((64, K), BF16),
            pltpu.VMEM((256, K), BF16),
            pltpu.VMEM((SX * SY, K), BF16),
            dma((SX,)), dma((SX,)), dma((SX,)), dma((SX,)), dma((SX,)),
            dma((6,)), dma((6,)), dma((9,)), dma((9,)),
            pltpu.VMEM((2, 2, 4, 4, 2, 4, 2 * K), F32),
            pltpu.VMEM((2, 4, 4, 2, 4, 2 * K), F32),
            *ring_buffers(),
            dma((3,)), dma((3,)), dma((27,)), dma((27,)),
        ],
        compiler_params=pltpu.CompilerParams(
            collective_id=0, has_side_effects=True, vmem_limit_bytes=60 * 1024 * 1024
        ),
    )(eigvecs, material, *small)


def per_device(eigvecs, material):
    both = local_products(eigvecs, material)
    return both[:, :K], both[:, K:]


def solution(mesh):
    return jax.shard_map(
        per_device,
        mesh=mesh,
        in_specs=(P("gx", "gy", "gz", None), P(None, "gx", "gy", "gz")),
        out_specs=(P(("gx", "gy", "gz"), None), P(("gx", "gy", "gz"), None)),
        check_vma=False,
    )
```

```python
import functools

import jax
import jax.numpy as jnp
import numpy as np
from jax import lax
from jax.experimental import pallas as pl
from jax.experimental.pallas import tpu as pltpu
from jax.sharding import PartitionSpec as P

MESH = pl.DeviceIdType.MESH
F32 = jnp.float32
BF16 = jnp.bfloat16
HIGH = lax.Precision.HIGHEST

SX, SY, SZ, K = 16, 8, 48, 512
PX, PY = SX + 2, SY + 2
HALF = PY // 2
PAIR_ROWS = 2 * SY * SZ + 4 * SZ
CELLS = 64 * 128 * 96
DIM0 = (((0,), (0,)), ((), ()))
COLORS = ((0, 384), (384, 384), (768, 256))
ORDERS = ("xyz", "yzx", "zxy")


def constants():
    rows = HALF * SZ
    tz = np.zeros((rows, rows), np.float32)
    for r in range(rows):
        for c in (r - 1, r, r + 1):
            if 0 <= c < rows and c // SZ == r // SZ:
                tz[r, c] = 2.0 if c == r else 1.0
    sel = np.zeros((SX * SY, 256), np.float32)
    txy = np.zeros((SX * SY, 256), np.float32)
    for x in range(SX):
        for y in range(SY):
            row = x * SY + y
            sel[row, (x + 1) * PY + y + 1] = 1.0
            for dx in (-1, 0, 1):
                for dy in (-1, 0, 1):
                    txy[row, (x + 1 + dx) * PY + y + 1 + dy] = (2 - abs(dx)) * (2 - abs(dy))
    places = {}
    for x in range(SX):
        for y in range(SY):
            places[(x, y)] = x * SY + y
    for x in range(SX):
        places[(x, SY)] = 128 + x
        places[(x, -1)] = 144 + x
    for y in range(SY):
        places[(SX, y)] = 160 + y
        places[(-1, y)] = 176 + y
    places[(SX, SY)] = 192
    places[(SX, -1)] = 208 + 7
    places[(-1, SY)] = 224
    places[(-1, -1)] = 240 + 7
    t2 = np.zeros((128, 256), np.float32)
    t4 = np.zeros((128, 256), np.float32)
    for x in range(SX):
        for y in range(SY):
            for dx in (-1, 0, 1):
                for dy in (-1, 0, 1):
                    place = places[(x + dx, y + dy)]
                    t2[x * SY + y, place] = (2 - abs(dx)) * (2 - abs(dy))
                    t4[x * SY + y, place] = (4 - 3 * abs(dx)) * (4 - 3 * abs(dy))
    pick = np.zeros((64, 128), np.float32)
    for x in range(SX):
        pick[x, x * SY] = 1.0
        pick[16 + x, x * SY + 7] = 1.0
    for y in range(SY):
        pick[32 + y, y] = 1.0
        pick[48 + y, 15 * SY + y] = 1.0
    return tz, sel, txy, t2, t4, np.ascontiguousarray(t2.T), pick


def local_kernel(
    v_hbm, mat, tz_ref, sel_ref, txy_ref, t2_ref, t4_ref, t2t_ref, pick_ref, out,
    vp, az, bz, ya, yb, xbufs, vts, xbuf, vt, coef, acc, zf, zs, zh, zface,
    own_sem, up_send, dn_send, up_recv, dn_recv, side_send, side_recv, z_send, z_recv,
    face_send, face_recv, zpiece_send, zpiece_recv,
    sym, core_in, *ring,
):
    core_send, core_recv, ring_send, ring_recv = ring[-4:]
    ring = ring[:-4]
    gx, gy, gz = lax.axis_index("gx"), lax.axis_index("gy"), lax.axis_index("gz")
    other = 1 - gz

    def at(dx, dy, z):
        return {"gx": lax.rem(gx + dx + 4, 4), "gy": lax.rem(gy + dy + 16, 16), "gz": z}

    around = [(dx, dy) for dx in (-1, 0, 1) for dy in (-1, 0, 1)]
    barrier = pltpu.get_barrier_semaphore()
    for dx, dy in around:
        if (dx, dy) != (0, 0):
            pl.semaphore_signal(barrier, inc=1, device_id=at(dx, dy, gz), device_id_type=MESH)
        pl.semaphore_signal(barrier, inc=1, device_id=at(dx, dy, other), device_id_type=MESH)

    core, z_lo = lax.rem(gx, 2), lax.div(gx, 2)
    ring_x, ring_y = lax.div(gy, 4), lax.rem(gy, 4)
    ring_z = 2 * gz + z_lo
    partner = {"gx": gx + 1 - 2 * core, "gy": gy, "gz": gz}

    def ring_place(dim, k):
        mine = {"x": ring_x, "y": ring_y, "z": ring_z}[dim]
        return lax.rem(mine + k, 4)

    def ring_peer(dim, k):
        spot = ring_place(dim, k)
        if dim == "x":
            return {"gx": gx, "gy": 4 * spot + ring_y, "gz": gz}
        if dim == "y":
            return {"gx": gx, "gy": 4 * ring_x + spot, "gz": gz}
        return {"gx": 2 * lax.rem(spot, 2) + core, "gy": gy, "gz": lax.div(spot, 2)}

    pl.semaphore_signal(barrier, inc=1, device_id=partner, device_id_type=MESH)
    for dim in "xyz":
        for k in (1, 2, 3):
            pl.semaphore_signal(barrier, inc=1, device_id=ring_peer(dim, k), device_id_type=MESH)

    def own_copy(x):
        return pltpu.make_async_copy(v_hbm.at[x], vp.at[x + 1, pl.ds(1, SY)], own_sem.at[x])

    @pl.loop(0, SX)
    def _(x):
        own_copy(x).start()

    def has(dx, dy):
        ok = jnp.bool_(True)
        if dx == 1:
            ok = jnp.logical_and(ok, gx < 3)
        if dx == -1:
            ok = jnp.logical_and(ok, gx > 0)
        if dy == 1:
            ok = jnp.logical_and(ok, gy < 15)
        if dy == -1:
            ok = jnp.logical_and(ok, gy > 0)
        return ok

    def remote(src, dst, send, recv, where):
        return pltpu.make_async_remote_copy(
            src_ref=src, dst_ref=dst, send_sem=send, recv_sem=recv, device_id=where, device_id_type=MESH
        )

    def up(x):
        return remote(v_hbm.at[x, SY - 1], vp.at[x + 1, 0], up_send.at[x], up_recv.at[x], at(0, 1, gz))

    def down(x):
        return remote(v_hbm.at[x, 0], vp.at[x + 1, PY - 1], dn_send.at[x], dn_recv.at[x], at(0, -1, gz))

    def side(index):
        dx, dy = sides[index]
        src_x = SX if dx == 1 else 1
        dst_x = 0 if dx == 1 else PX - 1
        row = 0 if dy == 1 else PY - 1
        return remote(
            vp.at[src_x, row], vp.at[dst_x, row], side_send.at[index], side_recv.at[index], at(dx, 0, gz)
        )

    def face(dx, row):
        index = 0 if dx == 1 else 1
        return remote(
            v_hbm.at[SX - 1 if dx == 1 else 0, row], vp.at[0 if dx == 1 else PX - 1, row + 1],
            face_send.at[index, row], face_recv.at[index, row], at(dx, 0, gz),
        )

    def side_sent(index):
        dx, dy = sides[index]
        return has(dx, -dy)

    sides = [(1, 1), (1, -1), (-1, 1), (-1, -1)]

    @pl.when(jnp.logical_not(has(0, -1)))
    def _():
        vp[:, 0] = jnp.zeros((PX, SZ, K), BF16)

    @pl.when(jnp.logical_not(has(0, 1)))
    def _():
        vp[:, PY - 1] = jnp.zeros((PX, SZ, K), BF16)

    @pl.when(jnp.logical_not(has(-1, 0)))
    def _():
        vp[0] = jnp.zeros((PY, SZ, K), BF16)

    @pl.when(jnp.logical_not(has(1, 0)))
    def _():
        vp[PX - 1] = jnp.zeros((PY, SZ, K), BF16)

    zrows = [(0, 0, 0, 128)]
    zrows += [(0, 1, 128, 16), (0, -1, 144, 16), (1, 0, 160, 16), (-1, 0, 176, 16)]
    zrows += [(1, 1, 192, 16), (1, -1, 208, 16), (-1, 1, 224, 16), (-1, -1, 240, 16)]
    for dx, dy, first, count in zrows[1:]:

        @pl.when(jnp.logical_not(has(dx, dy)))
        def _():
            zh[pl.ds(first, count)] = jnp.zeros((count, K), BF16)

    pl.semaphore_wait(barrier, 27)

    def send_plane(x):
        @pl.when(has(0, 1))
        def _():
            up(x).start()

        @pl.when(has(0, -1))
        def _():
            down(x).start()

    for n, x in enumerate((SX - 1, 0, 1, 2)):
        send_plane(x)
        for dx in (1, -1):

            @pl.when(has(dx, 0))
            def _():
                face(dx, 2 * n).start()
                face(dx, 2 * n + 1).start()

    pl.loop(3, 6)(send_plane)

    kappa = mat[0].reshape(SX * SY, SZ)
    rho = mat[1].reshape(SX * SY, SZ)
    own_kappa = lax.dot_general(kappa, sel_ref[...], DIM0, precision=HIGH, preferred_element_type=F32)
    own_rho = lax.dot_general(rho, sel_ref[...], DIM0, precision=HIGH, preferred_element_type=F32)
    near = lax.dot_general(kappa, txy_ref[...], DIM0, precision=HIGH, preferred_element_type=F32)
    edge_row = jnp.zeros((1, 256), F32)
    near = (
        jnp.concatenate([edge_row, near[:-1]], axis=0)
        + 2.0 * near
        + jnp.concatenate([near[1:], edge_row], axis=0)
    )
    alpha = 2.0 * own_kappa + near * (1.0 / 32.0)
    beta = own_kappa * (1.0 / 16.0)
    for xp in range(PX):
        span = slice(xp * PY, xp * PY + PY)
        coef[xp, 0, :, 0:PY] = alpha[:, span]
        coef[xp, 1, :, 0:PY] = beta[:, span]
        coef[xp, 2, :, 0:PY] = own_rho[:, span]

    @pl.loop(0, SX)
    def _(x):
        own_copy(x).wait()
        low = vp[x + 1, 1 : 1 + SY, 0:16, :].astype(F32)
        high = vp[x + 1, 1 : 1 + SY, SZ - 16 : SZ, :].astype(F32)
        spot = lax.broadcasted_iota(jnp.int32, (1, 16, 1), 1)
        low = jnp.sum(jnp.where(spot == 0, low, 0.0), axis=1)
        high = jnp.sum(jnp.where(spot == 15, high, 0.0), axis=1)
        zf[pl.ds(pl.multiple_of(x * SY, SY), SY)] = jnp.where(gz == 0, high, low)

    zface[...] = zf[...].astype(BF16)
    zs[...] = jnp.dot(pick_ref[...], zface[...], preferred_element_type=F32).astype(BF16)

    def zcopy(index, dx, dy):
        first, count = zrows[index][2:]
        if (dx, dy) == (0, 0):
            src = zface
        elif dx == 0:
            src = zs.at[pl.ds(16 if dy == 1 else 0, 16)]
        else:
            src = zs.at[pl.ds(48 if dx == 1 else 32, 16)]
        return remote(
            src, zh.at[pl.ds(first, count)], z_send.at[index], z_recv.at[index], at(dx, dy, other)
        )

    def zpiece(n):
        rows = pl.ds(16 * n, 16)
        return remote(
            zface.at[rows], zh.at[rows], zpiece_send.at[n], zpiece_recv.at[n], at(0, 0, other)
        )

    for n in range(8):
        zpiece(n).start()
        dx, dy = zrows[n + 1][:2]

        @pl.when(has(-dx, -dy))
        def _():
            zcopy(n + 1, -dx, -dy).start()

        send_plane(6 + n)
    send_plane(SX - 2)

    def wait_rows(x):
        @pl.when(has(0, -1))
        def _():
            up(x).wait_recv()

        @pl.when(has(0, 1))
        def _():
            down(x).wait_recv()

    wait_rows(SX - 1)
    wait_rows(0)
    for index in range(4):

        @pl.when(side_sent(index))
        def _():
            side(index).start()

    acc[...] = jnp.zeros_like(acc)

    def wait_sides(toward):
        @pl.when(has(-toward, 0))
        def _():
            for row in range(SY):
                face(toward, row).wait_recv()

        for index in (0, 1) if toward == 1 else (2, 3):
            dx, dy = sides[index]

            @pl.when(has(-dx, -dy))
            def _():
                side(index).wait_recv()

    def plane_stage(xp, slot):
        for b in range(2):
            for c in range(2):
                lanes = slice(256 * c, 256 * c + 256)
                own = vp[xp, HALF * b : HALF * b + HALF, :, lanes]
                a = jnp.dot(
                    tz_ref[...], own.reshape(HALF * SZ, 256), preferred_element_type=F32
                ).astype(BF16).reshape(HALF, SZ, 256)
                az[slot % 2][HALF * b : HALF * b + HALF, :, lanes] = a
                bz[slot % 2][HALF * b : HALF * b + HALF, :, lanes] = a + (own + own)
        for c in range(2):
            lanes = slice(256 * c, 256 * c + 256)
            a, b = az[slot % 2], bz[slot % 2]
            pair = a[0, :, lanes] + a[1, :, lanes]
            for y in range(SY):
                nxt = a[y + 1, :, lanes] + a[y + 2, :, lanes]
                ya[slot][y, :, lanes] = pair + nxt
                pair = nxt
                yb[slot][y, :, lanes] = (b[y, :, lanes] + b[y + 2, :, lanes]) + BF16(4.0) * b[y + 1, :, lanes]

    def cell_pair(x, slots, side_by):
        x_out, v_out = xbufs[side_by], vts[side_by]
        for y in range(SY):
            cols = [
                [coef[x + 1 + i, n, :, y + 1 : y + 2] for n in range(3)] for i in range(2)
            ]
            for c in range(2):
                lanes = slice(256 * c, 256 * c + 256)
                stage = [ya[n][y, :, lanes] for n in slots]
                sums = [stage[i] + stage[i + 1] for i in range(3)]
                other_stage = [yb[n][y, :, lanes] for n in slots]
                for i in range(2):
                    al, be, ro = cols[i]
                    row = pl.ds(SY * SZ * i + y * SZ, SZ)
                    u = (sums[i] + sums[i + 1]).astype(F32)
                    own = vp[x + 1 + i, y + 1, :, lanes].astype(F32)
                    x_out[row, 256 * c : 256 * c + 256] = (al * own - be * u).astype(BF16)
                    m = (other_stage[i] + other_stage[i + 2]) + BF16(4.0) * other_stage[i + 1]
                    x_out[row, K + 256 * c : K + 256 * c + 256] = (ro * m.astype(F32)).astype(BF16)
        for i in range(2):
            for n, yp in enumerate((0, PY - 1)):
                row = pl.ds(2 * SY * SZ + (2 * i + n) * SZ, SZ)
                x_out[row, 0:K] = halo_rows(x + 1 + i, yp).astype(BF16)
        for i in range(2):
            v_out[:, SY * SZ * i : SY * SZ * i + SY * SZ] = (
                vp[x + 1 + i, 1 : 1 + SY].reshape(SY * SZ, K).T
            )
        sides_of = jnp.concatenate([vp[x + 1 + i, yp] for i in range(2) for yp in (0, PY - 1)], axis=0)
        v_out[:, 2 * SY * SZ : 2 * SY * SZ + 4 * SZ] = sides_of.T

    def gram_pair(side_by, halves=(0, 1)):
        x_in, v_in = xbufs[side_by], vts[side_by]
        for c in halves:
            lanes = slice(K * c, K * c + K)
            depth = 2 * SY * SZ if c else PAIR_ROWS
            acc[:, lanes] += jnp.dot(
                v_in[:, 0:depth], x_in[0:depth, lanes], preferred_element_type=F32
            )

    def halo_rows(xp, yp):
        return coef[xp, 0, :, yp : yp + 1] * vp[xp, yp].astype(F32)

    def side_products():
        for xp in (0, PX - 1):
            for y in range(PY):
                xbuf[y * SZ : y * SZ + SZ, 0:K] = halo_rows(xp, y).astype(BF16)
            vt[...] = vp[xp].reshape(PY * SZ, K).T
            for c in range(2):
                lanes = slice(256 * c, 256 * c + 256)
                acc[:, lanes] += jnp.dot(vt[...], xbuf[:, lanes], preferred_element_type=F32)
    def z_products():
        for n in range(8):
            zpiece(n).wait_recv()
            dx, dy = zrows[n + 1][:2]

            @pl.when(has(dx, dy))
            def _():
                zcopy(n + 1, -dx, -dy).wait_recv()

        lane = lax.broadcasted_iota(jnp.int32, (SX * SY, SZ), 1)
        at_edge = lane == jnp.where(gz == 0, SZ - 1, 0)
        kappa_edge = jnp.sum(
            jnp.where(at_edge, mat[0].reshape(SX * SY, SZ), 0.0), axis=1, keepdims=True
        )
        rho_edge = jnp.sum(
            jnp.where(at_edge, mat[1].reshape(SX * SY, SZ), 0.0), axis=1, keepdims=True
        )
        far = zh[...]
        du = jnp.dot(t2_ref[...], far, preferred_element_type=F32)
        dm = jnp.dot(t4_ref[...], far, preferred_element_type=F32)
        xbuf[0:128, 0:K] = (kappa_edge * (-1.0 / 16.0) * du).astype(BF16)
        xbuf[0:128, K : 2 * K] = (rho_edge * dm).astype(BF16)
        reach = jnp.dot(
            t2t_ref[...], jnp.broadcast_to(kappa_edge, (128, 128)), precision=HIGH, preferred_element_type=F32
        ) * (1.0 / 32.0)
        for c in range(4):
            lanes = slice(128 * c, 128 * c + 128)
            xbuf[128:384, lanes] = (reach * far[:, lanes].astype(F32)).astype(BF16)
        vt[:, 0:128] = zface[...].T
        vt[:, 128:384] = far.T
        for c in range(4):
            lanes = slice(256 * c, 256 * c + 256)
            depth = 384 if c < 2 else 128
            acc[:, lanes] += jnp.dot(vt[:, 0:depth], xbuf[0:depth, lanes], preferred_element_type=F32)

    for ref in (xbufs[1], vts[1]):
        ref[...] = jnp.zeros_like(ref)
    plane_stage(1, 1)
    for n in (2, 3):
        wait_rows(n - 1)
        plane_stage(n, n)
    wait_sides(1)
    plane_stage(0, 0)

    @pl.loop(0, 3)
    def _(t):
        x = 4 * t
        for half in range(2):
            gram_pair(1 - half)
            cell_pair(x + 2 * half, (0, 1, 2, 3) if half == 0 else (2, 3, 0, 1), half)
            for n in range(2):
                wait_rows(x + 2 * half + 3 + n)
            for n in range(2):
                plane_stage(x + 2 * half + 4 + n, 2 * half + n)

        @pl.when(t == 1)
        def _():
            wait_sides(-1)
            side_products()
            plane_stage(SX, 4)
            plane_stage(SX + 1, 5)

    z_products()
    gram_pair(1)
    cell_pair(12, (0, 1, 2, 3), 0)
    gram_pair(0)
    cell_pair(14, (2, 3, 4, 5), 1)

    def core_copy(c):
        first, width = COLORS[c]
        cols = pl.ds(first, width)
        return remote(
            sym.at[1 - core, :, :, :, :, :, cols], core_in.at[:, :, :, :, :, cols],
            core_send.at[c], core_recv.at[c], partner,
        )

    def put(gx_row, col, block):
        for part in range(32):
            sym[
                gx_row % 2, gx_row // 2, part // 8, part // 2 % 4, part % 2, :, col : col + 128
            ] = block[4 * part : 4 * part + 4]

    for half, scale in ((0, 0.5 / CELLS), (1, 0.5 / (216.0 * CELLS))):
        gram_pair(1, (half,))
        for i in range(4):
            for j in range(i, 4):
                rows = slice(128 * i, 128 * i + 128)
                cols = slice(128 * j, 128 * j + 128)
                there = slice(K * half + 128 * j, K * half + 128 * j + 128)
                back = slice(K * half + 128 * i, K * half + 128 * i + 128)
                both = (acc[rows, there] + acc[cols, back].T) * scale
                put(i, K * half + 128 * j, both)
                if i != j:
                    put(j, K * half + 128 * i, both.T)
        if half == 0:
            core_copy(0).start()
        else:
            core_copy(1).start()
            core_copy(2).start()

    held = [[ring[6 * c + 2 * s] for s in range(3)] for c in range(3)]
    landed = [[ring[6 * c + 2 * s + 1] for s in range(3)] for c in range(3)]

    def piece(c, s, spot):
        ref, dim, left = held[c][s], ORDERS[c][s], ORDERS[c][s:]
        index = []
        for name in ("z_lo", "x", "y", "z_hi"):
            if name[0] not in left:
                continue
            if name[0] != dim:
                index.append(slice(None))
            elif name == "z_lo":
                index.append(lax.rem(spot, 2))
            elif name == "z_hi":
                index.append(lax.div(spot, 2))
            else:
                index.append(spot)
        return ref.at[tuple(index)]

    def ring_copies(c, s, ks):
        dim = ORDERS[c][s]
        copies = []
        for part in range(2 if s == 0 else 1):
            for k in ks:
                src, dst = piece(c, s, ring_place(dim, k)), landed[c][s].at[k - 1]
                if s == 0:
                    rows = pl.ds(part * (dst.shape[0] // 2), dst.shape[0] // 2)
                    src, dst = src.at[rows], dst.at[rows]
                number = 12 * c + (6 * part + k - 1 if s == 0 else 3 + 6 * (s - 1) + k - 1)
                copies.append(
                    remote(src, dst, ring_send.at[number], ring_recv.at[number], ring_peer(dim, k))
                )
        return copies

    for c in range(3):
        first, width = COLORS[c]
        cols = slice(first, first + width)
        core_copy(c).wait_recv()
        for zl in range(2):
            for x in range(4):
                held[c][0][zl, x] = sym[core, zl, x, :, :, :, cols] + core_in[zl, x, :, :, :, cols]
        for copy in ring_copies(c, 0, (2, 1, 3)):
            copy.start()
    for s in range(3):
        for c in range(3):
            first, width = COLORS[c]
            for copy in ring_copies(c, s, (1, 3, 2)):
                copy.wait_recv()
            total = piece(c, s, ring_place(ORDERS[c][s], 0))[...]
            for k in (1, 3, 2):
                total = total + landed[c][s][k - 1]
            if s < 2:
                held[c][s + 1][...] = total
                for copy in ring_copies(c, s + 1, (2, 1, 3)):
                    copy.start()
            else:
                for tile in range(width // 128):
                    col = first + 128 * tile
                    part = total[:, 128 * tile : 128 * tile + 128]
                    out[:, col : col + 128] = part
    for c in range(3):
        core_copy(c).wait_send()
        for s in range(3):
            for copy in ring_copies(c, s, (1, 2, 3)):
                copy.wait_send()

    @pl.loop(0, SX)
    def _(x):
        @pl.when(has(0, 1))
        def _():
            up(x).wait_send()

        @pl.when(has(0, -1))
        def _():
            down(x).wait_send()

    for index in range(4):

        @pl.when(side_sent(index))
        def _():
            side(index).wait_send()

    for dx in (1, -1):

        @pl.when(has(dx, 0))
        def _():
            for row in range(SY):
                face(dx, row).wait_send()

    for n in range(8):
        zpiece(n).wait_send()
        dx, dy = zrows[n + 1][:2]

        @pl.when(has(-dx, -dy))
        def _():
            zcopy(n + 1, -dx, -dy).wait_send()


def ring_buffers():
    buffers = []
    for (_, width), order in zip(COLORS, ORDERS):
        for s in range(3):
            left = [n for d, n in (("z", 2), ("x", 4), ("y", 4), ("z", 2)) if d in order[s:]]
            after = [n for d, n in (("z", 2), ("x", 4), ("y", 4), ("z", 2)) if d in order[s + 1 :]]
            buffers.append(pltpu.VMEM((*left, 4, width), F32))
            buffers.append(pltpu.VMEM((3, *after, 4, width), F32))
    return buffers


def local_products(eigvecs, material):
    tz, sel, txy, t2, t4, t2t, pick = constants()
    small = (
        jnp.asarray(tz, BF16), jnp.asarray(sel), jnp.asarray(txy), jnp.asarray(t2, BF16),
        jnp.asarray(t4, BF16), jnp.asarray(t2t), jnp.asarray(pick, BF16),
    )
    vmem = pl.BlockSpec(memory_space=pltpu.VMEM)
    dma = pltpu.SemaphoreType.DMA
    return pl.pallas_call(
        local_kernel,
        out_shape=jax.ShapeDtypeStruct((4, 2 * K), F32),
        in_specs=[pl.BlockSpec(memory_space=pl.ANY)] + [vmem] * 8,
        out_specs=vmem,
        scratch_shapes=[
            pltpu.VMEM((PX, PY, SZ, K), BF16),
            [pltpu.VMEM((PY, SZ, K), BF16)] * 2,
            [pltpu.VMEM((PY, SZ, K), BF16)] * 2,
            [pltpu.VMEM((SY, SZ, K), BF16)] * 6,
            [pltpu.VMEM((SY, SZ, K), BF16)] * 6,
            [pltpu.VMEM((PAIR_ROWS, 2 * K), BF16)] * 2,
            [pltpu.VMEM((K, PAIR_ROWS), BF16)] * 2,
            pltpu.VMEM((PY * SZ, 2 * K), BF16),
            pltpu.VMEM((K, PY * SZ), BF16),
            pltpu.VMEM((PX, 3, SZ, 128), F32),
            pltpu.VMEM((K, 2 * K), F32),
            pltpu.VMEM((SX * SY, K), F32),
            pltpu.VMEM((64, K), BF16),
            pltpu.VMEM((256, K), BF16),
            pltpu.VMEM((SX * SY, K), BF16),
            dma((SX,)), dma((SX,)), dma((SX,)), dma((SX,)), dma((SX,)),
            dma((4,)), dma((4,)), dma((9,)), dma((9,)),
            dma((2, SY)), dma((2, SY)), dma((8,)), dma((8,)),
            pltpu.VMEM((2, 2, 4, 4, 2, 4, 2 * K), F32),
            pltpu.VMEM((2, 4, 4, 2, 4, 2 * K), F32),
            *ring_buffers(),
            dma((3,)), dma((3,)), dma((36,)), dma((36,)),
        ],
        compiler_params=pltpu.CompilerParams(
            collective_id=0, has_side_effects=True, vmem_limit_bytes=60 * 1024 * 1024
        ),
    )(eigvecs, material, *small)


def per_device(eigvecs, material):
    both = local_products(eigvecs, material)
    return both[:, :K], both[:, K:]


def solution(mesh):
    return jax.shard_map(
        per_device,
        mesh=mesh,
        in_specs=(P("gx", "gy", "gz", None), P(None, "gx", "gy", "gz")),
        out_specs=(P(("gx", "gy", "gz"), None), P(("gx", "gy", "gz"), None)),
        check_vma=False,
    )
```

```python
import functools

import jax
import jax.numpy as jnp
import numpy as np
from jax import lax
from jax.experimental import pallas as pl
from jax.experimental.pallas import tpu as pltpu
from jax.sharding import PartitionSpec as P

MESH = pl.DeviceIdType.MESH
F32 = jnp.float32
BF16 = jnp.bfloat16
HIGH = lax.Precision.HIGHEST

SX, SY, SZ, K = 16, 8, 48, 512
PX, PY = SX + 2, SY + 2
HALF = PY // 2
PAIR_ROWS = 2 * SY * SZ + 4 * SZ
CELLS = 64 * 128 * 96
DIM0 = (((0,), (0,)), ((), ()))
COLORS = ((0, 384), (384, 384), (768, 256))
ORDERS = ("xyz", "yzx", "zxy")


def constants():
    rows = HALF * SZ
    tz = np.zeros((rows, rows), np.float32)
    for r in range(rows):
        for c in (r - 1, r, r + 1):
            if 0 <= c < rows and c // SZ == r // SZ:
                tz[r, c] = 2.0 if c == r else 1.0
    sel = np.zeros((SX * SY, 256), np.float32)
    txy = np.zeros((SX * SY, 256), np.float32)
    for x in range(SX):
        for y in range(SY):
            row = x * SY + y
            sel[row, (x + 1) * PY + y + 1] = 1.0
            for dx in (-1, 0, 1):
                for dy in (-1, 0, 1):
                    txy[row, (x + 1 + dx) * PY + y + 1 + dy] = (2 - abs(dx)) * (2 - abs(dy))
    places = {}
    for x in range(SX):
        for y in range(SY):
            places[(x, y)] = x * SY + y
    for x in range(SX):
        places[(x, SY)] = 128 + x
        places[(x, -1)] = 144 + x
    for y in range(SY):
        places[(SX, y)] = 160 + y
        places[(-1, y)] = 176 + y
    places[(SX, SY)] = 192
    places[(SX, -1)] = 208 + 7
    places[(-1, SY)] = 224
    places[(-1, -1)] = 240 + 7
    t2 = np.zeros((128, 256), np.float32)
    t4 = np.zeros((128, 256), np.float32)
    for x in range(SX):
        for y in range(SY):
            for dx in (-1, 0, 1):
                for dy in (-1, 0, 1):
                    place = places[(x + dx, y + dy)]
                    t2[x * SY + y, place] = (2 - abs(dx)) * (2 - abs(dy))
                    t4[x * SY + y, place] = (4 - 3 * abs(dx)) * (4 - 3 * abs(dy))
    pick = np.zeros((64, 128), np.float32)
    for x in range(SX):
        pick[x, x * SY] = 1.0
        pick[16 + x, x * SY + 7] = 1.0
    for y in range(SY):
        pick[32 + y, y] = 1.0
        pick[48 + y, 15 * SY + y] = 1.0
    return tz, sel, txy, t2, t4, np.ascontiguousarray(t2.T), pick


def local_kernel(
    v_hbm, mat, tz_ref, sel_ref, txy_ref, t2_ref, t4_ref, t2t_ref, pick_ref, out,
    vp, az, bz, ya, yb, xbufs, vts, xbuf, vt, coef, acc, zf, zs, zh, zface,
    own_sem, up_send, dn_send, up_recv, dn_recv, side_send, side_recv, z_send, z_recv,
    face_send, face_recv, zpiece_send, zpiece_recv,
    sym, core_in, *ring,
):
    core_send, core_recv, ring_send, ring_recv = ring[-4:]
    ring = ring[:-4]
    gx, gy, gz = lax.axis_index("gx"), lax.axis_index("gy"), lax.axis_index("gz")
    other = 1 - gz

    def at(dx, dy, z):
        return {"gx": lax.rem(gx + dx + 4, 4), "gy": lax.rem(gy + dy + 16, 16), "gz": z}

    around = [(dx, dy) for dx in (-1, 0, 1) for dy in (-1, 0, 1)]
    barrier = pltpu.get_barrier_semaphore()
    for dx, dy in around:
        if (dx, dy) != (0, 0):
            pl.semaphore_signal(barrier, inc=1, device_id=at(dx, dy, gz), device_id_type=MESH)
        pl.semaphore_signal(barrier, inc=1, device_id=at(dx, dy, other), device_id_type=MESH)

    core, z_lo = lax.rem(gx, 2), lax.div(gx, 2)
    ring_x, ring_y = lax.div(gy, 4), lax.rem(gy, 4)
    ring_z = 2 * gz + z_lo
    partner = {"gx": gx + 1 - 2 * core, "gy": gy, "gz": gz}

    def ring_place(dim, k):
        mine = {"x": ring_x, "y": ring_y, "z": ring_z}[dim]
        return lax.rem(mine + k, 4)

    def ring_peer(dim, k):
        spot = ring_place(dim, k)
        if dim == "x":
            return {"gx": gx, "gy": 4 * spot + ring_y, "gz": gz}
        if dim == "y":
            return {"gx": gx, "gy": 4 * ring_x + spot, "gz": gz}
        return {"gx": 2 * lax.rem(spot, 2) + core, "gy": gy, "gz": lax.div(spot, 2)}

    pl.semaphore_signal(barrier, inc=1, device_id=partner, device_id_type=MESH)
    for dim in "xyz":
        for k in (1, 2, 3):
            pl.semaphore_signal(barrier, inc=1, device_id=ring_peer(dim, k), device_id_type=MESH)

    def own_copy(x):
        return pltpu.make_async_copy(v_hbm.at[x], vp.at[x + 1, pl.ds(1, SY)], own_sem.at[x])

    @pl.loop(0, SX)
    def _(x):
        own_copy(x).start()

    def has(dx, dy):
        ok = jnp.bool_(True)
        if dx == 1:
            ok = jnp.logical_and(ok, gx < 3)
        if dx == -1:
            ok = jnp.logical_and(ok, gx > 0)
        if dy == 1:
            ok = jnp.logical_and(ok, gy < 15)
        if dy == -1:
            ok = jnp.logical_and(ok, gy > 0)
        return ok

    def remote(src, dst, send, recv, where):
        return pltpu.make_async_remote_copy(
            src_ref=src, dst_ref=dst, send_sem=send, recv_sem=recv, device_id=where, device_id_type=MESH
        )

    def up(x):
        return remote(v_hbm.at[x, SY - 1], vp.at[x + 1, 0], up_send.at[x], up_recv.at[x], at(0, 1, gz))

    def down(x):
        return remote(v_hbm.at[x, 0], vp.at[x + 1, PY - 1], dn_send.at[x], dn_recv.at[x], at(0, -1, gz))

    def side(index):
        dx, dy = sides[index]
        src_x = SX if dx == 1 else 1
        dst_x = 0 if dx == 1 else PX - 1
        row = 0 if dy == 1 else PY - 1
        return remote(
            vp.at[src_x, row], vp.at[dst_x, row], side_send.at[index], side_recv.at[index], at(dx, 0, gz)
        )

    def face(dx, row):
        index = 0 if dx == 1 else 1
        return remote(
            v_hbm.at[SX - 1 if dx == 1 else 0, row], vp.at[0 if dx == 1 else PX - 1, row + 1],
            face_send.at[index, row], face_recv.at[index, row], at(dx, 0, gz),
        )

    def side_sent(index):
        dx, dy = sides[index]
        return has(dx, -dy)

    sides = [(1, 1), (1, -1), (-1, 1), (-1, -1)]

    @pl.when(jnp.logical_not(has(0, -1)))
    def _():
        vp[:, 0] = jnp.zeros((PX, SZ, K), BF16)

    @pl.when(jnp.logical_not(has(0, 1)))
    def _():
        vp[:, PY - 1] = jnp.zeros((PX, SZ, K), BF16)

    @pl.when(jnp.logical_not(has(-1, 0)))
    def _():
        vp[0] = jnp.zeros((PY, SZ, K), BF16)

    @pl.when(jnp.logical_not(has(1, 0)))
    def _():
        vp[PX - 1] = jnp.zeros((PY, SZ, K), BF16)

    zrows = [(0, 0, 0, 128)]
    zrows += [(0, 1, 128, 16), (0, -1, 144, 16), (1, 0, 160, 16), (-1, 0, 176, 16)]
    zrows += [(1, 1, 192, 16), (1, -1, 208, 16), (-1, 1, 224, 16), (-1, -1, 240, 16)]
    for dx, dy, first, count in zrows[1:]:

        @pl.when(jnp.logical_not(has(dx, dy)))
        def _():
            zh[pl.ds(first, count)] = jnp.zeros((count, K), BF16)

    pl.semaphore_wait(barrier, 27)

    def send_plane(x):
        @pl.when(has(0, 1))
        def _():
            up(x).start()

        @pl.when(has(0, -1))
        def _():
            down(x).start()

    for n, x in enumerate((SX - 1, 0, 1, 2)):
        send_plane(x)
        for dx in (1, -1):

            @pl.when(has(dx, 0))
            def _():
                face(dx, 2 * n).start()
                face(dx, 2 * n + 1).start()

    send_plane(3)

    kappa = mat[0].reshape(SX * SY, SZ)
    rho = mat[1].reshape(SX * SY, SZ)
    own_kappa = lax.dot_general(kappa, sel_ref[...], DIM0, precision=HIGH, preferred_element_type=F32)
    own_rho = lax.dot_general(rho, sel_ref[...], DIM0, precision=HIGH, preferred_element_type=F32)
    near = lax.dot_general(kappa, txy_ref[...], DIM0, precision=HIGH, preferred_element_type=F32)
    edge_row = jnp.zeros((1, 256), F32)
    near = (
        jnp.concatenate([edge_row, near[:-1]], axis=0)
        + 2.0 * near
        + jnp.concatenate([near[1:], edge_row], axis=0)
    )
    alpha = 2.0 * own_kappa + near * (1.0 / 32.0)
    beta = own_kappa * (1.0 / 16.0)
    for xp in range(PX):
        span = slice(xp * PY, xp * PY + PY)
        coef[xp, 0, :, 0:PY] = alpha[:, span]
        coef[xp, 1, :, 0:PY] = beta[:, span]
        coef[xp, 2, :, 0:PY] = own_rho[:, span]

    def wait_rows(x):
        @pl.when(has(0, -1))
        def _():
            up(x).wait_recv()

        @pl.when(has(0, 1))
        def _():
            down(x).wait_recv()

    wait_rows(SX - 1)
    wait_rows(0)
    for index in range(4):

        @pl.when(side_sent(index))
        def _():
            side(index).start()

    send_plane(4)
    send_plane(5)

    @pl.loop(0, SX)
    def _(x):
        own_copy(x).wait()
        low = vp[x + 1, 1 : 1 + SY, 0:16, :].astype(F32)
        high = vp[x + 1, 1 : 1 + SY, SZ - 16 : SZ, :].astype(F32)
        spot = lax.broadcasted_iota(jnp.int32, (1, 16, 1), 1)
        low = jnp.sum(jnp.where(spot == 0, low, 0.0), axis=1)
        high = jnp.sum(jnp.where(spot == 15, high, 0.0), axis=1)
        zf[pl.ds(pl.multiple_of(x * SY, SY), SY)] = jnp.where(gz == 0, high, low)

    zface[...] = zf[...].astype(BF16)
    zs[...] = jnp.dot(pick_ref[...], zface[...], preferred_element_type=F32).astype(BF16)

    def zcopy(index, dx, dy):
        first, count = zrows[index][2:]
        if (dx, dy) == (0, 0):
            src = zface
        elif dx == 0:
            src = zs.at[pl.ds(16 if dy == 1 else 0, 16)]
        else:
            src = zs.at[pl.ds(48 if dx == 1 else 32, 16)]
        return remote(
            src, zh.at[pl.ds(first, count)], z_send.at[index], z_recv.at[index], at(dx, dy, other)
        )

    def zpiece(n):
        rows = pl.ds(16 * n, 16)
        return remote(
            zface.at[rows], zh.at[rows], zpiece_send.at[n], zpiece_recv.at[n], at(0, 0, other)
        )

    for n in range(8):
        zpiece(n).start()
        dx, dy = zrows[n + 1][:2]

        @pl.when(has(-dx, -dy))
        def _():
            zcopy(n + 1, -dx, -dy).start()

        send_plane(6 + n)
    send_plane(SX - 2)

    acc[...] = jnp.zeros_like(acc)

    def wait_sides(toward):
        @pl.when(has(-toward, 0))
        def _():
            for row in range(SY):
                face(toward, row).wait_recv()

        for index in (0, 1) if toward == 1 else (2, 3):
            dx, dy = sides[index]

            @pl.when(has(-dx, -dy))
            def _():
                side(index).wait_recv()

    def plane_stage(xp, slot):
        for b in range(2):
            for c in range(2):
                lanes = slice(256 * c, 256 * c + 256)
                own = vp[xp, HALF * b : HALF * b + HALF, :, lanes]
                a = jnp.dot(
                    tz_ref[...], own.reshape(HALF * SZ, 256), preferred_element_type=F32
                ).astype(BF16).reshape(HALF, SZ, 256)
                az[slot % 2][HALF * b : HALF * b + HALF, :, lanes] = a
                bz[slot % 2][HALF * b : HALF * b + HALF, :, lanes] = a + (own + own)
        for c in range(2):
            lanes = slice(256 * c, 256 * c + 256)
            a, b = az[slot % 2], bz[slot % 2]
            pair = a[0, :, lanes] + a[1, :, lanes]
            for y in range(SY):
                nxt = a[y + 1, :, lanes] + a[y + 2, :, lanes]
                ya[slot][y, :, lanes] = pair + nxt
                pair = nxt
                yb[slot][y, :, lanes] = (b[y, :, lanes] + b[y + 2, :, lanes]) + BF16(4.0) * b[y + 1, :, lanes]

    def cell_pair(x, slots, side_by):
        x_out, v_out = xbufs[side_by], vts[side_by]
        for y in range(SY):
            cols = [
                [coef[x + 1 + i, n, :, y + 1 : y + 2] for n in range(3)] for i in range(2)
            ]
            for c in range(2):
                lanes = slice(256 * c, 256 * c + 256)
                stage = [ya[n][y, :, lanes] for n in slots]
                sums = [stage[i] + stage[i + 1] for i in range(3)]
                other_stage = [yb[n][y, :, lanes] for n in slots]
                for i in range(2):
                    al, be, ro = cols[i]
                    row = pl.ds(SY * SZ * i + y * SZ, SZ)
                    u = (sums[i] + sums[i + 1]).astype(F32)
                    own = vp[x + 1 + i, y + 1, :, lanes].astype(F32)
                    x_out[row, 256 * c : 256 * c + 256] = (al * own - be * u).astype(BF16)
                    m = (other_stage[i] + other_stage[i + 2]) + BF16(4.0) * other_stage[i + 1]
                    x_out[row, K + 256 * c : K + 256 * c + 256] = (ro * m.astype(F32)).astype(BF16)
        for i in range(2):
            for n, yp in enumerate((0, PY - 1)):
                row = pl.ds(2 * SY * SZ + (2 * i + n) * SZ, SZ)
                x_out[row, 0:K] = halo_rows(x + 1 + i, yp).astype(BF16)
        for i in range(2):
            v_out[:, SY * SZ * i : SY * SZ * i + SY * SZ] = (
                vp[x + 1 + i, 1 : 1 + SY].reshape(SY * SZ, K).T
            )
        sides_of = jnp.concatenate([vp[x + 1 + i, yp] for i in range(2) for yp in (0, PY - 1)], axis=0)
        v_out[:, 2 * SY * SZ : 2 * SY * SZ + 4 * SZ] = sides_of.T

    def gram_pair(side_by, halves=(0, 1)):
        x_in, v_in = xbufs[side_by], vts[side_by]
        for c in halves:
            lanes = slice(K * c, K * c + K)
            depth = 2 * SY * SZ if c else PAIR_ROWS
            acc[:, lanes] += jnp.dot(
                v_in[:, 0:depth], x_in[0:depth, lanes], preferred_element_type=F32
            )

    def halo_rows(xp, yp):
        return coef[xp, 0, :, yp : yp + 1] * vp[xp, yp].astype(F32)

    def side_products():
        for xp in (0, PX - 1):
            for y in range(PY):
                xbuf[y * SZ : y * SZ + SZ, 0:K] = halo_rows(xp, y).astype(BF16)
            vt[...] = vp[xp].reshape(PY * SZ, K).T
            for c in range(2):
                lanes = slice(256 * c, 256 * c + 256)
                acc[:, lanes] += jnp.dot(vt[...], xbuf[:, lanes], preferred_element_type=F32)
    def z_products():
        for n in range(8):
            zpiece(n).wait_recv()
            dx, dy = zrows[n + 1][:2]

            @pl.when(has(dx, dy))
            def _():
                zcopy(n + 1, -dx, -dy).wait_recv()

        lane = lax.broadcasted_iota(jnp.int32, (SX * SY, SZ), 1)
        at_edge = lane == jnp.where(gz == 0, SZ - 1, 0)
        kappa_edge = jnp.sum(
            jnp.where(at_edge, mat[0].reshape(SX * SY, SZ), 0.0), axis=1, keepdims=True
        )
        rho_edge = jnp.sum(
            jnp.where(at_edge, mat[1].reshape(SX * SY, SZ), 0.0), axis=1, keepdims=True
        )
        far = zh[...]
        du = jnp.dot(t2_ref[...], far, preferred_element_type=F32)
        dm = jnp.dot(t4_ref[...], far, preferred_element_type=F32)
        xbuf[0:128, 0:K] = (kappa_edge * (-1.0 / 16.0) * du).astype(BF16)
        xbuf[0:128, K : 2 * K] = (rho_edge * dm).astype(BF16)
        reach = jnp.dot(
            t2t_ref[...], jnp.broadcast_to(kappa_edge, (128, 128)), precision=HIGH, preferred_element_type=F32
        ) * (1.0 / 32.0)
        for c in range(4):
            lanes = slice(128 * c, 128 * c + 128)
            xbuf[128:384, lanes] = (reach * far[:, lanes].astype(F32)).astype(BF16)
        vt[:, 0:128] = zface[...].T
        vt[:, 128:384] = far.T
        for c in range(4):
            lanes = slice(256 * c, 256 * c + 256)
            depth = 384 if c < 2 else 128
            acc[:, lanes] += jnp.dot(vt[:, 0:depth], xbuf[0:depth, lanes], preferred_element_type=F32)

    for ref in (xbufs[1], vts[1]):
        ref[...] = jnp.zeros_like(ref)
    plane_stage(1, 1)
    for n in (2, 3):
        wait_rows(n - 1)
        plane_stage(n, n)
    wait_sides(1)
    plane_stage(0, 0)

    @pl.loop(0, 3)
    def _(t):
        x = 4 * t
        for half in range(2):
            gram_pair(1 - half)
            cell_pair(x + 2 * half, (0, 1, 2, 3) if half == 0 else (2, 3, 0, 1), half)
            for n in range(2):
                wait_rows(x + 2 * half + 3 + n)
            for n in range(2):
                plane_stage(x + 2 * half + 4 + n, 2 * half + n)

        @pl.when(t == 1)
        def _():
            wait_sides(-1)
            side_products()
            plane_stage(SX, 4)
            plane_stage(SX + 1, 5)

    z_products()
    gram_pair(1)
    cell_pair(12, (0, 1, 2, 3), 0)
    gram_pair(0)
    cell_pair(14, (2, 3, 4, 5), 1)

    def core_copy(c):
        first, width = COLORS[c]
        cols = pl.ds(first, width)
        return remote(
            sym.at[1 - core, :, :, :, :, :, cols], core_in.at[:, :, :, :, :, cols],
            core_send.at[c], core_recv.at[c], partner,
        )

    def put(gx_row, col, block):
        for part in range(32):
            sym[
                gx_row % 2, gx_row // 2, part // 8, part // 2 % 4, part % 2, :, col : col + 128
            ] = block[4 * part : 4 * part + 4]

    for half, scale in ((0, 0.5 / CELLS), (1, 0.5 / (216.0 * CELLS))):
        gram_pair(1, (half,))
        for i in range(4):
            for j in range(i, 4):
                rows = slice(128 * i, 128 * i + 128)
                cols = slice(128 * j, 128 * j + 128)
                there = slice(K * half + 128 * j, K * half + 128 * j + 128)
                back = slice(K * half + 128 * i, K * half + 128 * i + 128)
                both = (acc[rows, there] + acc[cols, back].T) * scale
                put(i, K * half + 128 * j, both)
                if i != j:
                    put(j, K * half + 128 * i, both.T)
        if half == 0:
            core_copy(0).start()
        else:
            core_copy(1).start()
            core_copy(2).start()

    held = [[ring[6 * c + 2 * s] for s in range(3)] for c in range(3)]
    landed = [[ring[6 * c + 2 * s + 1] for s in range(3)] for c in range(3)]

    def piece(c, s, spot):
        ref, dim, left = held[c][s], ORDERS[c][s], ORDERS[c][s:]
        index = []
        for name in ("z_lo", "x", "y", "z_hi"):
            if name[0] not in left:
                continue
            if name[0] != dim:
                index.append(slice(None))
            elif name == "z_lo":
                index.append(lax.rem(spot, 2))
            elif name == "z_hi":
                index.append(lax.div(spot, 2))
            else:
                index.append(spot)
        return ref.at[tuple(index)]

    def ring_copies(c, s, ks):
        dim = ORDERS[c][s]
        copies = []
        for part in range(2 if s == 0 else 1):
            for k in ks:
                src, dst = piece(c, s, ring_place(dim, k)), landed[c][s].at[k - 1]
                if s == 0:
                    rows = pl.ds(part * (dst.shape[0] // 2), dst.shape[0] // 2)
                    src, dst = src.at[rows], dst.at[rows]
                number = 12 * c + (6 * part + k - 1 if s == 0 else 3 + 6 * (s - 1) + k - 1)
                copies.append(
                    remote(src, dst, ring_send.at[number], ring_recv.at[number], ring_peer(dim, k))
                )
        return copies

    for c in range(3):
        first, width = COLORS[c]
        cols = slice(first, first + width)
        core_copy(c).wait_recv()
        for zl in range(2):
            for x in range(4):
                held[c][0][zl, x] = sym[core, zl, x, :, :, :, cols] + core_in[zl, x, :, :, :, cols]
        for copy in ring_copies(c, 0, (2, 1, 3)):
            copy.start()
    for s in range(3):
        for c in range(3):
            first, width = COLORS[c]
            for copy in ring_copies(c, s, (1, 3, 2)):
                copy.wait_recv()
            total = piece(c, s, ring_place(ORDERS[c][s], 0))[...]
            for k in (1, 3, 2):
                total = total + landed[c][s][k - 1]
            if s < 2:
                held[c][s + 1][...] = total
                for copy in ring_copies(c, s + 1, (2, 1, 3)):
                    copy.start()
            else:
                for tile in range(width // 128):
                    col = first + 128 * tile
                    part = total[:, 128 * tile : 128 * tile + 128]
                    out[:, col : col + 128] = part
    for c in range(3):
        core_copy(c).wait_send()
        for s in range(3):
            for copy in ring_copies(c, s, (1, 2, 3)):
                copy.wait_send()

    @pl.loop(0, SX)
    def _(x):
        @pl.when(has(0, 1))
        def _():
            up(x).wait_send()

        @pl.when(has(0, -1))
        def _():
            down(x).wait_send()

    for index in range(4):

        @pl.when(side_sent(index))
        def _():
            side(index).wait_send()

    for dx in (1, -1):

        @pl.when(has(dx, 0))
        def _():
            for row in range(SY):
                face(dx, row).wait_send()

    for n in range(8):
        zpiece(n).wait_send()
        dx, dy = zrows[n + 1][:2]

        @pl.when(has(-dx, -dy))
        def _():
            zcopy(n + 1, -dx, -dy).wait_send()


def ring_buffers():
    buffers = []
    for (_, width), order in zip(COLORS, ORDERS):
        for s in range(3):
            left = [n for d, n in (("z", 2), ("x", 4), ("y", 4), ("z", 2)) if d in order[s:]]
            after = [n for d, n in (("z", 2), ("x", 4), ("y", 4), ("z", 2)) if d in order[s + 1 :]]
            buffers.append(pltpu.VMEM((*left, 4, width), F32))
            buffers.append(pltpu.VMEM((3, *after, 4, width), F32))
    return buffers


def local_products(eigvecs, material):
    tz, sel, txy, t2, t4, t2t, pick = constants()
    small = (
        jnp.asarray(tz, BF16), jnp.asarray(sel), jnp.asarray(txy), jnp.asarray(t2, BF16),
        jnp.asarray(t4, BF16), jnp.asarray(t2t), jnp.asarray(pick, BF16),
    )
    vmem = pl.BlockSpec(memory_space=pltpu.VMEM)
    dma = pltpu.SemaphoreType.DMA
    return pl.pallas_call(
        local_kernel,
        out_shape=jax.ShapeDtypeStruct((4, 2 * K), F32),
        in_specs=[pl.BlockSpec(memory_space=pl.ANY)] + [vmem] * 8,
        out_specs=vmem,
        scratch_shapes=[
            pltpu.VMEM((PX, PY, SZ, K), BF16),
            [pltpu.VMEM((PY, SZ, K), BF16)] * 2,
            [pltpu.VMEM((PY, SZ, K), BF16)] * 2,
            [pltpu.VMEM((SY, SZ, K), BF16)] * 6,
            [pltpu.VMEM((SY, SZ, K), BF16)] * 6,
            [pltpu.VMEM((PAIR_ROWS, 2 * K), BF16)] * 2,
            [pltpu.VMEM((K, PAIR_ROWS), BF16)] * 2,
            pltpu.VMEM((PY * SZ, 2 * K), BF16),
            pltpu.VMEM((K, PY * SZ), BF16),
            pltpu.VMEM((PX, 3, SZ, 128), F32),
            pltpu.VMEM((K, 2 * K), F32),
            pltpu.VMEM((SX * SY, K), F32),
            pltpu.VMEM((64, K), BF16),
            pltpu.VMEM((256, K), BF16),
            pltpu.VMEM((SX * SY, K), BF16),
            dma((SX,)), dma((SX,)), dma((SX,)), dma((SX,)), dma((SX,)),
            dma((4,)), dma((4,)), dma((9,)), dma((9,)),
            dma((2, SY)), dma((2, SY)), dma((8,)), dma((8,)),
            pltpu.VMEM((2, 2, 4, 4, 2, 4, 2 * K), F32),
            pltpu.VMEM((2, 4, 4, 2, 4, 2 * K), F32),
            *ring_buffers(),
            dma((3,)), dma((3,)), dma((36,)), dma((36,)),
        ],
        compiler_params=pltpu.CompilerParams(
            collective_id=0, has_side_effects=True, vmem_limit_bytes=60 * 1024 * 1024
        ),
    )(eigvecs, material, *small)


def per_device(eigvecs, material):
    both = local_products(eigvecs, material)
    return both[:, :K], both[:, K:]


def solution(mesh):
    return jax.shard_map(
        per_device,
        mesh=mesh,
        in_specs=(P("gx", "gy", "gz", None), P(None, "gx", "gy", "gz")),
        out_specs=(P(("gx", "gy", "gz"), None), P(("gx", "gy", "gz"), None)),
        check_vma=False,
    )
```

```python
import functools

import jax
import jax.numpy as jnp
import numpy as np
from jax import lax
from jax.experimental import pallas as pl
from jax.experimental.pallas import tpu as pltpu
from jax.sharding import PartitionSpec as P

MESH = pl.DeviceIdType.MESH
F32 = jnp.float32
BF16 = jnp.bfloat16
HIGH = lax.Precision.HIGHEST

SX, SY, SZ, K = 16, 8, 48, 512
PX, PY = SX + 2, SY + 2
HALF = PY // 2
PAIR_ROWS = 2 * SY * SZ + 4 * SZ
CELLS = 64 * 128 * 96
DIM0 = (((0,), (0,)), ((), ()))
COLORS = ((0, 384), (384, 384), (768, 256))
ORDERS = ("xyz", "yzx", "zxy")


def constants():
    rows = HALF * SZ
    tz = np.zeros((rows, rows), np.float32)
    for r in range(rows):
        for c in (r - 1, r, r + 1):
            if 0 <= c < rows and c // SZ == r // SZ:
                tz[r, c] = 2.0 if c == r else 1.0
    sel = np.zeros((SX * SY, 256), np.float32)
    txy = np.zeros((SX * SY, 256), np.float32)
    for x in range(SX):
        for y in range(SY):
            row = x * SY + y
            sel[row, (x + 1) * PY + y + 1] = 1.0
            for dx in (-1, 0, 1):
                for dy in (-1, 0, 1):
                    txy[row, (x + 1 + dx) * PY + y + 1 + dy] = (2 - abs(dx)) * (2 - abs(dy))
    places = {}
    for x in range(SX):
        for y in range(SY):
            places[(x, y)] = x * SY + y
    for x in range(SX):
        places[(x, SY)] = 128 + x
        places[(x, -1)] = 144 + x
    for y in range(SY):
        places[(SX, y)] = 160 + y
        places[(-1, y)] = 176 + y
    places[(SX, SY)] = 192
    places[(SX, -1)] = 208 + 7
    places[(-1, SY)] = 224
    places[(-1, -1)] = 240 + 7
    t2 = np.zeros((128, 256), np.float32)
    t4 = np.zeros((128, 256), np.float32)
    for x in range(SX):
        for y in range(SY):
            for dx in (-1, 0, 1):
                for dy in (-1, 0, 1):
                    place = places[(x + dx, y + dy)]
                    t2[x * SY + y, place] = (2 - abs(dx)) * (2 - abs(dy))
                    t4[x * SY + y, place] = (4 - 3 * abs(dx)) * (4 - 3 * abs(dy))
    pick = np.zeros((64, 128), np.float32)
    for x in range(SX):
        pick[x, x * SY] = 1.0
        pick[16 + x, x * SY + 7] = 1.0
    for y in range(SY):
        pick[32 + y, y] = 1.0
        pick[48 + y, 15 * SY + y] = 1.0
    return tz, sel, txy, t2, t4, np.ascontiguousarray(t2.T), pick


def local_kernel(
    v_hbm, mat, tz_ref, sel_ref, txy_ref, t2_ref, t4_ref, t2t_ref, pick_ref, out,
    vp, az, bz, ya, yb, xbufs, vts, xbuf, vt, coef, acc, zf, zs, zh, zface,
    own_sem, up_send, dn_send, up_recv, dn_recv, side_send, side_recv, z_send, z_recv,
    face_send, face_recv, zpiece_send, zpiece_recv,
    sym, core_in, *ring,
):
    core_send, core_recv, ring_send, ring_recv = ring[-4:]
    ring = ring[:-4]
    gx, gy, gz = lax.axis_index("gx"), lax.axis_index("gy"), lax.axis_index("gz")
    other = 1 - gz

    def at(dx, dy, z):
        return {"gx": lax.rem(gx + dx + 4, 4), "gy": lax.rem(gy + dy + 16, 16), "gz": z}

    around = [(dx, dy) for dx in (-1, 0, 1) for dy in (-1, 0, 1)]
    barrier = pltpu.get_barrier_semaphore()
    for dx, dy in around:
        if (dx, dy) != (0, 0):
            pl.semaphore_signal(barrier, inc=1, device_id=at(dx, dy, gz), device_id_type=MESH)
        pl.semaphore_signal(barrier, inc=1, device_id=at(dx, dy, other), device_id_type=MESH)

    core, z_lo = lax.rem(gx, 2), lax.div(gx, 2)
    ring_x, ring_y = lax.div(gy, 4), lax.rem(gy, 4)
    ring_z = 2 * gz + z_lo
    partner = {"gx": gx + 1 - 2 * core, "gy": gy, "gz": gz}

    def ring_place(dim, k):
        mine = {"x": ring_x, "y": ring_y, "z": ring_z}[dim]
        return lax.rem(mine + k, 4)

    def ring_peer(dim, k):
        spot = ring_place(dim, k)
        if dim == "x":
            return {"gx": gx, "gy": 4 * spot + ring_y, "gz": gz}
        if dim == "y":
            return {"gx": gx, "gy": 4 * ring_x + spot, "gz": gz}
        return {"gx": 2 * lax.rem(spot, 2) + core, "gy": gy, "gz": lax.div(spot, 2)}

    pl.semaphore_signal(barrier, inc=1, device_id=partner, device_id_type=MESH)
    for dim in "xyz":
        for k in (1, 2, 3):
            pl.semaphore_signal(barrier, inc=1, device_id=ring_peer(dim, k), device_id_type=MESH)

    def own_copy(x):
        return pltpu.make_async_copy(v_hbm.at[x], vp.at[x + 1, pl.ds(1, SY)], own_sem.at[x])

    @pl.loop(0, SX)
    def _(x):
        own_copy(x).start()

    def has(dx, dy):
        ok = jnp.bool_(True)
        if dx == 1:
            ok = jnp.logical_and(ok, gx < 3)
        if dx == -1:
            ok = jnp.logical_and(ok, gx > 0)
        if dy == 1:
            ok = jnp.logical_and(ok, gy < 15)
        if dy == -1:
            ok = jnp.logical_and(ok, gy > 0)
        return ok

    def remote(src, dst, send, recv, where):
        return pltpu.make_async_remote_copy(
            src_ref=src, dst_ref=dst, send_sem=send, recv_sem=recv, device_id=where, device_id_type=MESH
        )

    def up(x):
        return remote(v_hbm.at[x, SY - 1], vp.at[x + 1, 0], up_send.at[x], up_recv.at[x], at(0, 1, gz))

    def down(x):
        return remote(v_hbm.at[x, 0], vp.at[x + 1, PY - 1], dn_send.at[x], dn_recv.at[x], at(0, -1, gz))

    def side(index):
        dx, dy = sides[index]
        src_x = SX if dx == 1 else 1
        dst_x = 0 if dx == 1 else PX - 1
        row = 0 if dy == 1 else PY - 1
        return remote(
            vp.at[src_x, row], vp.at[dst_x, row], side_send.at[index], side_recv.at[index], at(dx, 0, gz)
        )

    def face(dx, row):
        index = 0 if dx == 1 else 1
        return remote(
            v_hbm.at[SX - 1 if dx == 1 else 0, row], vp.at[0 if dx == 1 else PX - 1, row + 1],
            face_send.at[index, row], face_recv.at[index, row], at(dx, 0, gz),
        )

    def side_sent(index):
        dx, dy = sides[index]
        return has(dx, -dy)

    sides = [(1, 1), (1, -1), (-1, 1), (-1, -1)]

    @pl.when(jnp.logical_not(has(0, -1)))
    def _():
        vp[:, 0] = jnp.zeros((PX, SZ, K), BF16)

    @pl.when(jnp.logical_not(has(0, 1)))
    def _():
        vp[:, PY - 1] = jnp.zeros((PX, SZ, K), BF16)

    @pl.when(jnp.logical_not(has(-1, 0)))
    def _():
        vp[0] = jnp.zeros((PY, SZ, K), BF16)

    @pl.when(jnp.logical_not(has(1, 0)))
    def _():
        vp[PX - 1] = jnp.zeros((PY, SZ, K), BF16)

    zrows = [(0, 0, 0, 128)]
    zrows += [(0, 1, 128, 16), (0, -1, 144, 16), (1, 0, 160, 16), (-1, 0, 176, 16)]
    zrows += [(1, 1, 192, 16), (1, -1, 208, 16), (-1, 1, 224, 16), (-1, -1, 240, 16)]
    for dx, dy, first, count in zrows[1:]:

        @pl.when(jnp.logical_not(has(dx, dy)))
        def _():
            zh[pl.ds(first, count)] = jnp.zeros((count, K), BF16)

    pl.semaphore_wait(barrier, 27)

    def send_plane(x):
        @pl.when(has(0, 1))
        def _():
            up(x).start()

        @pl.when(has(0, -1))
        def _():
            down(x).start()

    for n, x in enumerate((SX - 1, 0, 1, 2)):
        send_plane(x)
        for dx in (1, -1):

            @pl.when(has(dx, 0))
            def _():
                face(dx, 2 * n).start()
                face(dx, 2 * n + 1).start()

    send_plane(3)

    kappa = mat[0].reshape(SX * SY, SZ)
    rho = mat[1].reshape(SX * SY, SZ)
    own_kappa = lax.dot_general(kappa, sel_ref[...], DIM0, precision=HIGH, preferred_element_type=F32)
    own_rho = lax.dot_general(rho, sel_ref[...], DIM0, precision=HIGH, preferred_element_type=F32)
    near = lax.dot_general(kappa, txy_ref[...], DIM0, precision=HIGH, preferred_element_type=F32)
    edge_row = jnp.zeros((1, 256), F32)
    near = (
        jnp.concatenate([edge_row, near[:-1]], axis=0)
        + 2.0 * near
        + jnp.concatenate([near[1:], edge_row], axis=0)
    )
    alpha = 2.0 * own_kappa + near * (1.0 / 32.0)
    beta = own_kappa * (1.0 / 16.0)
    for xp in range(PX):
        span = slice(xp * PY, xp * PY + PY)
        coef[xp, 0, :, 0:PY] = alpha[:, span]
        coef[xp, 1, :, 0:PY] = beta[:, span]
        coef[xp, 2, :, 0:PY] = own_rho[:, span]

    def wait_rows(x):
        @pl.when(has(0, -1))
        def _():
            up(x).wait_recv()

        @pl.when(has(0, 1))
        def _():
            down(x).wait_recv()

    wait_rows(SX - 1)
    wait_rows(0)
    for index in range(4):

        @pl.when(side_sent(index))
        def _():
            side(index).start()

    send_plane(4)
    send_plane(5)

    @pl.loop(0, SX)
    def _(x):
        own_copy(x).wait()
        low = vp[x + 1, 1 : 1 + SY, 0:16, :].astype(F32)
        high = vp[x + 1, 1 : 1 + SY, SZ - 16 : SZ, :].astype(F32)
        spot = lax.broadcasted_iota(jnp.int32, (1, 16, 1), 1)
        low = jnp.sum(jnp.where(spot == 0, low, 0.0), axis=1)
        high = jnp.sum(jnp.where(spot == 15, high, 0.0), axis=1)
        zf[pl.ds(pl.multiple_of(x * SY, SY), SY)] = jnp.where(gz == 0, high, low)

    zface[...] = zf[...].astype(BF16)
    zs[...] = jnp.dot(pick_ref[...], zface[...], preferred_element_type=F32).astype(BF16)

    def zcopy(index, dx, dy):
        first, count = zrows[index][2:]
        if (dx, dy) == (0, 0):
            src = zface
        elif dx == 0:
            src = zs.at[pl.ds(16 if dy == 1 else 0, 16)]
        else:
            src = zs.at[pl.ds(48 if dx == 1 else 32, 16)]
        return remote(
            src, zh.at[pl.ds(first, count)], z_send.at[index], z_recv.at[index], at(dx, dy, other)
        )

    def zpiece(n):
        rows = pl.ds(16 * n, 16)
        return remote(
            zface.at[rows], zh.at[rows], zpiece_send.at[n], zpiece_recv.at[n], at(0, 0, other)
        )

    for n in range(8):
        zpiece(n).start()
        dx, dy = zrows[n + 1][:2]

        @pl.when(has(-dx, -dy))
        def _():
            zcopy(n + 1, -dx, -dy).start()

        send_plane(6 + n)
    send_plane(SX - 2)

    acc[...] = jnp.zeros_like(acc)

    def wait_sides(toward):
        @pl.when(has(-toward, 0))
        def _():
            for row in range(SY):
                face(toward, row).wait_recv()

        for index in (0, 1) if toward == 1 else (2, 3):
            dx, dy = sides[index]

            @pl.when(has(-dx, -dy))
            def _():
                side(index).wait_recv()

    def plane_stage(xp, slot):
        for b in range(2):
            for c in range(2):
                lanes = slice(256 * c, 256 * c + 256)
                own = vp[xp, HALF * b : HALF * b + HALF, :, lanes]
                a = jnp.dot(
                    tz_ref[...], own.reshape(HALF * SZ, 256), preferred_element_type=F32
                ).astype(BF16).reshape(HALF, SZ, 256)
                az[slot % 2][HALF * b : HALF * b + HALF, :, lanes] = a
                bz[slot % 2][HALF * b : HALF * b + HALF, :, lanes] = a + (own + own)
        for c in range(2):
            lanes = slice(256 * c, 256 * c + 256)
            a, b = az[slot % 2], bz[slot % 2]
            pair = a[0, :, lanes] + a[1, :, lanes]
            for y in range(SY):
                nxt = a[y + 1, :, lanes] + a[y + 2, :, lanes]
                ya[slot][y, :, lanes] = pair + nxt
                pair = nxt
                yb[slot][y, :, lanes] = (b[y, :, lanes] + b[y + 2, :, lanes]) + BF16(4.0) * b[y + 1, :, lanes]

    def cell_pair(x, slots, side_by):
        x_out, v_out = xbufs[side_by], vts[side_by]
        for y in range(SY):
            cols = [
                [coef[x + 1 + i, n, :, y + 1 : y + 2] for n in range(3)] for i in range(2)
            ]
            for c in range(2):
                lanes = slice(256 * c, 256 * c + 256)
                stage = [ya[n][y, :, lanes] for n in slots]
                sums = [stage[i] + stage[i + 1] for i in range(3)]
                other_stage = [yb[n][y, :, lanes] for n in slots]
                for i in range(2):
                    al, be, ro = cols[i]
                    row = pl.ds(SY * SZ * i + y * SZ, SZ)
                    u = (sums[i] + sums[i + 1]).astype(F32)
                    own = vp[x + 1 + i, y + 1, :, lanes].astype(F32)
                    x_out[row, 256 * c : 256 * c + 256] = (al * own - be * u).astype(BF16)
                    m = (other_stage[i] + other_stage[i + 2]) + BF16(4.0) * other_stage[i + 1]
                    x_out[row, K + 256 * c : K + 256 * c + 256] = (ro * m.astype(F32)).astype(BF16)
        for i in range(2):
            for n, yp in enumerate((0, PY - 1)):
                row = pl.ds(2 * SY * SZ + (2 * i + n) * SZ, SZ)
                x_out[row, 0:K] = halo_rows(x + 1 + i, yp).astype(BF16)
        for i in range(2):
            v_out[:, SY * SZ * i : SY * SZ * i + SY * SZ] = (
                vp[x + 1 + i, 1 : 1 + SY].reshape(SY * SZ, K).T
            )
        sides_of = jnp.concatenate([vp[x + 1 + i, yp] for i in range(2) for yp in (0, PY - 1)], axis=0)
        v_out[:, 2 * SY * SZ : 2 * SY * SZ + 4 * SZ] = sides_of.T

    def gram_pair(side_by, halves=(0, 1)):
        x_in, v_in = xbufs[side_by], vts[side_by]
        for c in halves:
            lanes = slice(K * c, K * c + K)
            depth = 2 * SY * SZ if c else PAIR_ROWS
            acc[:, lanes] += jnp.dot(
                v_in[:, 0:depth], x_in[0:depth, lanes], preferred_element_type=F32
            )

    def halo_rows(xp, yp):
        return coef[xp, 0, :, yp : yp + 1] * vp[xp, yp].astype(F32)

    def side_products():
        for xp in (0, PX - 1):
            for y in range(PY):
                xbuf[y * SZ : y * SZ + SZ, 0:K] = halo_rows(xp, y).astype(BF16)
            vt[...] = vp[xp].reshape(PY * SZ, K).T
            for c in range(2):
                lanes = slice(256 * c, 256 * c + 256)
                acc[:, lanes] += jnp.dot(vt[...], xbuf[:, lanes], preferred_element_type=F32)
    def z_products():
        for n in range(8):
            zpiece(n).wait_recv()
            dx, dy = zrows[n + 1][:2]

            @pl.when(has(dx, dy))
            def _():
                zcopy(n + 1, -dx, -dy).wait_recv()

        lane = lax.broadcasted_iota(jnp.int32, (SX * SY, SZ), 1)
        at_edge = lane == jnp.where(gz == 0, SZ - 1, 0)
        kappa_edge = jnp.sum(
            jnp.where(at_edge, mat[0].reshape(SX * SY, SZ), 0.0), axis=1, keepdims=True
        )
        rho_edge = jnp.sum(
            jnp.where(at_edge, mat[1].reshape(SX * SY, SZ), 0.0), axis=1, keepdims=True
        )
        far = zh[...]
        du = jnp.dot(t2_ref[...], far, preferred_element_type=F32)
        dm = jnp.dot(t4_ref[...], far, preferred_element_type=F32)
        xbuf[0:128, 0:K] = (kappa_edge * (-1.0 / 16.0) * du).astype(BF16)
        xbuf[0:128, K : 2 * K] = (rho_edge * dm).astype(BF16)
        reach = jnp.dot(
            t2t_ref[...], jnp.broadcast_to(kappa_edge, (128, 128)), precision=HIGH, preferred_element_type=F32
        ) * (1.0 / 32.0)
        for c in range(4):
            lanes = slice(128 * c, 128 * c + 128)
            xbuf[128:384, lanes] = (reach * far[:, lanes].astype(F32)).astype(BF16)
        vt[:, 0:128] = zface[...].T
        vt[:, 128:384] = far.T
        for c in range(4):
            lanes = slice(256 * c, 256 * c + 256)
            depth = 384 if c < 2 else 128
            acc[:, lanes] += jnp.dot(vt[:, 0:depth], xbuf[0:depth, lanes], preferred_element_type=F32)

    for ref in (xbufs[1], vts[1]):
        ref[...] = jnp.zeros_like(ref)
    plane_stage(1, 1)
    for n in (2, 3):
        wait_rows(n - 1)
        plane_stage(n, n)
    wait_sides(1)
    plane_stage(0, 0)
    wait_sides(-1)
    plane_stage(SX, 4)
    plane_stage(SX + 1, 5)
    side_products()

    @pl.loop(0, 3)
    def _(t):
        x = 4 * t
        for half in range(2):
            gram_pair(1 - half)
            cell_pair(x + 2 * half, (0, 1, 2, 3) if half == 0 else (2, 3, 0, 1), half)
            for n in range(2):
                wait_rows(x + 2 * half + 3 + n)
            for n in range(2):
                plane_stage(x + 2 * half + 4 + n, 2 * half + n)

    z_products()
    gram_pair(1)
    cell_pair(12, (0, 1, 2, 3), 0)
    gram_pair(0)
    cell_pair(14, (2, 3, 4, 5), 1)

    def core_copy(c):
        first, width = COLORS[c]
        cols = pl.ds(first, width)
        return remote(
            sym.at[1 - core, :, :, :, :, :, cols], core_in.at[:, :, :, :, :, cols],
            core_send.at[c], core_recv.at[c], partner,
        )

    def put(gx_row, col, block):
        for part in range(32):
            sym[
                gx_row % 2, gx_row // 2, part // 8, part // 2 % 4, part % 2, :, col : col + 128
            ] = block[4 * part : 4 * part + 4]

    for half, scale in ((0, 0.5 / CELLS), (1, 0.5 / (216.0 * CELLS))):
        gram_pair(1, (half,))
        for i in range(4):
            for j in range(i, 4):
                rows = slice(128 * i, 128 * i + 128)
                cols = slice(128 * j, 128 * j + 128)
                there = slice(K * half + 128 * j, K * half + 128 * j + 128)
                back = slice(K * half + 128 * i, K * half + 128 * i + 128)
                both = (acc[rows, there] + acc[cols, back].T) * scale
                put(i, K * half + 128 * j, both)
                if i != j:
                    put(j, K * half + 128 * i, both.T)
        if half == 0:
            core_copy(0).start()
        else:
            core_copy(1).start()
            core_copy(2).start()

    held = [[ring[6 * c + 2 * s] for s in range(3)] for c in range(3)]
    landed = [[ring[6 * c + 2 * s + 1] for s in range(3)] for c in range(3)]

    def piece(c, s, spot):
        ref, dim, left = held[c][s], ORDERS[c][s], ORDERS[c][s:]
        index = []
        for name in ("z_lo", "x", "y", "z_hi"):
            if name[0] not in left:
                continue
            if name[0] != dim:
                index.append(slice(None))
            elif name == "z_lo":
                index.append(lax.rem(spot, 2))
            elif name == "z_hi":
                index.append(lax.div(spot, 2))
            else:
                index.append(spot)
        return ref.at[tuple(index)]

    def ring_copies(c, s, ks):
        dim = ORDERS[c][s]
        copies = []
        for part in range(2 if s == 0 else 1):
            for k in ks:
                src, dst = piece(c, s, ring_place(dim, k)), landed[c][s].at[k - 1]
                if s == 0:
                    rows = pl.ds(part * (dst.shape[0] // 2), dst.shape[0] // 2)
                    src, dst = src.at[rows], dst.at[rows]
                number = 12 * c + (6 * part + k - 1 if s == 0 else 3 + 6 * (s - 1) + k - 1)
                copies.append(
                    remote(src, dst, ring_send.at[number], ring_recv.at[number], ring_peer(dim, k))
                )
        return copies

    for c in range(3):
        first, width = COLORS[c]
        cols = slice(first, first + width)
        core_copy(c).wait_recv()
        for zl in range(2):
            for x in range(4):
                held[c][0][zl, x] = sym[core, zl, x, :, :, :, cols] + core_in[zl, x, :, :, :, cols]
        for copy in ring_copies(c, 0, (2, 1, 3)):
            copy.start()
    for s in range(3):
        for c in range(3):
            first, width = COLORS[c]
            for copy in ring_copies(c, s, (1, 3, 2)):
                copy.wait_recv()
            total = piece(c, s, ring_place(ORDERS[c][s], 0))[...]
            for k in (1, 3, 2):
                total = total + landed[c][s][k - 1]
            if s < 2:
                held[c][s + 1][...] = total
                for copy in ring_copies(c, s + 1, (2, 1, 3)):
                    copy.start()
            else:
                for tile in range(width // 128):
                    col = first + 128 * tile
                    part = total[:, 128 * tile : 128 * tile + 128]
                    out[:, col : col + 128] = part
    for c in range(3):
        core_copy(c).wait_send()
        for s in range(3):
            for copy in ring_copies(c, s, (1, 2, 3)):
                copy.wait_send()

    @pl.loop(0, SX)
    def _(x):
        @pl.when(has(0, 1))
        def _():
            up(x).wait_send()

        @pl.when(has(0, -1))
        def _():
            down(x).wait_send()

    for index in range(4):

        @pl.when(side_sent(index))
        def _():
            side(index).wait_send()

    for dx in (1, -1):

        @pl.when(has(dx, 0))
        def _():
            for row in range(SY):
                face(dx, row).wait_send()

    for n in range(8):
        zpiece(n).wait_send()
        dx, dy = zrows[n + 1][:2]

        @pl.when(has(-dx, -dy))
        def _():
            zcopy(n + 1, -dx, -dy).wait_send()


def ring_buffers():
    buffers = []
    for (_, width), order in zip(COLORS, ORDERS):
        for s in range(3):
            left = [n for d, n in (("z", 2), ("x", 4), ("y", 4), ("z", 2)) if d in order[s:]]
            after = [n for d, n in (("z", 2), ("x", 4), ("y", 4), ("z", 2)) if d in order[s + 1 :]]
            buffers.append(pltpu.VMEM((*left, 4, width), F32))
            buffers.append(pltpu.VMEM((3, *after, 4, width), F32))
    return buffers


def local_products(eigvecs, material):
    tz, sel, txy, t2, t4, t2t, pick = constants()
    small = (
        jnp.asarray(tz, BF16), jnp.asarray(sel), jnp.asarray(txy), jnp.asarray(t2, BF16),
        jnp.asarray(t4, BF16), jnp.asarray(t2t), jnp.asarray(pick, BF16),
    )
    vmem = pl.BlockSpec(memory_space=pltpu.VMEM)
    dma = pltpu.SemaphoreType.DMA
    return pl.pallas_call(
        local_kernel,
        out_shape=jax.ShapeDtypeStruct((4, 2 * K), F32),
        in_specs=[pl.BlockSpec(memory_space=pl.ANY)] + [vmem] * 8,
        out_specs=vmem,
        scratch_shapes=[
            pltpu.VMEM((PX, PY, SZ, K), BF16),
            [pltpu.VMEM((PY, SZ, K), BF16)] * 2,
            [pltpu.VMEM((PY, SZ, K), BF16)] * 2,
            [pltpu.VMEM((SY, SZ, K), BF16)] * 6,
            [pltpu.VMEM((SY, SZ, K), BF16)] * 6,
            [pltpu.VMEM((PAIR_ROWS, 2 * K), BF16)] * 2,
            [pltpu.VMEM((K, PAIR_ROWS), BF16)] * 2,
            pltpu.VMEM((PY * SZ, 2 * K), BF16),
            pltpu.VMEM((K, PY * SZ), BF16),
            pltpu.VMEM((PX, 3, SZ, 128), F32),
            pltpu.VMEM((K, 2 * K), F32),
            pltpu.VMEM((SX * SY, K), F32),
            pltpu.VMEM((64, K), BF16),
            pltpu.VMEM((256, K), BF16),
            pltpu.VMEM((SX * SY, K), BF16),
            dma((SX,)), dma((SX,)), dma((SX,)), dma((SX,)), dma((SX,)),
            dma((4,)), dma((4,)), dma((9,)), dma((9,)),
            dma((2, SY)), dma((2, SY)), dma((8,)), dma((8,)),
            pltpu.VMEM((2, 2, 4, 4, 2, 4, 2 * K), F32),
            pltpu.VMEM((2, 4, 4, 2, 4, 2 * K), F32),
            *ring_buffers(),
            dma((3,)), dma((3,)), dma((36,)), dma((36,)),
        ],
        compiler_params=pltpu.CompilerParams(
            collective_id=0, has_side_effects=True, vmem_limit_bytes=60 * 1024 * 1024
        ),
    )(eigvecs, material, *small)


def per_device(eigvecs, material):
    both = local_products(eigvecs, material)
    return both[:, :K], both[:, K:]


def solution(mesh):
    return jax.shard_map(
        per_device,
        mesh=mesh,
        in_specs=(P("gx", "gy", "gz", None), P(None, "gx", "gy", "gz")),
        out_specs=(P(("gx", "gy", "gz"), None), P(("gx", "gy", "gz"), None)),
        check_vma=False,
    )
```

```python
import functools

import jax
import jax.numpy as jnp
import numpy as np
from jax import lax
from jax.experimental import pallas as pl
from jax.experimental.pallas import tpu as pltpu
from jax.sharding import PartitionSpec as P

MESH = pl.DeviceIdType.MESH
F32 = jnp.float32
BF16 = jnp.bfloat16
HIGH = lax.Precision.HIGHEST

SX, SY, SZ, K = 16, 8, 48, 512
PX, PY = SX + 2, SY + 2
HALF = PY // 2
PAIR_ROWS = 2 * SY * SZ + 4 * SZ
CELLS = 64 * 128 * 96
DIM0 = (((0,), (0,)), ((), ()))
COLORS = ((0, 384), (384, 384), (768, 256))
ORDERS = ("zxy", "xyz", "yzx")


def constants():
    rows = HALF * SZ
    tz = np.zeros((rows, rows), np.float32)
    for r in range(rows):
        for c in (r - 1, r, r + 1):
            if 0 <= c < rows and c // SZ == r // SZ:
                tz[r, c] = 2.0 if c == r else 1.0
    sel = np.zeros((SX * SY, 256), np.float32)
    txy = np.zeros((SX * SY, 256), np.float32)
    for x in range(SX):
        for y in range(SY):
            row = x * SY + y
            sel[row, (x + 1) * PY + y + 1] = 1.0
            for dx in (-1, 0, 1):
                for dy in (-1, 0, 1):
                    txy[row, (x + 1 + dx) * PY + y + 1 + dy] = (2 - abs(dx)) * (2 - abs(dy))
    places = {}
    for x in range(SX):
        for y in range(SY):
            places[(x, y)] = x * SY + y
    for x in range(SX):
        places[(x, SY)] = 128 + x
        places[(x, -1)] = 144 + x
    for y in range(SY):
        places[(SX, y)] = 160 + y
        places[(-1, y)] = 176 + y
    places[(SX, SY)] = 192
    places[(SX, -1)] = 208 + 7
    places[(-1, SY)] = 224
    places[(-1, -1)] = 240 + 7
    t2 = np.zeros((128, 256), np.float32)
    t4 = np.zeros((128, 256), np.float32)
    for x in range(SX):
        for y in range(SY):
            for dx in (-1, 0, 1):
                for dy in (-1, 0, 1):
                    place = places[(x + dx, y + dy)]
                    t2[x * SY + y, place] = (2 - abs(dx)) * (2 - abs(dy))
                    t4[x * SY + y, place] = (4 - 3 * abs(dx)) * (4 - 3 * abs(dy))
    pick = np.zeros((64, 128), np.float32)
    for x in range(SX):
        pick[x, x * SY] = 1.0
        pick[16 + x, x * SY + 7] = 1.0
    for y in range(SY):
        pick[32 + y, y] = 1.0
        pick[48 + y, 15 * SY + y] = 1.0
    return tz, sel, txy, t2, t4, np.ascontiguousarray(t2.T), pick


def local_kernel(
    v_hbm, mat, tz_ref, sel_ref, txy_ref, t2_ref, t4_ref, t2t_ref, pick_ref, out,
    vp, az, bz, ya, yb, xbufs, vts, xbuf, vt, coef, acc, zf, zs, zh, zface,
    own_sem, up_send, dn_send, up_recv, dn_recv, side_send, side_recv, z_send, z_recv,
    face_send, face_recv, zpiece_send, zpiece_recv,
    sym, core_in, *ring,
):
    core_send, core_recv, ring_send, ring_recv = ring[-4:]
    ring = ring[:-4]
    gx, gy, gz = lax.axis_index("gx"), lax.axis_index("gy"), lax.axis_index("gz")
    other = 1 - gz

    def at(dx, dy, z):
        return {"gx": lax.rem(gx + dx + 4, 4), "gy": lax.rem(gy + dy + 16, 16), "gz": z}

    around = [(dx, dy) for dx in (-1, 0, 1) for dy in (-1, 0, 1)]
    barrier = pltpu.get_barrier_semaphore()
    for dx, dy in around:
        if (dx, dy) != (0, 0):
            pl.semaphore_signal(barrier, inc=1, device_id=at(dx, dy, gz), device_id_type=MESH)
        pl.semaphore_signal(barrier, inc=1, device_id=at(dx, dy, other), device_id_type=MESH)

    core, z_lo = lax.rem(gx, 2), lax.div(gx, 2)
    ring_x, ring_y = lax.div(gy, 4), lax.rem(gy, 4)
    ring_z = 2 * gz + z_lo
    partner = {"gx": gx + 1 - 2 * core, "gy": gy, "gz": gz}

    def ring_place(dim, k):
        mine = {"x": ring_x, "y": ring_y, "z": ring_z}[dim]
        return lax.rem(mine + k, 4)

    def ring_peer(dim, k):
        spot = ring_place(dim, k)
        if dim == "x":
            return {"gx": gx, "gy": 4 * spot + ring_y, "gz": gz}
        if dim == "y":
            return {"gx": gx, "gy": 4 * ring_x + spot, "gz": gz}
        return {"gx": 2 * lax.rem(spot, 2) + core, "gy": gy, "gz": lax.div(spot, 2)}

    pl.semaphore_signal(barrier, inc=1, device_id=partner, device_id_type=MESH)
    for dim in "xyz":
        for k in (1, 2, 3):
            pl.semaphore_signal(barrier, inc=1, device_id=ring_peer(dim, k), device_id_type=MESH)

    def own_copy(x):
        return pltpu.make_async_copy(v_hbm.at[x], vp.at[x + 1, pl.ds(1, SY)], own_sem.at[x])

    @pl.loop(0, SX)
    def _(x):
        own_copy(x).start()

    def has(dx, dy):
        ok = jnp.bool_(True)
        if dx == 1:
            ok = jnp.logical_and(ok, gx < 3)
        if dx == -1:
            ok = jnp.logical_and(ok, gx > 0)
        if dy == 1:
            ok = jnp.logical_and(ok, gy < 15)
        if dy == -1:
            ok = jnp.logical_and(ok, gy > 0)
        return ok

    def remote(src, dst, send, recv, where):
        return pltpu.make_async_remote_copy(
            src_ref=src, dst_ref=dst, send_sem=send, recv_sem=recv, device_id=where, device_id_type=MESH
        )

    def up(x):
        return remote(v_hbm.at[x, SY - 1], vp.at[x + 1, 0], up_send.at[x], up_recv.at[x], at(0, 1, gz))

    def down(x):
        return remote(v_hbm.at[x, 0], vp.at[x + 1, PY - 1], dn_send.at[x], dn_recv.at[x], at(0, -1, gz))

    def side(index):
        dx, dy = sides[index]
        src_x = SX if dx == 1 else 1
        dst_x = 0 if dx == 1 else PX - 1
        row = 0 if dy == 1 else PY - 1
        return remote(
            vp.at[src_x, row], vp.at[dst_x, row], side_send.at[index], side_recv.at[index], at(dx, 0, gz)
        )

    def face(dx, row):
        index = 0 if dx == 1 else 1
        return remote(
            v_hbm.at[SX - 1 if dx == 1 else 0, row], vp.at[0 if dx == 1 else PX - 1, row + 1],
            face_send.at[index, row], face_recv.at[index, row], at(dx, 0, gz),
        )

    def side_sent(index):
        dx, dy = sides[index]
        return has(dx, -dy)

    sides = [(1, 1), (1, -1), (-1, 1), (-1, -1)]

    @pl.when(jnp.logical_not(has(0, -1)))
    def _():
        vp[:, 0] = jnp.zeros((PX, SZ, K), BF16)

    @pl.when(jnp.logical_not(has(0, 1)))
    def _():
        vp[:, PY - 1] = jnp.zeros((PX, SZ, K), BF16)

    @pl.when(jnp.logical_not(has(-1, 0)))
    def _():
        vp[0] = jnp.zeros((PY, SZ, K), BF16)

    @pl.when(jnp.logical_not(has(1, 0)))
    def _():
        vp[PX - 1] = jnp.zeros((PY, SZ, K), BF16)

    zrows = [(0, 0, 0, 128)]
    zrows += [(0, 1, 128, 16), (0, -1, 144, 16), (1, 0, 160, 16), (-1, 0, 176, 16)]
    zrows += [(1, 1, 192, 16), (1, -1, 208, 16), (-1, 1, 224, 16), (-1, -1, 240, 16)]
    for dx, dy, first, count in zrows[1:]:

        @pl.when(jnp.logical_not(has(dx, dy)))
        def _():
            zh[pl.ds(first, count)] = jnp.zeros((count, K), BF16)

    pl.semaphore_wait(barrier, 27)

    def send_plane(x):
        @pl.when(has(0, 1))
        def _():
            up(x).start()

        @pl.when(has(0, -1))
        def _():
            down(x).start()

    for n, x in enumerate((SX - 1, 0, 1, 2)):
        send_plane(x)
        for dx in (1, -1):

            @pl.when(has(dx, 0))
            def _():
                face(dx, 2 * n).start()
                face(dx, 2 * n + 1).start()

    send_plane(3)

    kappa = mat[0].reshape(SX * SY, SZ)
    rho = mat[1].reshape(SX * SY, SZ)
    own_kappa = lax.dot_general(kappa, sel_ref[...], DIM0, precision=HIGH, preferred_element_type=F32)
    own_rho = lax.dot_general(rho, sel_ref[...], DIM0, precision=HIGH, preferred_element_type=F32)
    near = lax.dot_general(kappa, txy_ref[...], DIM0, precision=HIGH, preferred_element_type=F32)
    edge_row = jnp.zeros((1, 256), F32)
    near = (
        jnp.concatenate([edge_row, near[:-1]], axis=0)
        + 2.0 * near
        + jnp.concatenate([near[1:], edge_row], axis=0)
    )
    alpha = 2.0 * own_kappa + near * (1.0 / 32.0)
    beta = own_kappa * (1.0 / 16.0)
    for xp in range(PX):
        span = slice(xp * PY, xp * PY + PY)
        coef[xp, 0, :, 0:PY] = alpha[:, span]
        coef[xp, 1, :, 0:PY] = beta[:, span]
        coef[xp, 2, :, 0:PY] = own_rho[:, span]

    def wait_rows(x):
        @pl.when(has(0, -1))
        def _():
            up(x).wait_recv()

        @pl.when(has(0, 1))
        def _():
            down(x).wait_recv()

    wait_rows(SX - 1)
    wait_rows(0)
    for index in range(4):

        @pl.when(side_sent(index))
        def _():
            side(index).start()

    send_plane(4)
    send_plane(5)

    @pl.loop(0, SX)
    def _(x):
        own_copy(x).wait()
        low = vp[x + 1, 1 : 1 + SY, 0:16, :].astype(F32)
        high = vp[x + 1, 1 : 1 + SY, SZ - 16 : SZ, :].astype(F32)
        spot = lax.broadcasted_iota(jnp.int32, (1, 16, 1), 1)
        low = jnp.sum(jnp.where(spot == 0, low, 0.0), axis=1)
        high = jnp.sum(jnp.where(spot == 15, high, 0.0), axis=1)
        zf[pl.ds(pl.multiple_of(x * SY, SY), SY)] = jnp.where(gz == 0, high, low)

    zface[...] = zf[...].astype(BF16)
    zs[...] = jnp.dot(pick_ref[...], zface[...], preferred_element_type=F32).astype(BF16)

    def zcopy(index, dx, dy):
        first, count = zrows[index][2:]
        if (dx, dy) == (0, 0):
            src = zface
        elif dx == 0:
            src = zs.at[pl.ds(16 if dy == 1 else 0, 16)]
        else:
            src = zs.at[pl.ds(48 if dx == 1 else 32, 16)]
        return remote(
            src, zh.at[pl.ds(first, count)], z_send.at[index], z_recv.at[index], at(dx, dy, other)
        )

    def zpiece(n):
        rows = pl.ds(16 * n, 16)
        return remote(
            zface.at[rows], zh.at[rows], zpiece_send.at[n], zpiece_recv.at[n], at(0, 0, other)
        )

    for n in range(8):
        zpiece(n).start()
        dx, dy = zrows[n + 1][:2]

        @pl.when(has(-dx, -dy))
        def _():
            zcopy(n + 1, -dx, -dy).start()

        send_plane(6 + n)
    send_plane(SX - 2)

    acc[...] = jnp.zeros_like(acc)

    def wait_sides(toward):
        @pl.when(has(-toward, 0))
        def _():
            for row in range(SY):
                face(toward, row).wait_recv()

        for index in (0, 1) if toward == 1 else (2, 3):
            dx, dy = sides[index]

            @pl.when(has(-dx, -dy))
            def _():
                side(index).wait_recv()

    def plane_stage(xp, slot):
        for b in range(2):
            for c in range(2):
                lanes = slice(256 * c, 256 * c + 256)
                own = vp[xp, HALF * b : HALF * b + HALF, :, lanes]
                a = jnp.dot(
                    tz_ref[...], own.reshape(HALF * SZ, 256), preferred_element_type=F32
                ).astype(BF16).reshape(HALF, SZ, 256)
                az[slot % 2][HALF * b : HALF * b + HALF, :, lanes] = a
                bz[slot % 2][HALF * b : HALF * b + HALF, :, lanes] = a + (own + own)
        for c in range(2):
            lanes = slice(256 * c, 256 * c + 256)
            a, b = az[slot % 2], bz[slot % 2]
            pair = a[0, :, lanes] + a[1, :, lanes]
            for y in range(SY):
                nxt = a[y + 1, :, lanes] + a[y + 2, :, lanes]
                ya[slot][y, :, lanes] = pair + nxt
                pair = nxt
                yb[slot][y, :, lanes] = (b[y, :, lanes] + b[y + 2, :, lanes]) + BF16(4.0) * b[y + 1, :, lanes]

    def cell_pair(x, slots, side_by):
        x_out, v_out = xbufs[side_by], vts[side_by]
        for y in range(SY):
            cols = [
                [coef[x + 1 + i, n, :, y + 1 : y + 2] for n in range(3)] for i in range(2)
            ]
            for c in range(2):
                lanes = slice(256 * c, 256 * c + 256)
                stage = [ya[n][y, :, lanes] for n in slots]
                sums = [stage[i] + stage[i + 1] for i in range(3)]
                other_stage = [yb[n][y, :, lanes] for n in slots]
                for i in range(2):
                    al, be, ro = cols[i]
                    row = pl.ds(SY * SZ * i + y * SZ, SZ)
                    u = (sums[i] + sums[i + 1]).astype(F32)
                    own = vp[x + 1 + i, y + 1, :, lanes].astype(F32)
                    x_out[row, 256 * c : 256 * c + 256] = (al * own - be * u).astype(BF16)
                    m = (other_stage[i] + other_stage[i + 2]) + BF16(4.0) * other_stage[i + 1]
                    x_out[row, K + 256 * c : K + 256 * c + 256] = (ro * m.astype(F32)).astype(BF16)
        for i in range(2):
            for n, yp in enumerate((0, PY - 1)):
                row = pl.ds(2 * SY * SZ + (2 * i + n) * SZ, SZ)
                x_out[row, 0:K] = halo_rows(x + 1 + i, yp).astype(BF16)
        for i in range(2):
            v_out[:, SY * SZ * i : SY * SZ * i + SY * SZ] = (
                vp[x + 1 + i, 1 : 1 + SY].reshape(SY * SZ, K).T
            )
        sides_of = jnp.concatenate([vp[x + 1 + i, yp] for i in range(2) for yp in (0, PY - 1)], axis=0)
        v_out[:, 2 * SY * SZ : 2 * SY * SZ + 4 * SZ] = sides_of.T

    def gram_pair(side_by, halves=(0, 1)):
        x_in, v_in = xbufs[side_by], vts[side_by]
        for c in halves:
            lanes = slice(K * c, K * c + K)
            depth = 2 * SY * SZ if c else PAIR_ROWS
            acc[:, lanes] += jnp.dot(
                v_in[:, 0:depth], x_in[0:depth, lanes], preferred_element_type=F32
            )

    def halo_rows(xp, yp):
        return coef[xp, 0, :, yp : yp + 1] * vp[xp, yp].astype(F32)

    def side_products():
        for xp in (0, PX - 1):
            for y in range(PY):
                xbuf[y * SZ : y * SZ + SZ, 0:K] = halo_rows(xp, y).astype(BF16)
            vt[...] = vp[xp].reshape(PY * SZ, K).T
            for c in range(2):
                lanes = slice(256 * c, 256 * c + 256)
                acc[:, lanes] += jnp.dot(vt[...], xbuf[:, lanes], preferred_element_type=F32)
    def z_products():
        for n in range(8):
            zpiece(n).wait_recv()
            dx, dy = zrows[n + 1][:2]

            @pl.when(has(dx, dy))
            def _():
                zcopy(n + 1, -dx, -dy).wait_recv()

        lane = lax.broadcasted_iota(jnp.int32, (SX * SY, SZ), 1)
        at_edge = lane == jnp.where(gz == 0, SZ - 1, 0)
        kappa_edge = jnp.sum(
            jnp.where(at_edge, mat[0].reshape(SX * SY, SZ), 0.0), axis=1, keepdims=True
        )
        rho_edge = jnp.sum(
            jnp.where(at_edge, mat[1].reshape(SX * SY, SZ), 0.0), axis=1, keepdims=True
        )
        far = zh[...]
        du = jnp.dot(t2_ref[...], far, preferred_element_type=F32)
        dm = jnp.dot(t4_ref[...], far, preferred_element_type=F32)
        xbuf[0:128, 0:K] = (kappa_edge * (-1.0 / 16.0) * du).astype(BF16)
        xbuf[0:128, K : 2 * K] = (rho_edge * dm).astype(BF16)
        reach = jnp.dot(
            t2t_ref[...], jnp.broadcast_to(kappa_edge, (128, 128)), precision=HIGH, preferred_element_type=F32
        ) * (1.0 / 32.0)
        for c in range(4):
            lanes = slice(128 * c, 128 * c + 128)
            xbuf[128:384, lanes] = (reach * far[:, lanes].astype(F32)).astype(BF16)
        vt[:, 0:128] = zface[...].T
        vt[:, 128:384] = far.T
        for c in range(4):
            lanes = slice(256 * c, 256 * c + 256)
            depth = 384 if c < 2 else 128
            acc[:, lanes] += jnp.dot(vt[:, 0:depth], xbuf[0:depth, lanes], preferred_element_type=F32)

    for ref in (xbufs[1], vts[1]):
        ref[...] = jnp.zeros_like(ref)
    plane_stage(1, 1)
    for n in (2, 3):
        wait_rows(n - 1)
        plane_stage(n, n)
    wait_sides(1)
    plane_stage(0, 0)

    @pl.loop(0, 3)
    def _(t):
        x = 4 * t
        for half in range(2):
            gram_pair(1 - half)
            cell_pair(x + 2 * half, (0, 1, 2, 3) if half == 0 else (2, 3, 0, 1), half)
            for n in range(2):
                wait_rows(x + 2 * half + 3 + n)
            for n in range(2):
                plane_stage(x + 2 * half + 4 + n, 2 * half + n)

        @pl.when(t == 0)
        def _():
            wait_sides(-1)
            side_products()
            plane_stage(SX, 4)
            plane_stage(SX + 1, 5)

    z_products()
    gram_pair(1)
    cell_pair(12, (0, 1, 2, 3), 0)
    gram_pair(0)
    cell_pair(14, (2, 3, 4, 5), 1)

    def core_copy(c):
        first, width = COLORS[c]
        cols = pl.ds(first, width)
        return remote(
            sym.at[1 - core, :, :, :, :, :, cols], core_in.at[:, :, :, :, :, cols],
            core_send.at[c], core_recv.at[c], partner,
        )

    def put(gx_row, col, block):
        for part in range(32):
            sym[
                gx_row % 2, gx_row // 2, part // 8, part // 2 % 4, part % 2, :, col : col + 128
            ] = block[4 * part : 4 * part + 4]

    for half, scale in ((0, 0.5 / CELLS), (1, 0.5 / (216.0 * CELLS))):
        gram_pair(1, (half,))
        for i in range(4):
            for j in range(i, 4):
                rows = slice(128 * i, 128 * i + 128)
                cols = slice(128 * j, 128 * j + 128)
                there = slice(K * half + 128 * j, K * half + 128 * j + 128)
                back = slice(K * half + 128 * i, K * half + 128 * i + 128)
                both = (acc[rows, there] + acc[cols, back].T) * scale
                put(i, K * half + 128 * j, both)
                if i != j:
                    put(j, K * half + 128 * i, both.T)
        if half == 0:
            core_copy(0).start()
        else:
            core_copy(1).start()
            core_copy(2).start()

    held = [[ring[6 * c + 2 * s] for s in range(3)] for c in range(3)]
    landed = [[ring[6 * c + 2 * s + 1] for s in range(3)] for c in range(3)]

    def piece(c, s, spot):
        ref, dim, left = held[c][s], ORDERS[c][s], ORDERS[c][s:]
        index = []
        for name in ("z_lo", "x", "y", "z_hi"):
            if name[0] not in left:
                continue
            if name[0] != dim:
                index.append(slice(None))
            elif name == "z_lo":
                index.append(lax.rem(spot, 2))
            elif name == "z_hi":
                index.append(lax.div(spot, 2))
            else:
                index.append(spot)
        return ref.at[tuple(index)]

    def ring_copies(c, s, ks):
        dim = ORDERS[c][s]
        copies = []
        for part in range(2 if s == 0 else 1):
            for k in ks:
                src, dst = piece(c, s, ring_place(dim, k)), landed[c][s].at[k - 1]
                if s == 0:
                    rows = pl.ds(part * (dst.shape[0] // 2), dst.shape[0] // 2)
                    src, dst = src.at[rows], dst.at[rows]
                number = 12 * c + (6 * part + k - 1 if s == 0 else 3 + 6 * (s - 1) + k - 1)
                copies.append(
                    remote(src, dst, ring_send.at[number], ring_recv.at[number], ring_peer(dim, k))
                )
        return copies

    for c in range(3):
        first, width = COLORS[c]
        cols = slice(first, first + width)
        core_copy(c).wait_recv()
        for zl in range(2):
            for x in range(4):
                held[c][0][zl, x] = sym[core, zl, x, :, :, :, cols] + core_in[zl, x, :, :, :, cols]
        for copy in ring_copies(c, 0, (2, 1, 3)):
            copy.start()
    for s in range(3):
        for c in range(3):
            first, width = COLORS[c]
            for copy in ring_copies(c, s, (1, 3, 2)):
                copy.wait_recv()
            total = piece(c, s, ring_place(ORDERS[c][s], 0))[...]
            for k in (1, 3, 2):
                total = total + landed[c][s][k - 1]
            if s < 2:
                held[c][s + 1][...] = total
                for copy in ring_copies(c, s + 1, (2, 1, 3)):
                    copy.start()
            else:
                for tile in range(width // 128):
                    col = first + 128 * tile
                    part = total[:, 128 * tile : 128 * tile + 128]
                    out[:, col : col + 128] = part
    for c in range(3):
        core_copy(c).wait_send()
        for s in range(3):
            for copy in ring_copies(c, s, (1, 2, 3)):
                copy.wait_send()

    @pl.loop(0, SX)
    def _(x):
        @pl.when(has(0, 1))
        def _():
            up(x).wait_send()

        @pl.when(has(0, -1))
        def _():
            down(x).wait_send()

    for index in range(4):

        @pl.when(side_sent(index))
        def _():
            side(index).wait_send()

    for dx in (1, -1):

        @pl.when(has(dx, 0))
        def _():
            for row in range(SY):
                face(dx, row).wait_send()

    for n in range(8):
        zpiece(n).wait_send()
        dx, dy = zrows[n + 1][:2]

        @pl.when(has(-dx, -dy))
        def _():
            zcopy(n + 1, -dx, -dy).wait_send()


def ring_buffers():
    buffers = []
    for (_, width), order in zip(COLORS, ORDERS):
        for s in range(3):
            left = [n for d, n in (("z", 2), ("x", 4), ("y", 4), ("z", 2)) if d in order[s:]]
            after = [n for d, n in (("z", 2), ("x", 4), ("y", 4), ("z", 2)) if d in order[s + 1 :]]
            buffers.append(pltpu.VMEM((*left, 4, width), F32))
            buffers.append(pltpu.VMEM((3, *after, 4, width), F32))
    return buffers


def local_products(eigvecs, material):
    tz, sel, txy, t2, t4, t2t, pick = constants()
    small = (
        jnp.asarray(tz, BF16), jnp.asarray(sel), jnp.asarray(txy), jnp.asarray(t2, BF16),
        jnp.asarray(t4, BF16), jnp.asarray(t2t), jnp.asarray(pick, BF16),
    )
    vmem = pl.BlockSpec(memory_space=pltpu.VMEM)
    dma = pltpu.SemaphoreType.DMA
    return pl.pallas_call(
        local_kernel,
        out_shape=jax.ShapeDtypeStruct((4, 2 * K), F32),
        in_specs=[pl.BlockSpec(memory_space=pl.ANY)] + [vmem] * 8,
        out_specs=vmem,
        scratch_shapes=[
            pltpu.VMEM((PX, PY, SZ, K), BF16),
            [pltpu.VMEM((PY, SZ, K), BF16)] * 2,
            [pltpu.VMEM((PY, SZ, K), BF16)] * 2,
            [pltpu.VMEM((SY, SZ, K), BF16)] * 6,
            [pltpu.VMEM((SY, SZ, K), BF16)] * 6,
            [pltpu.VMEM((PAIR_ROWS, 2 * K), BF16)] * 2,
            [pltpu.VMEM((K, PAIR_ROWS), BF16)] * 2,
            pltpu.VMEM((PY * SZ, 2 * K), BF16),
            pltpu.VMEM((K, PY * SZ), BF16),
            pltpu.VMEM((PX, 3, SZ, 128), F32),
            pltpu.VMEM((K, 2 * K), F32),
            pltpu.VMEM((SX * SY, K), F32),
            pltpu.VMEM((64, K), BF16),
            pltpu.VMEM((256, K), BF16),
            pltpu.VMEM((SX * SY, K), BF16),
            dma((SX,)), dma((SX,)), dma((SX,)), dma((SX,)), dma((SX,)),
            dma((4,)), dma((4,)), dma((9,)), dma((9,)),
            dma((2, SY)), dma((2, SY)), dma((8,)), dma((8,)),
            pltpu.VMEM((2, 2, 4, 4, 2, 4, 2 * K), F32),
            pltpu.VMEM((2, 4, 4, 2, 4, 2 * K), F32),
            *ring_buffers(),
            dma((3,)), dma((3,)), dma((36,)), dma((36,)),
        ],
        compiler_params=pltpu.CompilerParams(
            collective_id=0, has_side_effects=True, vmem_limit_bytes=60 * 1024 * 1024
        ),
    )(eigvecs, material, *small)


def per_device(eigvecs, material):
    both = local_products(eigvecs, material)
    return both[:, :K], both[:, K:]


def solution(mesh):
    return jax.shard_map(
        per_device,
        mesh=mesh,
        in_specs=(P("gx", "gy", "gz", None), P(None, "gx", "gy", "gz")),
        out_specs=(P(("gx", "gy", "gz"), None), P(("gx", "gy", "gz"), None)),
        check_vma=False,
    )
```

```python
import functools

import jax
import jax.numpy as jnp
import numpy as np
from jax import lax
from jax.experimental import pallas as pl
from jax.experimental.pallas import tpu as pltpu
from jax.sharding import PartitionSpec as P

MESH = pl.DeviceIdType.MESH
F32 = jnp.float32
BF16 = jnp.bfloat16
HIGH = lax.Precision.HIGHEST

SX, SY, SZ, K = 16, 8, 48, 512
PX, PY = SX + 2, SY + 2
HALF = PY // 2
PAIR_ROWS = 2 * SY * SZ + 4 * SZ
CELLS = 64 * 128 * 96
DIM0 = (((0,), (0,)), ((), ()))
COLORS = ((0, 384), (384, 384), (768, 256))
ORDERS = ("zxy", "xyz", "yzx")


def constants():
    rows = HALF * SZ
    tz = np.zeros((rows, rows), np.float32)
    for r in range(rows):
        for c in (r - 1, r, r + 1):
            if 0 <= c < rows and c // SZ == r // SZ:
                tz[r, c] = 2.0 if c == r else 1.0
    sel = np.zeros((SX * SY, 256), np.float32)
    txy = np.zeros((SX * SY, 256), np.float32)
    for x in range(SX):
        for y in range(SY):
            row = x * SY + y
            sel[row, (x + 1) * PY + y + 1] = 1.0
            for dx in (-1, 0, 1):
                for dy in (-1, 0, 1):
                    txy[row, (x + 1 + dx) * PY + y + 1 + dy] = (2 - abs(dx)) * (2 - abs(dy))
    places = {}
    for x in range(SX):
        for y in range(SY):
            places[(x, y)] = x * SY + y
    for x in range(SX):
        places[(x, SY)] = 128 + x
        places[(x, -1)] = 144 + x
    for y in range(SY):
        places[(SX, y)] = 160 + y
        places[(-1, y)] = 176 + y
    places[(SX, SY)] = 192
    places[(SX, -1)] = 208 + 7
    places[(-1, SY)] = 224
    places[(-1, -1)] = 240 + 7
    t2 = np.zeros((128, 256), np.float32)
    t4 = np.zeros((128, 256), np.float32)
    for x in range(SX):
        for y in range(SY):
            for dx in (-1, 0, 1):
                for dy in (-1, 0, 1):
                    place = places[(x + dx, y + dy)]
                    t2[x * SY + y, place] = (2 - abs(dx)) * (2 - abs(dy))
                    t4[x * SY + y, place] = (4 - 3 * abs(dx)) * (4 - 3 * abs(dy))
    pick = np.zeros((64, 128), np.float32)
    for x in range(SX):
        pick[x, x * SY] = 1.0
        pick[16 + x, x * SY + 7] = 1.0
    for y in range(SY):
        pick[32 + y, y] = 1.0
        pick[48 + y, 15 * SY + y] = 1.0
    return tz, sel, txy, t2, t4, np.ascontiguousarray(t2.T), pick


def local_kernel(
    v_hbm, mat, tz_ref, sel_ref, txy_ref, t2_ref, t4_ref, t2t_ref, pick_ref, out,
    vp, az, bz, ya, yb, xbufs, vts, xbuf, vt, coef, acc, zf, zs, zh, zface,
    own_sem, up_send, dn_send, up_recv, dn_recv, side_send, side_recv, z_send, z_recv,
    face_send, face_recv, zpiece_send, zpiece_recv,
    sym, core_in, *ring,
):
    core_send, core_recv, ring_send, ring_recv = ring[-4:]
    ring = ring[:-4]
    gx, gy, gz = lax.axis_index("gx"), lax.axis_index("gy"), lax.axis_index("gz")
    other = 1 - gz

    def at(dx, dy, z):
        return {"gx": lax.rem(gx + dx + 4, 4), "gy": lax.rem(gy + dy + 16, 16), "gz": z}

    around = [(dx, dy) for dx in (-1, 0, 1) for dy in (-1, 0, 1)]
    barrier = pltpu.get_barrier_semaphore()
    for dx, dy in around:
        if (dx, dy) != (0, 0):
            pl.semaphore_signal(barrier, inc=1, device_id=at(dx, dy, gz), device_id_type=MESH)
        pl.semaphore_signal(barrier, inc=1, device_id=at(dx, dy, other), device_id_type=MESH)

    core, z_lo = lax.rem(gx, 2), lax.div(gx, 2)
    ring_x, ring_y = lax.div(gy, 4), lax.rem(gy, 4)
    ring_z = 2 * gz + z_lo
    partner = {"gx": gx + 1 - 2 * core, "gy": gy, "gz": gz}

    def ring_place(dim, k):
        mine = {"x": ring_x, "y": ring_y, "z": ring_z}[dim]
        return lax.rem(mine + k, 4)

    def ring_peer(dim, k):
        spot = ring_place(dim, k)
        if dim == "x":
            return {"gx": gx, "gy": 4 * spot + ring_y, "gz": gz}
        if dim == "y":
            return {"gx": gx, "gy": 4 * ring_x + spot, "gz": gz}
        return {"gx": 2 * lax.rem(spot, 2) + core, "gy": gy, "gz": lax.div(spot, 2)}

    pl.semaphore_signal(barrier, inc=1, device_id=partner, device_id_type=MESH)
    for dim in "xyz":
        for k in (1, 2, 3):
            pl.semaphore_signal(barrier, inc=1, device_id=ring_peer(dim, k), device_id_type=MESH)

    def own_copy(x):
        return pltpu.make_async_copy(v_hbm.at[x], vp.at[x + 1, pl.ds(1, SY)], own_sem.at[x])

    @pl.loop(0, SX)
    def _(x):
        own_copy(x).start()

    def has(dx, dy):
        ok = jnp.bool_(True)
        if dx == 1:
            ok = jnp.logical_and(ok, gx < 3)
        if dx == -1:
            ok = jnp.logical_and(ok, gx > 0)
        if dy == 1:
            ok = jnp.logical_and(ok, gy < 15)
        if dy == -1:
            ok = jnp.logical_and(ok, gy > 0)
        return ok

    def remote(src, dst, send, recv, where):
        return pltpu.make_async_remote_copy(
            src_ref=src, dst_ref=dst, send_sem=send, recv_sem=recv, device_id=where, device_id_type=MESH
        )

    def up(x):
        return remote(v_hbm.at[x, SY - 1], vp.at[x + 1, 0], up_send.at[x], up_recv.at[x], at(0, 1, gz))

    def down(x):
        return remote(v_hbm.at[x, 0], vp.at[x + 1, PY - 1], dn_send.at[x], dn_recv.at[x], at(0, -1, gz))

    def side(index):
        dx, dy = sides[index]
        src_x = SX if dx == 1 else 1
        dst_x = 0 if dx == 1 else PX - 1
        row = 0 if dy == 1 else PY - 1
        return remote(
            vp.at[src_x, row], vp.at[dst_x, row], side_send.at[index], side_recv.at[index], at(dx, 0, gz)
        )

    def face(dx, row):
        index = 0 if dx == 1 else 1
        return remote(
            v_hbm.at[SX - 1 if dx == 1 else 0, row], vp.at[0 if dx == 1 else PX - 1, row + 1],
            face_send.at[index, row], face_recv.at[index, row], at(dx, 0, gz),
        )

    def side_sent(index):
        dx, dy = sides[index]
        return has(dx, -dy)

    sides = [(1, 1), (1, -1), (-1, 1), (-1, -1)]

    @pl.when(jnp.logical_not(has(0, -1)))
    def _():
        vp[:, 0] = jnp.zeros((PX, SZ, K), BF16)

    @pl.when(jnp.logical_not(has(0, 1)))
    def _():
        vp[:, PY - 1] = jnp.zeros((PX, SZ, K), BF16)

    @pl.when(jnp.logical_not(has(-1, 0)))
    def _():
        vp[0] = jnp.zeros((PY, SZ, K), BF16)

    @pl.when(jnp.logical_not(has(1, 0)))
    def _():
        vp[PX - 1] = jnp.zeros((PY, SZ, K), BF16)

    zrows = [(0, 0, 0, 128)]
    zrows += [(0, 1, 128, 16), (0, -1, 144, 16), (1, 0, 160, 16), (-1, 0, 176, 16)]
    zrows += [(1, 1, 192, 16), (1, -1, 208, 16), (-1, 1, 224, 16), (-1, -1, 240, 16)]
    for dx, dy, first, count in zrows[1:]:

        @pl.when(jnp.logical_not(has(dx, dy)))
        def _():
            zh[pl.ds(first, count)] = jnp.zeros((count, K), BF16)

    pl.semaphore_wait(barrier, 27)

    def send_plane(x):
        @pl.when(has(0, 1))
        def _():
            up(x).start()

        @pl.when(has(0, -1))
        def _():
            down(x).start()

    for n, x in enumerate((SX - 1, 0, 1, 2)):
        send_plane(x)
        for dx in (1, -1):

            @pl.when(has(dx, 0))
            def _():
                face(dx, 2 * n).start()
                face(dx, 2 * n + 1).start()

    send_plane(3)

    kappa = mat[0].reshape(SX * SY, SZ)
    rho = mat[1].reshape(SX * SY, SZ)
    own_kappa = lax.dot_general(kappa, sel_ref[...], DIM0, precision=HIGH, preferred_element_type=F32)
    own_rho = lax.dot_general(rho, sel_ref[...], DIM0, precision=HIGH, preferred_element_type=F32)
    near = lax.dot_general(kappa, txy_ref[...], DIM0, precision=HIGH, preferred_element_type=F32)
    edge_row = jnp.zeros((1, 256), F32)
    near = (
        jnp.concatenate([edge_row, near[:-1]], axis=0)
        + 2.0 * near
        + jnp.concatenate([near[1:], edge_row], axis=0)
    )
    alpha = 2.0 * own_kappa + near * (1.0 / 32.0)
    beta = own_kappa * (1.0 / 16.0)
    for xp in range(PX):
        span = slice(xp * PY, xp * PY + PY)
        coef[xp, 0, :, 0:PY] = alpha[:, span]
        coef[xp, 1, :, 0:PY] = beta[:, span]
        coef[xp, 2, :, 0:PY] = own_rho[:, span]

    def wait_rows(x):
        @pl.when(has(0, -1))
        def _():
            up(x).wait_recv()

        @pl.when(has(0, 1))
        def _():
            down(x).wait_recv()

    wait_rows(SX - 1)
    wait_rows(0)
    for index in range(4):

        @pl.when(side_sent(index))
        def _():
            side(index).start()

    send_plane(4)
    send_plane(5)

    @pl.loop(0, SX)
    def _(x):
        own_copy(x).wait()
        low = vp[x + 1, 1 : 1 + SY, 0:16, :].astype(F32)
        high = vp[x + 1, 1 : 1 + SY, SZ - 16 : SZ, :].astype(F32)
        spot = lax.broadcasted_iota(jnp.int32, (1, 16, 1), 1)
        low = jnp.sum(jnp.where(spot == 0, low, 0.0), axis=1)
        high = jnp.sum(jnp.where(spot == 15, high, 0.0), axis=1)
        zf[pl.ds(pl.multiple_of(x * SY, SY), SY)] = jnp.where(gz == 0, high, low)

    zface[...] = zf[...].astype(BF16)
    zs[...] = jnp.dot(pick_ref[...], zface[...], preferred_element_type=F32).astype(BF16)

    def zcopy(index, dx, dy):
        first, count = zrows[index][2:]
        if (dx, dy) == (0, 0):
            src = zface
        elif dx == 0:
            src = zs.at[pl.ds(16 if dy == 1 else 0, 16)]
        else:
            src = zs.at[pl.ds(48 if dx == 1 else 32, 16)]
        return remote(
            src, zh.at[pl.ds(first, count)], z_send.at[index], z_recv.at[index], at(dx, dy, other)
        )

    def zpiece(n):
        rows = pl.ds(16 * n, 16)
        return remote(
            zface.at[rows], zh.at[rows], zpiece_send.at[n], zpiece_recv.at[n], at(0, 0, other)
        )

    for n in range(8):
        zpiece(n).start()
        dx, dy = zrows[n + 1][:2]

        @pl.when(has(-dx, -dy))
        def _():
            zcopy(n + 1, -dx, -dy).start()

        send_plane(6 + n)
    send_plane(SX - 2)

    acc[...] = jnp.zeros_like(acc)

    def wait_sides(toward):
        @pl.when(has(-toward, 0))
        def _():
            for row in range(SY):
                face(toward, row).wait_recv()

        for index in (0, 1) if toward == 1 else (2, 3):
            dx, dy = sides[index]

            @pl.when(has(-dx, -dy))
            def _():
                side(index).wait_recv()

    def plane_stage(xp, slot):
        for b in range(2):
            for c in range(2):
                lanes = slice(256 * c, 256 * c + 256)
                own = vp[xp, HALF * b : HALF * b + HALF, :, lanes]
                a = jnp.dot(
                    tz_ref[...], own.reshape(HALF * SZ, 256), preferred_element_type=F32
                ).astype(BF16).reshape(HALF, SZ, 256)
                az[slot % 2][HALF * b : HALF * b + HALF, :, lanes] = a
                bz[slot % 2][HALF * b : HALF * b + HALF, :, lanes] = a + (own + own)
        for c in range(2):
            lanes = slice(256 * c, 256 * c + 256)
            a, b = az[slot % 2], bz[slot % 2]
            pair = a[0, :, lanes] + a[1, :, lanes]
            for y in range(SY):
                nxt = a[y + 1, :, lanes] + a[y + 2, :, lanes]
                ya[slot][y, :, lanes] = pair + nxt
                pair = nxt
                yb[slot][y, :, lanes] = (b[y, :, lanes] + b[y + 2, :, lanes]) + BF16(4.0) * b[y + 1, :, lanes]

    def cell_pair(x, slots, side_by):
        x_out, v_out = xbufs[side_by], vts[side_by]
        for y in range(SY):
            cols = [
                [coef[x + 1 + i, n, :, y + 1 : y + 2] for n in range(3)] for i in range(2)
            ]
            for c in range(2):
                lanes = slice(256 * c, 256 * c + 256)
                stage = [ya[n][y, :, lanes] for n in slots]
                sums = [stage[i] + stage[i + 1] for i in range(3)]
                other_stage = [yb[n][y, :, lanes] for n in slots]
                for i in range(2):
                    al, be, ro = cols[i]
                    row = pl.ds(SY * SZ * i + y * SZ, SZ)
                    u = (sums[i] + sums[i + 1]).astype(F32)
                    own = vp[x + 1 + i, y + 1, :, lanes].astype(F32)
                    x_out[row, 256 * c : 256 * c + 256] = (al * own - be * u).astype(BF16)
                    m = (other_stage[i] + other_stage[i + 2]) + BF16(4.0) * other_stage[i + 1]
                    x_out[row, K + 256 * c : K + 256 * c + 256] = (ro * m.astype(F32)).astype(BF16)
        for i in range(2):
            for n, yp in enumerate((0, PY - 1)):
                row = pl.ds(2 * SY * SZ + (2 * i + n) * SZ, SZ)
                x_out[row, 0:K] = halo_rows(x + 1 + i, yp).astype(BF16)
        for i in range(2):
            v_out[:, SY * SZ * i : SY * SZ * i + SY * SZ] = (
                vp[x + 1 + i, 1 : 1 + SY].reshape(SY * SZ, K).T
            )
        sides_of = jnp.concatenate([vp[x + 1 + i, yp] for i in range(2) for yp in (0, PY - 1)], axis=0)
        v_out[:, 2 * SY * SZ : 2 * SY * SZ + 4 * SZ] = sides_of.T

    def gram_pair(side_by, halves=(0, 1)):
        x_in, v_in = xbufs[side_by], vts[side_by]
        for c in halves:
            lanes = slice(K * c, K * c + K)
            depth = 2 * SY * SZ if c else PAIR_ROWS
            acc[:, lanes] += jnp.dot(
                v_in[:, 0:depth], x_in[0:depth, lanes], preferred_element_type=F32
            )

    def halo_rows(xp, yp):
        return coef[xp, 0, :, yp : yp + 1] * vp[xp, yp].astype(F32)

    def side_products():
        for xp in (0, PX - 1):
            for y in range(PY):
                xbuf[y * SZ : y * SZ + SZ, 0:K] = halo_rows(xp, y).astype(BF16)
            vt[...] = vp[xp].reshape(PY * SZ, K).T
            for c in range(2):
                lanes = slice(256 * c, 256 * c + 256)
                acc[:, lanes] += jnp.dot(vt[...], xbuf[:, lanes], preferred_element_type=F32)
    def z_products():
        for n in range(8):
            zpiece(n).wait_recv()
            dx, dy = zrows[n + 1][:2]

            @pl.when(has(dx, dy))
            def _():
                zcopy(n + 1, -dx, -dy).wait_recv()

        lane = lax.broadcasted_iota(jnp.int32, (SX * SY, SZ), 1)
        at_edge = lane == jnp.where(gz == 0, SZ - 1, 0)
        kappa_edge = jnp.sum(
            jnp.where(at_edge, mat[0].reshape(SX * SY, SZ), 0.0), axis=1, keepdims=True
        )
        rho_edge = jnp.sum(
            jnp.where(at_edge, mat[1].reshape(SX * SY, SZ), 0.0), axis=1, keepdims=True
        )
        far = zh[...]
        du = jnp.dot(t2_ref[...], far, preferred_element_type=F32)
        dm = jnp.dot(t4_ref[...], far, preferred_element_type=F32)
        xbuf[0:128, 0:K] = (kappa_edge * (-1.0 / 16.0) * du).astype(BF16)
        xbuf[0:128, K : 2 * K] = (rho_edge * dm).astype(BF16)
        reach = jnp.dot(
            t2t_ref[...], jnp.broadcast_to(kappa_edge, (128, 128)), precision=HIGH, preferred_element_type=F32
        ) * (1.0 / 32.0)
        for c in range(4):
            lanes = slice(128 * c, 128 * c + 128)
            xbuf[128:384, lanes] = (reach * far[:, lanes].astype(F32)).astype(BF16)
        vt[:, 0:128] = zface[...].T
        vt[:, 128:384] = far.T
        for c in range(4):
            lanes = slice(256 * c, 256 * c + 256)
            depth = 384 if c < 2 else 128
            acc[:, lanes] += jnp.dot(vt[:, 0:depth], xbuf[0:depth, lanes], preferred_element_type=F32)

    for ref in (xbufs[1], vts[1]):
        ref[...] = jnp.zeros_like(ref)
    plane_stage(1, 1)
    for n in (2, 3):
        wait_rows(n - 1)
        plane_stage(n, n)
    wait_sides(1)
    plane_stage(0, 0)

    @pl.loop(0, 3)
    def _(t):
        x = 4 * t
        for half in range(2):
            gram_pair(1 - half)
            cell_pair(x + 2 * half, (0, 1, 2, 3) if half == 0 else (2, 3, 0, 1), half)
            for n in range(2):
                wait_rows(x + 2 * half + 3 + n)
                plane_stage(x + 2 * half + 4 + n, 2 * half + n)

        @pl.when(t == 0)
        def _():
            wait_sides(-1)
            side_products()
            plane_stage(SX, 4)
            plane_stage(SX + 1, 5)

    z_products()
    gram_pair(1)
    cell_pair(12, (0, 1, 2, 3), 0)
    gram_pair(0)
    cell_pair(14, (2, 3, 4, 5), 1)

    def core_copy(c):
        first, width = COLORS[c]
        cols = pl.ds(first, width)
        return remote(
            sym.at[1 - core, :, :, :, :, :, cols], core_in.at[:, :, :, :, :, cols],
            core_send.at[c], core_recv.at[c], partner,
        )

    def put(gx_row, col, block):
        for part in range(32):
            sym[
                gx_row % 2, gx_row // 2, part // 8, part // 2 % 4, part % 2, :, col : col + 128
            ] = block[4 * part : 4 * part + 4]

    for half, scale in ((0, 0.5 / CELLS), (1, 0.5 / (216.0 * CELLS))):
        gram_pair(1, (half,))
        for i in range(4):
            for j in range(i, 4):
                rows = slice(128 * i, 128 * i + 128)
                cols = slice(128 * j, 128 * j + 128)
                there = slice(K * half + 128 * j, K * half + 128 * j + 128)
                back = slice(K * half + 128 * i, K * half + 128 * i + 128)
                both = (acc[rows, there] + acc[cols, back].T) * scale
                put(i, K * half + 128 * j, both)
                if i != j:
                    put(j, K * half + 128 * i, both.T)
        if half == 0:
            core_copy(0).start()
        else:
            core_copy(1).start()
            core_copy(2).start()

    held = [[ring[6 * c + 2 * s] for s in range(3)] for c in range(3)]
    landed = [[ring[6 * c + 2 * s + 1] for s in range(3)] for c in range(3)]

    def piece(c, s, spot):
        ref, dim, left = held[c][s], ORDERS[c][s], ORDERS[c][s:]
        index = []
        for name in ("z_lo", "x", "y", "z_hi"):
            if name[0] not in left:
                continue
            if name[0] != dim:
                index.append(slice(None))
            elif name == "z_lo":
                index.append(lax.rem(spot, 2))
            elif name == "z_hi":
                index.append(lax.div(spot, 2))
            else:
                index.append(spot)
        return ref.at[tuple(index)]

    def ring_copies(c, s, ks):
        dim = ORDERS[c][s]
        copies = []
        for part in range(2 if s == 0 else 1):
            for k in ks:
                src, dst = piece(c, s, ring_place(dim, k)), landed[c][s].at[k - 1]
                if s == 0:
                    rows = pl.ds(part * (dst.shape[0] // 2), dst.shape[0] // 2)
                    src, dst = src.at[rows], dst.at[rows]
                number = 12 * c + (6 * part + k - 1 if s == 0 else 3 + 6 * (s - 1) + k - 1)
                copies.append(
                    remote(src, dst, ring_send.at[number], ring_recv.at[number], ring_peer(dim, k))
                )
        return copies

    for c in range(3):
        first, width = COLORS[c]
        cols = slice(first, first + width)
        core_copy(c).wait_recv()
        for zl in range(2):
            for x in range(4):
                held[c][0][zl, x] = sym[core, zl, x, :, :, :, cols] + core_in[zl, x, :, :, :, cols]
        for copy in ring_copies(c, 0, (2, 1, 3)):
            copy.start()
    for s in range(3):
        for c in range(3):
            first, width = COLORS[c]
            for copy in ring_copies(c, s, (1, 3, 2)):
                copy.wait_recv()
            total = piece(c, s, ring_place(ORDERS[c][s], 0))[...]
            for k in (1, 3, 2):
                total = total + landed[c][s][k - 1]
            if s < 2:
                held[c][s + 1][...] = total
                for copy in ring_copies(c, s + 1, (2, 1, 3)):
                    copy.start()
            else:
                for tile in range(width // 128):
                    col = first + 128 * tile
                    part = total[:, 128 * tile : 128 * tile + 128]
                    out[:, col : col + 128] = part
    for c in range(3):
        core_copy(c).wait_send()
        for s in range(3):
            for copy in ring_copies(c, s, (1, 2, 3)):
                copy.wait_send()

    @pl.loop(0, SX)
    def _(x):
        @pl.when(has(0, 1))
        def _():
            up(x).wait_send()

        @pl.when(has(0, -1))
        def _():
            down(x).wait_send()

    for index in range(4):

        @pl.when(side_sent(index))
        def _():
            side(index).wait_send()

    for dx in (1, -1):

        @pl.when(has(dx, 0))
        def _():
            for row in range(SY):
                face(dx, row).wait_send()

    for n in range(8):
        zpiece(n).wait_send()
        dx, dy = zrows[n + 1][:2]

        @pl.when(has(-dx, -dy))
        def _():
            zcopy(n + 1, -dx, -dy).wait_send()


def ring_buffers():
    buffers = []
    for (_, width), order in zip(COLORS, ORDERS):
        for s in range(3):
            left = [n for d, n in (("z", 2), ("x", 4), ("y", 4), ("z", 2)) if d in order[s:]]
            after = [n for d, n in (("z", 2), ("x", 4), ("y", 4), ("z", 2)) if d in order[s + 1 :]]
            buffers.append(pltpu.VMEM((*left, 4, width), F32))
            buffers.append(pltpu.VMEM((3, *after, 4, width), F32))
    return buffers


def local_products(eigvecs, material):
    tz, sel, txy, t2, t4, t2t, pick = constants()
    small = (
        jnp.asarray(tz, BF16), jnp.asarray(sel), jnp.asarray(txy), jnp.asarray(t2, BF16),
        jnp.asarray(t4, BF16), jnp.asarray(t2t), jnp.asarray(pick, BF16),
    )
    vmem = pl.BlockSpec(memory_space=pltpu.VMEM)
    dma = pltpu.SemaphoreType.DMA
    return pl.pallas_call(
        local_kernel,
        out_shape=jax.ShapeDtypeStruct((4, 2 * K), F32),
        in_specs=[pl.BlockSpec(memory_space=pl.ANY)] + [vmem] * 8,
        out_specs=vmem,
        scratch_shapes=[
            pltpu.VMEM((PX, PY, SZ, K), BF16),
            [pltpu.VMEM((PY, SZ, K), BF16)] * 2,
            [pltpu.VMEM((PY, SZ, K), BF16)] * 2,
            [pltpu.VMEM((SY, SZ, K), BF16)] * 6,
            [pltpu.VMEM((SY, SZ, K), BF16)] * 6,
            [pltpu.VMEM((PAIR_ROWS, 2 * K), BF16)] * 2,
            [pltpu.VMEM((K, PAIR_ROWS), BF16)] * 2,
            pltpu.VMEM((PY * SZ, 2 * K), BF16),
            pltpu.VMEM((K, PY * SZ), BF16),
            pltpu.VMEM((PX, 3, SZ, 128), F32),
            pltpu.VMEM((K, 2 * K), F32),
            pltpu.VMEM((SX * SY, K), F32),
            pltpu.VMEM((64, K), BF16),
            pltpu.VMEM((256, K), BF16),
            pltpu.VMEM((SX * SY, K), BF16),
            dma((SX,)), dma((SX,)), dma((SX,)), dma((SX,)), dma((SX,)),
            dma((4,)), dma((4,)), dma((9,)), dma((9,)),
            dma((2, SY)), dma((2, SY)), dma((8,)), dma((8,)),
            pltpu.VMEM((2, 2, 4, 4, 2, 4, 2 * K), F32),
            pltpu.VMEM((2, 4, 4, 2, 4, 2 * K), F32),
            *ring_buffers(),
            dma((3,)), dma((3,)), dma((36,)), dma((36,)),
        ],
        compiler_params=pltpu.CompilerParams(
            collective_id=0, has_side_effects=True, vmem_limit_bytes=60 * 1024 * 1024
        ),
    )(eigvecs, material, *small)


def per_device(eigvecs, material):
    both = local_products(eigvecs, material)
    return both[:, :K], both[:, K:]


def solution(mesh):
    return jax.shard_map(
        per_device,
        mesh=mesh,
        in_specs=(P("gx", "gy", "gz", None), P(None, "gx", "gy", "gz")),
        out_specs=(P(("gx", "gy", "gz"), None), P(("gx", "gy", "gz"), None)),
        check_vma=False,
    )
```
